8 devices in a mesh: data: 1 (over z), fsdp: 2 (over y), ep: 4 (over x, core).
Axes of the slice: x: 2, y: 2, z: 1, core: 2. Of those that a mesh axis runs over, the one named last changes fastest.
Arguments:
- tokens: bfloat16 [64, 512, 1024], P(('data', 'fsdp', 'ep'))
- w_qkv: bfloat16 [1024, 3, 16, 64], P('fsdp')
- w_out: bfloat16 [16, 64, 1024], P(None, None, 'fsdp')
- w_gate: bfloat16 [32, 1024, 512], P('ep', 'fsdp')
- w_up: bfloat16 [32, 1024, 512], P('ep', 'fsdp')
- w_down: bfloat16 [32, 512, 1024], P('ep', None, 'fsdp')
- expert_idx: int32 [64, 512, 8], P(('data', 'fsdp', 'ep'))
- expert_slot: int32 [64, 512, 8], P(('data', 'fsdp', 'ep'))
- gate_wts: bfloat16 [64, 512, 8], P(('data', 'fsdp', 'ep'))
- d_out: bfloat16 [64, 512, 1024], P(('data', 'fsdp', 'ep'))
Outputs:
- output 1: bfloat16 [64, 512, 1024], P(('data', 'fsdp', 'ep'))
- output 2: bfloat16 [64, 512, 1024], P(('data', 'fsdp', 'ep'))
- output 3: float32 [32, 1024, 512], P(('data', 'ep'), 'fsdp')
- output 4: float32 [32, 1024, 512], P(('data', 'ep'), 'fsdp')
- output 5: float32 [32, 512, 1024], P(('data', 'ep'), None, 'fsdp')
All inputs are finite; a program needn't handle non-finite values.
Results may differ from the reference program's by a relative error of at most 0.02.
Values are sent between devices in bfloat16 or wider.
A program may use at most 1 GiB of HBM per device.

```python
import jax
import jax.numpy as jnp
from jax import lax

SEQ_DEV = 8
SEQ_LEN = 512
D_MODEL = 1024
D_FF = 512
N_EXPERTS = 32
TOP_K = 8
N_HEADS = 16
HEAD_DIM = 64
FSDP_SIZE = 2
EP_SIZE = 4
CAPACITY = 1280

GROUPS = FSDP_SIZE * EP_SIZE
TOK_DEV = SEQ_DEV * SEQ_LEN
N_BATCH = GROUPS * SEQ_DEV


def draw_routing(key):
    key_bias, key_hot, key_noise, key_order = jax.random.split(key, 4)
    n_assign = TOK_DEV * TOP_K
    expert_ids = jnp.arange(N_EXPERTS, dtype=jnp.int32)
    expert_bias = jax.random.randint(key_bias, (GROUPS, 1, N_EXPERTS), 0, 512, dtype=jnp.int32)
    hot_expert = jax.random.randint(key_hot, (GROUPS, 1, 1), 0, N_EXPERTS, dtype=jnp.int32)
    noise_int = jax.random.randint(key_noise, (GROUPS, TOK_DEV, N_EXPERTS), 0, 1024, dtype=jnp.int32)
    hot_bonus = jnp.where(expert_ids[None, None, :] == hot_expert, 2048, 0).astype(jnp.int32)
    scores = (noise_int + expert_bias + hot_bonus) * N_EXPERTS + expert_ids[None, None, :]
    chosen = lax.top_k(scores, TOP_K)[1].astype(jnp.int32)
    flat_ids = chosen.reshape(GROUPS, n_assign)
    priority = jax.vmap(lambda key_one: jax.random.permutation(key_one, n_assign))(jax.random.split(key_order, GROUPS)).astype(jnp.int32)
    sort_order = jnp.argsort(flat_ids * n_assign + priority, axis=1)
    sorted_ids = jnp.take_along_axis(flat_ids, sort_order, axis=1)
    counts = jax.vmap(lambda ids_one: jnp.bincount(ids_one, length=N_EXPERTS))(flat_ids).astype(jnp.int32)
    starts = jnp.cumsum(counts, axis=1) - counts
    rank_sorted = jnp.arange(n_assign, dtype=jnp.int32)[None, :] - jnp.take_along_axis(starts, sorted_ids, axis=1)
    slot_rank = jax.vmap(lambda order_one, rank_one: jnp.zeros((n_assign,), jnp.int32).at[order_one].set(rank_one))(sort_order, rank_sorted)
    slot_ids = jnp.where(slot_rank < CAPACITY, slot_rank, -1).astype(jnp.int32)
    return chosen.reshape(N_BATCH, SEQ_LEN, TOP_K), slot_ids.reshape(N_BATCH, SEQ_LEN, TOP_K)


def setup_inputs(seed: int = 0, part: int = 0) -> dict:
    part_key = jax.random.fold_in(jax.random.key(seed), part)
    key_tok, key_gate, key_dout, key_route = jax.random.split(part_key, 4)
    key_qkv, key_out, key_w1, key_w3, key_w2 = jax.random.split(jax.random.key(seed + 1), 5)
    tokens = jax.random.normal(key_tok, (N_BATCH, SEQ_LEN, D_MODEL), jnp.float32).astype(jnp.bfloat16)
    w_qkv = (jax.random.normal(key_qkv, (D_MODEL, 3, N_HEADS, HEAD_DIM), jnp.float32) * (1.5 * D_MODEL ** -0.5)).astype(jnp.bfloat16)
    w_out = (jax.random.normal(key_out, (N_HEADS, HEAD_DIM, D_MODEL), jnp.float32) * (N_HEADS * HEAD_DIM) ** -0.5).astype(jnp.bfloat16)
    w_gate = (jax.random.normal(key_w1, (N_EXPERTS, D_MODEL, D_FF), jnp.float32) * D_MODEL ** -0.5).astype(jnp.bfloat16)
    w_up = (jax.random.normal(key_w3, (N_EXPERTS, D_MODEL, D_FF), jnp.float32) * D_MODEL ** -0.5).astype(jnp.bfloat16)
    w_down = (jax.random.normal(key_w2, (N_EXPERTS, D_FF, D_MODEL), jnp.float32) * (1.5 * D_FF ** -0.5)).astype(jnp.bfloat16)
    expert_idx, expert_slot = draw_routing(key_route)
    gate_wts = jax.random.uniform(key_gate, (N_BATCH, SEQ_LEN, TOP_K), jnp.float32, 0.2, 1.0).astype(jnp.bfloat16)
    d_out = jax.random.normal(key_dout, (N_BATCH, SEQ_LEN, D_MODEL), jnp.float32).astype(jnp.bfloat16)
    return {'tokens': tokens, 'w_qkv': w_qkv, 'w_out': w_out, 'w_gate': w_gate, 'w_up': w_up, 'w_down': w_down, 'expert_idx': expert_idx, 'expert_slot': expert_slot, 'gate_wts': gate_wts, 'd_out': d_out}


def rms_norm(values):
    wide_vals = values.astype(jnp.float32)
    inv_rms = lax.rsqrt(jnp.mean(wide_vals * wide_vals, axis=-1, keepdims=True) + 1e-6)
    return (wide_vals * inv_rms).astype(jnp.bfloat16)


def attend_group(tok_grp, wqkv_f, wout_f):
    normed = rms_norm(tok_grp).astype(jnp.float32)
    qkv_all = jnp.einsum('bsd,dthe->bsthe', normed, wqkv_f).astype(jnp.bfloat16).astype(jnp.float32)
    scores = jnp.einsum('bqhe,bkhe->bhqk', qkv_all[:, :, 0], qkv_all[:, :, 1]) * (HEAD_DIM ** -0.5)
    causal = lax.broadcasted_iota(jnp.int32, (SEQ_LEN, SEQ_LEN), 0) >= lax.broadcasted_iota(jnp.int32, (SEQ_LEN, SEQ_LEN), 1)
    attn_probs = jax.nn.softmax(jnp.where(causal, scores, -1e30), axis=-1).astype(jnp.bfloat16).astype(jnp.float32)
    context = jnp.einsum('bhqk,bkhe->bqhe', attn_probs, qkv_all[:, :, 2]).astype(jnp.bfloat16).astype(jnp.float32)
    attn_proj = jnp.einsum('bqhe,hed->bqd', context, wout_f)
    return (tok_grp.astype(jnp.float32) + attn_proj).astype(jnp.bfloat16)


def moe_group(h_grp, idx_one, slot_one, gate_one, w1_f, w3_f, w2_f):
    n_assign = TOK_DEV * TOP_K
    h_tok = h_grp.reshape(TOK_DEV, D_MODEL)
    u_tok = rms_norm(h_tok)
    flat_slot = slot_one.reshape(n_assign)
    row_pos = jnp.where(flat_slot >= 0, idx_one.reshape(n_assign) * CAPACITY + flat_slot, N_EXPERTS * CAPACITY)
    src_assign = jnp.full((N_EXPERTS * CAPACITY,), n_assign, jnp.int32).at[row_pos].set(jnp.arange(n_assign, dtype=jnp.int32), mode='drop')
    disp_buf = jnp.take(u_tok, src_assign // TOP_K, axis=0, mode='fill', fill_value=0)
    disp_f = disp_buf.reshape(N_EXPERTS, CAPACITY, D_MODEL).astype(jnp.float32)
    act_a = jnp.einsum('ecd,edf->ecf', disp_f, w1_f)
    act_b = jnp.einsum('ecd,edf->ecf', disp_f, w3_f)
    gated_act = (jax.nn.silu(act_a) * act_b).astype(jnp.bfloat16).astype(jnp.float32)
    y_buf = jnp.einsum('ecf,efd->ecd', gated_act, w2_f).astype(jnp.bfloat16).reshape(N_EXPERTS * CAPACITY, D_MODEL)
    y_rows = jnp.take(y_buf, row_pos, axis=0, mode='fill', fill_value=0).reshape(TOK_DEV, TOP_K, D_MODEL)
    mixed_sum = jnp.sum(y_rows.astype(jnp.float32) * gate_one.reshape(TOK_DEV, TOP_K, 1).astype(jnp.float32), axis=1)
    return (h_tok.astype(jnp.float32) + mixed_sum).astype(jnp.bfloat16).reshape(SEQ_DEV, SEQ_LEN, D_MODEL)


def reference(tokens, w_qkv, w_out, w_gate, w_up, w_down, expert_idx, expert_slot, gate_wts, d_out):
    wqkv_f = w_qkv.astype(jnp.float32)
    wout_f = w_out.astype(jnp.float32)
    idx_grp = expert_idx.reshape(GROUPS, SEQ_DEV, SEQ_LEN, TOP_K)
    slot_grp = expert_slot.reshape(GROUPS, SEQ_DEV, SEQ_LEN, TOP_K)
    gate_grp = gate_wts.reshape(GROUPS, SEQ_DEV, SEQ_LEN, TOP_K)

    def forward(tok_in, w1_f, w3_f, w2_f):
        def one_group(args_grp):
            tok_grp, idx_one, slot_one, gate_one = args_grp
            h_grp = attend_group(tok_grp, wqkv_f, wout_f)
            return moe_group(h_grp, idx_one, slot_one, gate_one, w1_f, w3_f, w2_f)
        group_outs = lax.map(jax.checkpoint(one_group), (tok_in.reshape(GROUPS, SEQ_DEV, SEQ_LEN, D_MODEL), idx_grp, slot_grp, gate_grp))
        return group_outs.reshape(N_BATCH, SEQ_LEN, D_MODEL)

    layer_out, pullback = jax.vjp(forward, tokens, w_gate.astype(jnp.float32), w_up.astype(jnp.float32), w_down.astype(jnp.float32))
    d_tokens, dw_gate, dw_up, dw_down = pullback(d_out)
    return layer_out, d_tokens, dw_gate, dw_up, dw_down
```

```python
import functools

import jax
import jax.numpy as jnp
from jax import lax
from jax.experimental import pallas as pl
from jax.experimental.pallas import tpu as pltpu
from jax.sharding import PartitionSpec as P

F32 = jnp.float32
BF16 = jnp.bfloat16
BLOCK = 256
TILE = 256
ALIGN = 16
EPS = 1e-6


def rms_norm(values):
    wide_vals = values.astype(F32)
    inv_rms = lax.rsqrt(jnp.mean(wide_vals * wide_vals, axis=-1, keepdims=True) + EPS)
    return (wide_vals * inv_rms).astype(BF16)


def attention_block(tok_seq, w_qkv, w_out):
    seq_len = tok_seq.shape[1]
    head_dim = w_qkv.shape[3]
    normed = rms_norm(tok_seq)
    qkv_all = jnp.einsum('bsd,dthe->tbshe', normed, w_qkv, preferred_element_type=F32).astype(BF16)
    scores = jnp.einsum('bqhe,bkhe->bhqk', qkv_all[0], qkv_all[1], preferred_element_type=F32) * (head_dim ** -0.5)
    causal = lax.broadcasted_iota(jnp.int32, (seq_len, seq_len), 0) >= lax.broadcasted_iota(jnp.int32, (seq_len, seq_len), 1)
    attn_probs = jax.nn.softmax(jnp.where(causal, scores, -1e30), axis=-1).astype(BF16)
    context = jnp.einsum('bhqk,bkhe->bqhe', attn_probs, qkv_all[2], preferred_element_type=F32).astype(BF16)
    attn_proj = jnp.einsum('crif,ife->cre', context, w_out, preferred_element_type=F32)
    return (tok_seq.astype(F32) + attn_proj).astype(BF16)


def capacity_of(tok_count, top_k, num_experts):
    return max(8, (5 * tok_count * top_k // (4 * num_experts) + 7) // 8 * 8)


def route(expert_idx, expert_slot, num_experts):
    n_seq, seq_len, top_k = expert_idx.shape
    per_seq = seq_len // BLOCK

    def blocks(values):
        values = values.transpose(0, 2, 1).reshape(n_seq, top_k, per_seq, BLOCK)
        return values.transpose(0, 2, 1, 3).reshape(n_seq * per_seq, top_k, BLOCK)

    idx_b, slot_b = blocks(expert_idx), blocks(expert_slot)
    kept = slot_b >= 0
    ids = jnp.arange(num_experts, dtype=jnp.int32)[None, :, None]
    member = jnp.zeros((idx_b.shape[0], num_experts, BLOCK), BF16)
    for j in range(top_k):
        member = member + ((idx_b[:, j:j + 1] == ids) & kept[:, j:j + 1]).astype(BF16)
    upper = (jnp.arange(BLOCK)[:, None] <= jnp.arange(BLOCK)[None, :]).astype(BF16)
    count = jnp.einsum('bet,ts->bes', member, upper, preferred_element_type=F32).astype(jnp.int32)
    seg_rows = (count[:, :, -1] + (ALIGN - 1)) // ALIGN * ALIGN
    seg_start = jnp.cumsum(seg_rows, axis=1) - seg_rows
    seg_off = jnp.cumsum(seg_rows, axis=0) - seg_rows
    place = seg_start[:, :, None] + count - 1
    dest = []
    for j in range(top_k):
        hit = (idx_b[:, j:j + 1] == ids)
        row = jnp.sum(jnp.where(hit, place, 0), axis=1)
        dest.append(jnp.where(kept[:, j], row, -1))
    dest = jnp.stack(dest, axis=1)
    return dest, seg_start, seg_rows, seg_off


def one_hot(dest_ref, gate_ref, first_row):
    rows = lax.broadcasted_iota(jnp.int32, (TILE, BLOCK), 0) + first_row
    dest = dest_ref[0]
    gate = gate_ref[0]
    picked = jnp.zeros((TILE, BLOCK), F32)
    for j in range(dest.shape[0]):
        picked = jnp.where(rows == dest[j:j + 1], gate[j:j + 1], picked)
    return picked


def dispatch_kernel(start_ref, rows_ref, off_ref, h_ref, dout_ref, dest_ref, gate_ref, r_hbm, d_hbm, u_s, rbuf, dbuf, sem):
    b = pl.program_id(0)
    n_blocks = pl.num_programs(0)
    n_exp = rows_ref.shape[1]
    slot = lax.rem(b, 2)

    def total(blk):
        return start_ref[blk, n_exp - 1] + rows_ref[blk, n_exp - 1]

    def drain(blk, which):
        n = pl.multiple_of(total(blk), ALIGN)

        @pl.when(n > 0)
        def _():
            pltpu.make_async_copy(rbuf.at[which, pl.ds(0, n), :], rbuf.at[which, pl.ds(0, n), :], sem.at[0, which]).wait()
            pltpu.make_async_copy(dbuf.at[which, pl.ds(0, n), :], dbuf.at[which, pl.ds(0, n), :], sem.at[1, which]).wait()

    @pl.when(b >= 2)
    def _():
        drain(b - 2, slot)

    hf = h_ref[...].astype(F32)
    u_s[...] = (hf * lax.rsqrt(jnp.mean(hf * hf, axis=-1, keepdims=True) + EPS)).astype(BF16)

    def tile(i, carry):
        first = pl.multiple_of(i * TILE, TILE)
        picked = one_hot(dest_ref, gate_ref, first)
        ones = jnp.where(picked > 0, 1.0, 0.0).astype(BF16)
        rbuf[slot, pl.ds(first, TILE), :] = jnp.dot(ones, u_s[...], preferred_element_type=F32).astype(BF16)
        dbuf[slot, pl.ds(first, TILE), :] = jnp.dot(picked.astype(BF16), dout_ref[...], preferred_element_type=F32).astype(BF16)
        return carry

    lax.fori_loop(0, (total(b) + (TILE - 1)) // TILE, tile, 0)

    def send(e, carry):
        n = pl.multiple_of(rows_ref[b, e], ALIGN)
        src = pl.multiple_of(start_ref[b, e], ALIGN)
        dst = pl.multiple_of(off_ref[b, e], ALIGN)

        @pl.when(n > 0)
        def _():
            pltpu.make_async_copy(rbuf.at[slot, pl.ds(src, n), :], r_hbm.at[e, pl.ds(dst, n), :], sem.at[0, slot]).start()
            pltpu.make_async_copy(dbuf.at[slot, pl.ds(src, n), :], d_hbm.at[e, pl.ds(dst, n), :], sem.at[1, slot]).start()
        return carry

    lax.fori_loop(0, n_exp, send, 0)

    @pl.when(b == n_blocks - 1)
    def _():
        @pl.when(n_blocks > 1)
        def _():
            drain(b - 1, 1 - slot)
        drain(b, slot)


def dispatch(h_tok, dout_tok, dest, gate, segs, num_experts, max_rows):
    tok_count, d_model = h_tok.shape
    n_blocks, top_k, _ = dest.shape
    buf_rows = -(-(BLOCK * top_k + num_experts * (ALIGN - 1)) // TILE) * TILE
    tok_spec = pl.BlockSpec((BLOCK, d_model), lambda b, *_: (b, 0))
    map_spec = pl.BlockSpec((1, top_k, BLOCK), lambda b, *_: (b, 0, 0))
    rows_shape = jax.ShapeDtypeStruct((num_experts, max_rows, d_model), BF16)
    return pl.pallas_call(
        dispatch_kernel,
        grid_spec=pltpu.PrefetchScalarGridSpec(
            num_scalar_prefetch=3,
            grid=(n_blocks,),
            in_specs=[tok_spec, tok_spec, map_spec, map_spec],
            out_specs=[pl.BlockSpec(memory_space=pl.ANY), pl.BlockSpec(memory_space=pl.ANY)],
            scratch_shapes=[
                pltpu.VMEM((BLOCK, d_model), BF16),
                pltpu.VMEM((2, buf_rows, d_model), BF16),
                pltpu.VMEM((2, buf_rows, d_model), BF16),
                pltpu.SemaphoreType.DMA((2, 2)),
            ],
        ),
        out_shape=[rows_shape, rows_shape],
        compiler_params=pltpu.CompilerParams(dimension_semantics=('arbitrary',), vmem_limit_bytes=60 * 2 ** 20),
        cost_estimate=pl.CostEstimate(flops=80 * 10 ** 9, bytes_accessed=180 * 10 ** 6, transcendentals=0),
        name='dispatch',
    )(*segs, h_tok, dout_tok, dest, gate)


def nt_dot(lhs, rhs):
    return lax.dot_general(lhs, rhs, (((1,), (1,)), ((), ())), preferred_element_type=F32)


def tn_dot(lhs, rhs):
    return lax.dot_general(lhs, rhs, (((0,), (0,)), ((), ())), preferred_element_type=F32)


def expert_kernel(count_ref, r_ref, d_ref, w_ref, y_ref, dr_ref, dw_ref, *, expert_of):
    n_rows = count_ref[expert_of(pl.program_id(0))]
    dw_ref[...] = jnp.zeros(dw_ref.shape, F32)
    half = w_ref.shape[-1]

    def tile(i, carry):
        first = pl.multiple_of(i * TILE, TILE)
        valid = lax.broadcasted_iota(jnp.int32, (TILE, 1), 0) + first < n_rows
        r = jnp.where(valid, r_ref[0, pl.ds(first, TILE), :], 0)
        dy = jnp.where(valid, d_ref[0, pl.ds(first, TILE), :], 0)
        w1 = jnp.concatenate([w_ref[0, 0, 0, 0], w_ref[1, 0, 0, 0]], axis=0)
        w3 = jnp.concatenate([w_ref[0, 0, 1, 0], w_ref[1, 0, 1, 0]], axis=0)
        w2 = jnp.concatenate([w_ref[0, 0, 2, 0], w_ref[1, 0, 2, 0]], axis=1)
        act_a = jnp.dot(r, w1, preferred_element_type=F32)
        act_b = jnp.dot(r, w3, preferred_element_type=F32)
        d_g = nt_dot(dy, w2)
        sig = 1.0 / (1.0 + jnp.exp(-act_a))
        silu = act_a * sig
        g = (silu * act_b).astype(BF16)
        d_up = (d_g * silu).astype(BF16)
        d_gate = (d_g * act_b * sig * (1.0 + act_a * (1.0 - sig))).astype(BF16)
        y_ref[0, pl.ds(first, TILE), :] = jnp.dot(g, w2, preferred_element_type=F32).astype(BF16)
        dr_ref[0, pl.ds(first, TILE), :] = (nt_dot(d_gate, w1) + nt_dot(d_up, w3)).astype(BF16)
        r_lo, r_hi = r[:, :half], r[:, half:]
        dw_ref[0, 0, 0, 0] += tn_dot(r_lo, d_gate)
        dw_ref[1, 0, 0, 0] += tn_dot(r_hi, d_gate)
        dw_ref[0, 0, 1, 0] += tn_dot(r_lo, d_up)
        dw_ref[1, 0, 1, 0] += tn_dot(r_hi, d_up)
        dw_ref[0, 0, 2, 0] += tn_dot(g, dy[:, :half])
        dw_ref[1, 0, 2, 0] += tn_dot(g, dy[:, half:])
        return carry

    lax.fori_loop(0, (n_rows + (TILE - 1)) // TILE, tile, 0)


def experts(rows, d_rows, weights, counts, chunk, per_chunk, local_experts):
    _, max_rows, d_model = rows.shape
    n_fsdp, n_ep, three, _, half, _ = weights.shape

    def expert_of(g):
        return g // per_chunk * local_experts + chunk * per_chunk + lax.rem(g, per_chunk)

    row_spec = pl.BlockSpec((1, max_rows, d_model), lambda g, *_: (expert_of(g), 0, 0))
    w_spec = pl.BlockSpec((n_fsdp, 1, three, 1, half, half), lambda g, *_: (0, g // per_chunk, 0, lax.rem(g, per_chunk), 0, 0))
    return pl.pallas_call(
        functools.partial(expert_kernel, expert_of=expert_of),
        grid_spec=pltpu.PrefetchScalarGridSpec(
            num_scalar_prefetch=1,
            grid=(n_ep * per_chunk,),
            in_specs=[row_spec, row_spec, w_spec],
            out_specs=[row_spec, row_spec, w_spec],
        ),
        out_shape=[
            jax.ShapeDtypeStruct(rows.shape, BF16),
            jax.ShapeDtypeStruct(rows.shape, BF16),
            jax.ShapeDtypeStruct(weights.shape, F32),
        ],
        input_output_aliases={1: 0, 2: 1},
        compiler_params=pltpu.CompilerParams(dimension_semantics=('arbitrary',), vmem_limit_bytes=62 * 2 ** 20),
        cost_estimate=pl.CostEstimate(flops=110 * 10 ** 9, bytes_accessed=200 * 10 ** 6, transcendentals=0),
        name='experts',
    )(counts, rows, d_rows, weights)


def combine_kernel(start_ref, rows_ref, off_ref, y_hbm, dr_hbm, h_ref, dout_ref, dest_ref, gate_ref, out_ref, dh_ref, ybuf, dbuf, acc_y, acc_d, sem):
    b = pl.program_id(0)
    n_blocks = pl.num_programs(0)
    n_exp = rows_ref.shape[1]
    slot = lax.rem(b, 2)

    def total(blk):
        return start_ref[blk, n_exp - 1] + rows_ref[blk, n_exp - 1]

    def fetch(blk, which):
        def one(e, carry):
            n = pl.multiple_of(rows_ref[blk, e], ALIGN)
            dst = pl.multiple_of(start_ref[blk, e], ALIGN)
            src = pl.multiple_of(off_ref[blk, e], ALIGN)

            @pl.when(n > 0)
            def _():
                pltpu.make_async_copy(y_hbm.at[e, pl.ds(src, n), :], ybuf.at[which, pl.ds(dst, n), :], sem.at[0, which]).start()
                pltpu.make_async_copy(dr_hbm.at[e, pl.ds(src, n), :], dbuf.at[which, pl.ds(dst, n), :], sem.at[1, which]).start()
            return carry

        lax.fori_loop(0, n_exp, one, 0)

    @pl.when(b == 0)
    def _():
        ybuf[...] = jnp.zeros(ybuf.shape, BF16)
        dbuf[...] = jnp.zeros(dbuf.shape, BF16)
        fetch(0, 0)

    @pl.when(b + 1 < n_blocks)
    def _():
        fetch(b + 1, 1 - slot)

    n = pl.multiple_of(total(b), ALIGN)

    @pl.when(n > 0)
    def _():
        pltpu.make_async_copy(ybuf.at[slot, pl.ds(0, n), :], ybuf.at[slot, pl.ds(0, n), :], sem.at[0, slot]).wait()
        pltpu.make_async_copy(dbuf.at[slot, pl.ds(0, n), :], dbuf.at[slot, pl.ds(0, n), :], sem.at[1, slot]).wait()

    acc_y[...] = jnp.zeros(acc_y.shape, F32)
    acc_d[...] = jnp.zeros(acc_d.shape, F32)

    def tile(i, carry):
        first = pl.multiple_of(i * TILE, TILE)
        picked = one_hot(dest_ref, gate_ref, first)
        ones = jnp.where(picked > 0, 1.0, 0.0).astype(BF16)
        acc_y[...] += tn_dot(picked.astype(BF16), ybuf[slot, pl.ds(first, TILE), :])
        acc_d[...] += tn_dot(ones, dbuf[slot, pl.ds(first, TILE), :])
        return carry

    lax.fori_loop(0, (n + (TILE - 1)) // TILE, tile, 0)

    hf = h_ref[...].astype(F32)
    out_ref[...] = (hf + acc_y[...]).astype(BF16)
    d_u = acc_d[...].astype(BF16).astype(F32)
    inv = lax.rsqrt(jnp.mean(hf * hf, axis=-1, keepdims=True) + EPS)
    proj = jnp.mean(d_u * hf, axis=-1, keepdims=True)
    d_norm = (d_u * inv - hf * (inv * inv * inv * proj)).astype(BF16).astype(F32)
    dh_ref[...] = (dout_ref[...].astype(F32) + d_norm).astype(BF16)


def combine(y_rows, dr_rows, h_tok, dout_tok, dest, gate, segs):
    tok_count, d_model = h_tok.shape
    n_blocks, top_k, _ = dest.shape
    num_experts = y_rows.shape[0]
    buf_rows = -(-(BLOCK * top_k + num_experts * (ALIGN - 1)) // TILE) * TILE
    tok_spec = pl.BlockSpec((BLOCK, d_model), lambda b, *_: (b, 0))
    map_spec = pl.BlockSpec((1, top_k, BLOCK), lambda b, *_: (b, 0, 0))
    hbm = pl.BlockSpec(memory_space=pl.ANY)
    return pl.pallas_call(
        combine_kernel,
        grid_spec=pltpu.PrefetchScalarGridSpec(
            num_scalar_prefetch=3,
            grid=(n_blocks,),
            in_specs=[hbm, hbm, tok_spec, tok_spec, map_spec, map_spec],
            out_specs=[tok_spec, tok_spec],
            scratch_shapes=[
                pltpu.VMEM((2, buf_rows, d_model), BF16),
                pltpu.VMEM((2, buf_rows, d_model), BF16),
                pltpu.VMEM((BLOCK, d_model), F32),
                pltpu.VMEM((BLOCK, d_model), F32),
                pltpu.SemaphoreType.DMA((2, 2)),
            ],
        ),
        out_shape=[jax.ShapeDtypeStruct((tok_count, d_model), BF16)] * 2,
        compiler_params=pltpu.CompilerParams(dimension_semantics=('arbitrary',), vmem_limit_bytes=60 * 2 ** 20),
        cost_estimate=pl.CostEstimate(flops=90 * 10 ** 9, bytes_accessed=180 * 10 ** 6, transcendentals=0),
        name='combine',
    )(*segs, y_rows, dr_rows, h_tok, dout_tok, dest, gate)


N_CHUNKS = 4


def solution(mesh):
    ep_size, fsdp_size = mesh.shape['ep'], mesh.shape['fsdp']
    tok_spec = P(('data', 'fsdp', 'ep'))
    in_specs = (tok_spec, P('fsdp'), P(None, None, 'fsdp'), P('ep', 'fsdp'), P('ep', 'fsdp'), P('ep', None, 'fsdp'), tok_spec, tok_spec, tok_spec, tok_spec)
    out_specs = (tok_spec, tok_spec, P(('data', 'ep'), 'fsdp'), P(('data', 'ep'), 'fsdp'), P(('data', 'ep'), None, 'fsdp'))

    def device_fn(tokens, w_qkv, w_out, w_gate, w_up, w_down, expert_idx, expert_slot, gate_wts, d_out):
        n_seq, seq_len, d_model = tokens.shape
        tok_count = n_seq * seq_len
        top_k = expert_idx.shape[2]
        local_experts, half, _ = w_gate.shape
        num_experts = local_experts * ep_size
        n_blocks = tok_count // BLOCK
        capacity = capacity_of(tok_count, top_k, num_experts)
        max_rows = -(-(capacity + n_blocks * (ALIGN - 1)) // TILE) * TILE
        per_chunk = local_experts // N_CHUNKS

        qkv_full = lax.all_gather(w_qkv, 'fsdp', axis=0, tiled=True)
        out_full = lax.all_gather(w_out, 'fsdp', axis=2, tiled=True)
        weights = []
        for c in range(N_CHUNKS):
            part = slice(c * per_chunk, (c + 1) * per_chunk)
            mine = jnp.stack([w_gate[part], w_up[part], w_down[part]], axis=0)
            full = lax.all_gather(mine, ('fsdp', 'ep'), axis=0, tiled=False)
            weights.append(full.reshape(fsdp_size, ep_size, *mine.shape))

        dest, *segs = route(expert_idx, expert_slot, num_experts)
        counts = jnp.sum(segs[1], axis=0)
        gate = gate_wts.transpose(0, 2, 1).reshape(n_seq, top_k, seq_len // BLOCK, BLOCK)
        gate = gate.transpose(0, 2, 1, 3).reshape(n_blocks, top_k, BLOCK).astype(F32)

        h_seq, attn_pullback = jax.vjp(lambda tok_in: attention_block(tok_in, qkv_full, out_full), tokens)
        h_tok = h_seq.reshape(tok_count, d_model)
        dout_tok = d_out.reshape(tok_count, d_model)
        rows, d_rows = dispatch(h_tok, dout_tok, dest, gate, segs, num_experts, max_rows)
        parts = []
        for c in range(N_CHUNKS):
            rows, d_rows, d_w = experts(rows, d_rows, weights[c], counts, c, per_chunk, local_experts)
            d_w = d_w.reshape(fsdp_size * ep_size, 3, per_chunk, half, half)
            parts.append(lax.psum_scatter(d_w, ('fsdp', 'ep'), scatter_dimension=0, tiled=False))
        layer_out, d_h = combine(rows, d_rows, h_tok, dout_tok, dest, gate, segs)
        d_tokens = attn_pullback(d_h.reshape(n_seq, seq_len, d_model))[0]
        d_ws = [jnp.concatenate([part[k] for part in parts], axis=0) for k in range(3)]
        return layer_out.reshape(n_seq, seq_len, d_model), d_tokens, *d_ws

    return jax.shard_map(device_fn, mesh=mesh, in_specs=in_specs, out_specs=out_specs, check_vma=False)
```

```python
import functools

import jax
import jax.numpy as jnp
from jax import lax
from jax.experimental import pallas as pl
from jax.experimental.pallas import tpu as pltpu
from jax.sharding import PartitionSpec as P

F32 = jnp.float32
BF16 = jnp.bfloat16
BLOCK = 256
TILE = 256
ALIGN = 16
LANES = 128
EPS = 1e-6


def rms_norm(values):
    wide_vals = values.astype(F32)
    inv_rms = lax.rsqrt(jnp.mean(wide_vals * wide_vals, axis=-1, keepdims=True) + EPS)
    return (wide_vals * inv_rms).astype(BF16)


def attention_block(tok_seq, w_qkv, w_out):
    seq_len = tok_seq.shape[1]
    head_dim = w_qkv.shape[3]
    normed = rms_norm(tok_seq)
    qkv_all = jnp.einsum('bsd,dthe->tbshe', normed, w_qkv, preferred_element_type=F32).astype(BF16)
    scores = jnp.einsum('bqhe,bkhe->bhqk', qkv_all[0], qkv_all[1], preferred_element_type=F32) * (head_dim ** -0.5)
    causal = lax.broadcasted_iota(jnp.int32, (seq_len, seq_len), 0) >= lax.broadcasted_iota(jnp.int32, (seq_len, seq_len), 1)
    attn_probs = jax.nn.softmax(jnp.where(causal, scores, -1e30), axis=-1).astype(BF16)
    context = jnp.einsum('bhqk,bkhe->bqhe', attn_probs, qkv_all[2], preferred_element_type=F32).astype(BF16)
    attn_proj = jnp.einsum('crif,ife->cre', context, w_out, preferred_element_type=F32)
    return (tok_seq.astype(F32) + attn_proj).astype(BF16)


def capacity_of(tok_count, top_k, num_experts):
    return max(8, (5 * tok_count * top_k // (4 * num_experts) + 7) // 8 * 8)


def route_kernel(loc_ref, dest_ref, start_ref, rows_ref, off_ref, total, *, n_local):
    top_k = loc_ref.shape[1]
    ids = lax.broadcasted_iota(jnp.int32, (n_local, BLOCK), 0)
    upper = (lax.broadcasted_iota(jnp.int32, (BLOCK, BLOCK), 0) <= lax.broadcasted_iota(jnp.int32, (BLOCK, BLOCK), 1)).astype(F32).astype(BF16)
    before = (lax.broadcasted_iota(jnp.int32, (n_local, n_local), 0) > lax.broadcasted_iota(jnp.int32, (n_local, n_local), 1)).astype(F32).astype(BF16)

    @pl.when(pl.program_id(0) == 0)
    def _():
        total[...] = jnp.zeros(total.shape, jnp.int32)

    so_far = total[...]
    for s in range(loc_ref.shape[0]):
        for p in range(loc_ref.shape[2] // BLOCK):
            q = s * (loc_ref.shape[2] // BLOCK) + p
            loc = loc_ref[s, :, p * BLOCK:(p + 1) * BLOCK]
            member = jnp.zeros((n_local, BLOCK), F32)
            for j in range(top_k):
                member = jnp.where(loc[j:j + 1] == ids, 1.0, member)
            count = jnp.dot(member.astype(BF16), upper, preferred_element_type=F32)
            units = (count[:, BLOCK - 1:].astype(jnp.int32) + (ALIGN - 1)) // ALIGN
            units = jnp.broadcast_to(units, (n_local, LANES))
            start = jnp.dot(before, units.astype(F32).astype(BF16), preferred_element_type=F32).astype(jnp.int32) * ALIGN
            place = start[:, :1] + count.astype(jnp.int32) - 1
            for j in range(top_k):
                row = jnp.sum(jnp.where(loc[j:j + 1] == ids, place, 0), axis=0, keepdims=True)
                dest_ref[q, j:j + 1, :] = jnp.where(loc[j:j + 1] >= 0, row, -1)
            start_ref[q] = start
            rows_ref[q] = units * ALIGN
            off_ref[q] = so_far
            so_far = so_far + units * ALIGN
    total[...] = so_far


def route(local_ids, n_local):
    n_seq, top_k, seq_len = local_ids.shape
    per_seq = seq_len // BLOCK
    step = 2 if n_seq % 2 == 0 else 1
    n_blocks = n_seq * per_seq
    seg = jax.ShapeDtypeStruct((n_blocks, n_local, LANES), jnp.int32)
    seg_spec = pl.BlockSpec((step * per_seq, n_local, LANES), lambda s: (s, 0, 0))
    dest, *segs = pl.pallas_call(
        functools.partial(route_kernel, n_local=n_local),
        grid=(n_seq // step,),
        in_specs=[pl.BlockSpec((step, top_k, seq_len), lambda s: (s, 0, 0))],
        out_specs=[pl.BlockSpec((step * per_seq, top_k, BLOCK), lambda s: (s, 0, 0)), seg_spec, seg_spec, seg_spec],
        out_shape=[jax.ShapeDtypeStruct((n_blocks, top_k, BLOCK), jnp.int32), seg, seg, seg],
        scratch_shapes=[pltpu.VMEM((n_local, LANES), jnp.int32)],
        compiler_params=pltpu.CompilerParams(dimension_semantics=('arbitrary',)),
        cost_estimate=pl.CostEstimate(flops=10 ** 9, bytes_accessed=3 * 10 ** 6, transcendentals=0),
        name='route',
    )(local_ids)
    return dest, [part[:, :, 0] for part in segs]


def one_hot(dest_ref, gate_ref, first_row):
    rows = lax.broadcasted_iota(jnp.int32, (TILE, BLOCK), 0) + first_row
    dest = dest_ref[0]
    gate = gate_ref[0]
    picked = jnp.zeros((TILE, BLOCK), F32)
    for j in range(dest.shape[0]):
        picked = jnp.where(rows == dest[j:j + 1], gate[j:j + 1], picked)
    return picked


def dispatch_kernel(start_ref, rows_ref, off_ref, h_ref, dout_ref, dest_ref, gate_ref, *refs, base):
    r_hbm, d_hbm, u_s, rbuf, dbuf, sem = refs[-6:]
    step = pl.program_id(0)
    n_blocks = pl.num_programs(0)
    b = step + base
    n_exp = rows_ref.shape[1]
    slot = lax.rem(b, 2)

    def total(blk):
        return start_ref[blk, n_exp - 1] + rows_ref[blk, n_exp - 1]

    def drain(blk, which):
        n = pl.multiple_of(total(blk), ALIGN)

        @pl.when(n > 0)
        def _():
            pltpu.make_async_copy(rbuf.at[which, pl.ds(0, n), :], rbuf.at[which, pl.ds(0, n), :], sem.at[0, which]).wait()
            pltpu.make_async_copy(dbuf.at[which, pl.ds(0, n), :], dbuf.at[which, pl.ds(0, n), :], sem.at[1, which]).wait()

    @pl.when(step >= 2)
    def _():
        drain(b - 2, slot)

    hf = h_ref[...].astype(F32)
    u_s[...] = (hf * lax.rsqrt(jnp.mean(hf * hf, axis=-1, keepdims=True) + EPS)).astype(BF16)

    def tile(i, carry):
        first = pl.multiple_of(i * TILE, TILE)
        picked = one_hot(dest_ref, gate_ref, first)
        ones = jnp.where(picked > 0, 1.0, 0.0).astype(BF16)
        rbuf[slot, pl.ds(first, TILE), :] = jnp.dot(ones, u_s[...], preferred_element_type=F32).astype(BF16)
        dbuf[slot, pl.ds(first, TILE), :] = jnp.dot(picked.astype(BF16), dout_ref[...], preferred_element_type=F32).astype(BF16)
        return carry

    lax.fori_loop(0, (total(b) + (TILE - 1)) // TILE, tile, 0)

    def send(e, carry):
        n = pl.multiple_of(rows_ref[b, e], ALIGN)
        src = pl.multiple_of(start_ref[b, e], ALIGN)
        dst = pl.multiple_of(off_ref[b, e], ALIGN)

        @pl.when(n > 0)
        def _():
            pltpu.make_async_copy(rbuf.at[slot, pl.ds(src, n), :], r_hbm.at[e, pl.ds(dst, n), :], sem.at[0, slot]).start()
            pltpu.make_async_copy(dbuf.at[slot, pl.ds(src, n), :], d_hbm.at[e, pl.ds(dst, n), :], sem.at[1, slot]).start()
        return carry

    lax.fori_loop(0, n_exp, send, 0)

    @pl.when(step == n_blocks - 1)
    def _():
        @pl.when(n_blocks > 1)
        def _():
            drain(b - 1, 1 - slot)
        drain(b, slot)


def block_rows(top_k, n_local):
    return -(-(BLOCK * top_k + n_local * (ALIGN - 1)) // TILE) * TILE


def dispatch(h_tok, dout_tok, dest, gate, segs, base, held, n_local, max_rows):
    tok_count, d_model = h_tok.shape
    top_k = dest.shape[1]
    n_blocks = tok_count // BLOCK
    buf_rows = block_rows(top_k, n_local)
    tok_spec = pl.BlockSpec((BLOCK, d_model), lambda b, *_: (b, 0))
    map_spec = pl.BlockSpec((1, top_k, BLOCK), lambda b, *_: (b + base, 0, 0))
    rows_shape = jax.ShapeDtypeStruct((n_local, max_rows, d_model), BF16)
    hbm = pl.BlockSpec(memory_space=pl.ANY)
    return pl.pallas_call(
        functools.partial(dispatch_kernel, base=base),
        grid_spec=pltpu.PrefetchScalarGridSpec(
            num_scalar_prefetch=3,
            grid=(n_blocks,),
            in_specs=[tok_spec, tok_spec, map_spec, map_spec] + [hbm] * len(held),
            out_specs=[hbm, hbm],
            scratch_shapes=[
                pltpu.VMEM((BLOCK, d_model), BF16),
                pltpu.VMEM((2, buf_rows, d_model), BF16),
                pltpu.VMEM((2, buf_rows, d_model), BF16),
                pltpu.SemaphoreType.DMA((2, 2)),
            ],
        ),
        out_shape=[rows_shape, rows_shape],
        input_output_aliases={7: 0, 8: 1} if held else {},
        compiler_params=pltpu.CompilerParams(dimension_semantics=('arbitrary',), vmem_limit_bytes=60 * 2 ** 20),
        cost_estimate=pl.CostEstimate(flops=40 * 10 ** 9, bytes_accessed=90 * 10 ** 6, transcendentals=0),
        name='dispatch',
    )(*segs, h_tok, dout_tok, dest, gate, *held)


def nt_dot(lhs, rhs):
    return lax.dot_general(lhs, rhs, (((1,), (1,)), ((), ())), preferred_element_type=F32)


def tn_dot(lhs, rhs):
    return lax.dot_general(lhs, rhs, (((0,), (0,)), ((), ())), preferred_element_type=F32)


def expert_kernel(count_ref, r_hbm, d_hbm, w_ref, y_hbm, dr_hbm, dw_ref, rbuf, dbuf, ybuf, drbuf, done, in_sem, out_sem, *, expert_of):
    step = pl.program_id(0)
    n_steps = pl.num_programs(0)
    expert = expert_of(step)
    n_rows = count_ref[expert]
    n_tiles = jnp.maximum((n_rows + (TILE - 1)) // TILE, 1)
    half = w_ref.shape[-1]

    def loads(who, i, slot):
        rows = pl.ds(pl.multiple_of(i * TILE, TILE), TILE)
        return (pltpu.make_async_copy(r_hbm.at[who, rows, :], rbuf.at[slot], in_sem.at[0, slot]),
                pltpu.make_async_copy(d_hbm.at[who, rows, :], dbuf.at[slot], in_sem.at[1, slot]))

    def stores(who, i, slot):
        rows = pl.ds(pl.multiple_of(i * TILE, TILE), TILE)
        return (pltpu.make_async_copy(ybuf.at[slot], y_hbm.at[who, rows, :], out_sem.at[0, slot]),
                pltpu.make_async_copy(drbuf.at[slot], dr_hbm.at[who, rows, :], out_sem.at[1, slot]))

    @pl.when(step == 0)
    def _():
        done[0] = 0
        for copy in loads(expert, 0, 0):
            copy.start()

    before = done[0]
    dw_ref[...] = jnp.zeros(dw_ref.shape, F32)

    def tile(i, carry):
        slot = lax.rem(before + i, 2)
        first = i * TILE

        @pl.when(i + 1 < n_tiles)
        def _():
            for copy in loads(expert, i + 1, 1 - slot):
                copy.start()

        @pl.when((i + 1 == n_tiles) & (step + 1 < n_steps))
        def _():
            for copy in loads(expert_of(step + 1), 0, 1 - slot):
                copy.start()

        for copy in loads(expert, i, slot):
            copy.wait()

        @pl.when(before + i >= 2)
        def _():
            for copy in stores(expert, i, slot):
                copy.wait()

        valid = lax.broadcasted_iota(jnp.int32, (TILE, 1), 0) + first < n_rows
        r = jnp.where(valid, rbuf[slot], 0)
        dy = jnp.where(valid, dbuf[slot], 0)
        w1 = jnp.concatenate([w_ref[0, 0, 0, 0], w_ref[1, 0, 0, 0]], axis=0)
        w3 = jnp.concatenate([w_ref[0, 0, 1, 0], w_ref[1, 0, 1, 0]], axis=0)
        w2 = jnp.concatenate([w_ref[0, 0, 2, 0], w_ref[1, 0, 2, 0]], axis=1)
        act_a = jnp.dot(r, w1, preferred_element_type=F32)
        act_b = jnp.dot(r, w3, preferred_element_type=F32)
        d_g = nt_dot(dy, w2)
        sig = 1.0 / (1.0 + jnp.exp(-act_a))
        silu = act_a * sig
        g = (silu * act_b).astype(BF16)
        d_up = (d_g * silu).astype(BF16)
        d_gate = (d_g * act_b * sig * (1.0 + act_a * (1.0 - sig))).astype(BF16)
        ybuf[slot] = jnp.dot(g, w2, preferred_element_type=F32).astype(BF16)
        drbuf[slot] = (nt_dot(d_gate, w1) + nt_dot(d_up, w3)).astype(BF16)
        for copy in stores(expert, i, slot):
            copy.start()
        r_lo, r_hi = r[:, :half], r[:, half:]
        dw_ref[0, 0, 0, 0] += tn_dot(r_lo, d_gate)
        dw_ref[1, 0, 0, 0] += tn_dot(r_hi, d_gate)
        dw_ref[0, 0, 1, 0] += tn_dot(r_lo, d_up)
        dw_ref[1, 0, 1, 0] += tn_dot(r_hi, d_up)
        dw_ref[0, 0, 2, 0] += tn_dot(g, dy[:, :half])
        dw_ref[1, 0, 2, 0] += tn_dot(g, dy[:, half:])
        return carry

    lax.fori_loop(0, n_tiles, tile, 0)
    done[0] = before + n_tiles

    @pl.when(step == n_steps - 1)
    def _():
        last = before + n_tiles - 1
        for copy in stores(expert, 0, lax.rem(last, 2)):
            copy.wait()

        @pl.when(last >= 1)
        def _():
            for copy in stores(expert, 0, lax.rem(last + 1, 2)):
                copy.wait()


def experts(rows, d_rows, weights, counts, chunk, per_chunk, local_experts):
    d_model = rows.shape[2]
    n_fsdp, n_side, three, _, half, _ = weights.shape

    def expert_of(g):
        return g // per_chunk * local_experts + chunk * per_chunk + lax.rem(g, per_chunk)

    hbm = pl.BlockSpec(memory_space=pl.ANY)
    w_spec = pl.BlockSpec((n_fsdp, 1, three, 1, half, half), lambda g, *_: (0, g // per_chunk, 0, lax.rem(g, per_chunk), 0, 0))
    return pl.pallas_call(
        functools.partial(expert_kernel, expert_of=expert_of),
        grid_spec=pltpu.PrefetchScalarGridSpec(
            num_scalar_prefetch=1,
            grid=(n_side * per_chunk,),
            in_specs=[hbm, hbm, w_spec],
            out_specs=[hbm, hbm, w_spec],
            scratch_shapes=[pltpu.VMEM((2, TILE, d_model), BF16)] * 4 + [
                pltpu.SMEM((1,), jnp.int32),
                pltpu.SemaphoreType.DMA((2, 2)),
                pltpu.SemaphoreType.DMA((2, 2)),
            ],
        ),
        out_shape=[
            jax.ShapeDtypeStruct(rows.shape, BF16),
            jax.ShapeDtypeStruct(rows.shape, BF16),
            jax.ShapeDtypeStruct(weights.shape, F32),
        ],
        input_output_aliases={1: 0, 2: 1},
        compiler_params=pltpu.CompilerParams(dimension_semantics=('arbitrary',), vmem_limit_bytes=56 * 2 ** 20),
        cost_estimate=pl.CostEstimate(flops=110 * 10 ** 9, bytes_accessed=200 * 10 ** 6, transcendentals=0),
        name='experts',
    )(counts, rows, d_rows, weights)


def combine_kernel(start_ref, rows_ref, off_ref, y_hbm, dr_hbm, dest_ref, gate_ref, *refs, base, own):
    ybuf, dbuf, acc_y, acc_d, sem = refs[-5:]
    step = pl.program_id(0)
    n_blocks = pl.num_programs(0)
    b = step + base
    n_exp = rows_ref.shape[1]
    slot = lax.rem(step, 2)

    def total(blk):
        return start_ref[blk, n_exp - 1] + rows_ref[blk, n_exp - 1]

    def fetch(blk, which):
        def one(e, carry):
            n = pl.multiple_of(rows_ref[blk, e], ALIGN)
            dst = pl.multiple_of(start_ref[blk, e], ALIGN)
            src = pl.multiple_of(off_ref[blk, e], ALIGN)

            @pl.when(n > 0)
            def _():
                pltpu.make_async_copy(y_hbm.at[e, pl.ds(src, n), :], ybuf.at[which, pl.ds(dst, n), :], sem.at[0, which]).start()
                pltpu.make_async_copy(dr_hbm.at[e, pl.ds(src, n), :], dbuf.at[which, pl.ds(dst, n), :], sem.at[1, which]).start()
            return carry

        lax.fori_loop(0, n_exp, one, 0)

    @pl.when(step == 0)
    def _():
        ybuf[...] = jnp.zeros(ybuf.shape, BF16)
        dbuf[...] = jnp.zeros(dbuf.shape, BF16)
        fetch(b, 0)

    @pl.when(step + 1 < n_blocks)
    def _():
        fetch(b + 1, 1 - slot)

    n = pl.multiple_of(total(b), ALIGN)

    @pl.when(n > 0)
    def _():
        pltpu.make_async_copy(ybuf.at[slot, pl.ds(0, n), :], ybuf.at[slot, pl.ds(0, n), :], sem.at[0, slot]).wait()
        pltpu.make_async_copy(dbuf.at[slot, pl.ds(0, n), :], dbuf.at[slot, pl.ds(0, n), :], sem.at[1, slot]).wait()

    acc_y[...] = jnp.zeros(acc_y.shape, F32)
    acc_d[...] = jnp.zeros(acc_d.shape, F32)

    def tile(i, carry):
        first = pl.multiple_of(i * TILE, TILE)
        picked = one_hot(dest_ref, gate_ref, first)
        ones = jnp.where(picked > 0, 1.0, 0.0).astype(BF16)
        acc_y[...] += tn_dot(picked.astype(BF16), ybuf[slot, pl.ds(first, TILE), :])
        acc_d[...] += tn_dot(ones, dbuf[slot, pl.ds(first, TILE), :])
        return carry

    lax.fori_loop(0, (n + (TILE - 1)) // TILE, tile, 0)

    if not own:
        out_y, out_d = refs[:2]
        out_y[...] = acc_y[...]
        out_d[...] = acc_d[...]
        return
    more_y, more_d, h_ref, dout_ref, out_ref, dh_ref = refs[:6]
    hf = h_ref[...].astype(F32)
    out_ref[...] = (hf + (acc_y[...] + more_y[...])).astype(BF16)
    d_u = (acc_d[...] + more_d[...]).astype(BF16).astype(F32)
    inv = lax.rsqrt(jnp.mean(hf * hf, axis=-1, keepdims=True) + EPS)
    proj = jnp.mean(d_u * hf, axis=-1, keepdims=True)
    d_norm = (d_u * inv - hf * (inv * inv * inv * proj)).astype(BF16).astype(F32)
    dh_ref[...] = (dout_ref[...].astype(F32) + d_norm).astype(BF16)


def combine(y_rows, dr_rows, dest, gate, segs, base, n_blocks, extra):
    n_local, _, d_model = y_rows.shape
    top_k = dest.shape[1]
    buf_rows = block_rows(top_k, n_local)
    tok_spec = pl.BlockSpec((BLOCK, d_model), lambda b, *_: (b, 0))
    map_spec = pl.BlockSpec((1, top_k, BLOCK), lambda b, *_: (b + base, 0, 0))
    hbm = pl.BlockSpec(memory_space=pl.ANY)
    out = jax.ShapeDtypeStruct((n_blocks * BLOCK, d_model), BF16 if extra else F32)
    return pl.pallas_call(
        functools.partial(combine_kernel, base=base, own=bool(extra)),
        grid_spec=pltpu.PrefetchScalarGridSpec(
            num_scalar_prefetch=3,
            grid=(n_blocks,),
            in_specs=[hbm, hbm, map_spec, map_spec] + [tok_spec] * len(extra),
            out_specs=[tok_spec, tok_spec],
            scratch_shapes=[
                pltpu.VMEM((2, buf_rows, d_model), BF16),
                pltpu.VMEM((2, buf_rows, d_model), BF16),
                pltpu.VMEM((BLOCK, d_model), F32),
                pltpu.VMEM((BLOCK, d_model), F32),
                pltpu.SemaphoreType.DMA((2, 2)),
            ],
        ),
        out_shape=[out, out],
        compiler_params=pltpu.CompilerParams(dimension_semantics=('arbitrary',), vmem_limit_bytes=60 * 2 ** 20),
        cost_estimate=pl.CostEstimate(flops=45 * 10 ** 9, bytes_accessed=120 * 10 ** 6, transcendentals=0),
        name='combine',
    )(*segs, y_rows, dr_rows, dest, gate, *extra)


def place_kernel(part_ref, *refs):
    for k, out_ref in enumerate(refs[-3:]):
        out_ref[...] = part_ref[k]


def place(part, held, chunk, n_total):
    three, per_chunk, rows, cols = part.shape
    hbm = pl.BlockSpec(memory_space=pl.ANY)
    return pl.pallas_call(
        place_kernel,
        grid=(per_chunk,),
        in_specs=[pl.BlockSpec((three, 1, rows, cols), lambda i: (0, i, 0, 0))] + [hbm] * len(held),
        out_specs=[pl.BlockSpec((1, rows, cols), lambda i: (chunk * per_chunk + i, 0, 0))] * three,
        out_shape=[jax.ShapeDtypeStruct((n_total, rows, cols), F32)] * three,
        input_output_aliases={1: 0, 2: 1, 3: 2} if held else {},
        compiler_params=pltpu.CompilerParams(dimension_semantics=('arbitrary',)),
        cost_estimate=pl.CostEstimate(flops=3 * 10 ** 8, bytes_accessed=12 * 10 ** 6, transcendentals=0),
        name='place',
    )(part, *held)


N_CHUNKS = 4
CORES = 2


def solution(mesh):
    ep_size, fsdp_size = mesh.shape['ep'], mesh.shape['fsdp']
    tok_spec = P(('data', 'fsdp', 'ep'))
    in_specs = (tok_spec, P('fsdp'), P(None, None, 'fsdp'), P('ep', 'fsdp'), P('ep', 'fsdp'), P('ep', None, 'fsdp'), tok_spec, tok_spec, tok_spec, tok_spec)
    out_specs = (tok_spec, tok_spec, P(('data', 'ep'), 'fsdp'), P(('data', 'ep'), 'fsdp'), P(('data', 'ep'), None, 'fsdp'))

    def device_fn(tokens, w_qkv, w_out, w_gate, w_up, w_down, expert_idx, expert_slot, gate_wts, d_out):
        n_seq, seq_len, d_model = tokens.shape
        tok_count = n_seq * seq_len
        top_k = expert_idx.shape[2]
        local_experts, half, _ = w_gate.shape
        num_experts = local_experts * ep_size
        n_side = ep_size // CORES
        n_local = local_experts * n_side
        n_blocks = tok_count // BLOCK
        capacity = capacity_of(tok_count, top_k, num_experts)
        max_rows = -(-(CORES * (capacity + n_blocks * (ALIGN - 1))) // TILE) * TILE
        per_chunk = local_experts // N_CHUNKS
        ep = lax.axis_index('ep')
        groups = [[c + CORES * i for i in range(fsdp_size * n_side)] for c in range(CORES)]

        def swap(values):
            return lax.ppermute(values, 'ep', [(i, i ^ 1) for i in range(ep_size)])

        qkv_rows = half // ep_size
        qkv_full = lax.all_gather(lax.dynamic_slice_in_dim(w_qkv, ep * qkv_rows, qkv_rows, axis=0), ('fsdp', 'ep'), axis=0, tiled=True)
        n_heads, head_dim, out_cols = w_out.shape
        out_heads = n_heads // ep_size
        out_parts = lax.all_gather(lax.dynamic_slice_in_dim(w_out, ep * out_heads, out_heads, axis=0), ('fsdp', 'ep'), axis=0, tiled=True)
        out_full = out_parts.reshape(fsdp_size, n_heads, head_dim, out_cols).transpose(1, 2, 0, 3).reshape(n_heads, head_dim, d_model)
        weights = []
        for c in range(N_CHUNKS):
            part = slice(c * per_chunk, (c + 1) * per_chunk)
            mine = jnp.stack([w_gate[part], w_up[part], w_down[part]], axis=0)
            full = lax.all_gather(mine, ('fsdp', 'ep'), axis=0, tiled=False, axis_index_groups=groups)
            weights.append(full.reshape(fsdp_size, n_side, *mine.shape))

        dout_tok = d_out.reshape(tok_count, d_model)
        dout_other = swap(dout_tok)
        kept_ids = jnp.where(expert_slot >= 0, expert_idx, -1).transpose(0, 2, 1)
        all_ids = jnp.concatenate([kept_ids, swap(kept_ids)], axis=0)
        owner = all_ids // local_experts
        mine_too = (all_ids >= 0) & (lax.rem(owner, CORES) == lax.rem(ep, CORES))
        local_ids = jnp.where(mine_too, owner // CORES * local_experts + lax.rem(all_ids, local_experts), -1)
        dest, segs = route(local_ids, n_local)
        counts = jnp.sum(segs[1], axis=0)
        gate = gate_wts.transpose(0, 2, 1)
        gate = jnp.concatenate([gate, swap(gate)], axis=0).astype(F32)
        gate = gate.reshape(2 * n_seq, top_k, seq_len // BLOCK, BLOCK).transpose(0, 2, 1, 3).reshape(2 * n_blocks, top_k, BLOCK)

        h_seq, attn_pullback = jax.vjp(lambda tok_in: attention_block(tok_in, qkv_full, out_full), tokens)
        h_tok = h_seq.reshape(tok_count, d_model)
        h_other = swap(h_tok)
        held = dispatch(h_tok, dout_tok, dest, gate, segs, 0, [], n_local, max_rows)
        rows, d_rows = dispatch(h_other, dout_other, dest, gate, segs, n_blocks, held, n_local, max_rows)
        d_ws = []
        for c in range(N_CHUNKS):
            rows, d_rows, d_w = experts(rows, d_rows, weights[c], counts, c, per_chunk, local_experts)
            d_w = d_w.reshape(fsdp_size * n_side, 3, per_chunk, half, half)
            d_w = lax.psum_scatter(d_w, ('fsdp', 'ep'), scatter_dimension=0, tiled=False, axis_index_groups=groups)
            d_ws = place(d_w, d_ws, c, local_experts)
        sums = combine(rows, d_rows, dest, gate, segs, n_blocks, n_blocks, [])
        more = [swap(value) for value in sums]
        layer_out, d_h = combine(rows, d_rows, dest, gate, segs, 0, n_blocks, [*more, h_tok, dout_tok])
        d_tokens = attn_pullback(d_h.reshape(n_seq, seq_len, d_model))[0]
        return layer_out.reshape(n_seq, seq_len, d_model), d_tokens, *d_ws

    return jax.shard_map(device_fn, mesh=mesh, in_specs=in_specs, out_specs=out_specs, check_vma=False)
```

```python
import functools
import math

import jax
import jax.numpy as jnp
from jax import lax
from jax.experimental import pallas as pl
from jax.experimental.pallas import tpu as pltpu
from jax.sharding import PartitionSpec as P

F32 = jnp.float32
BF16 = jnp.bfloat16
BLOCK = 256
TILE = 256
ALIGN = 16
LANES = 128
LOG2E = math.log2(math.e)
EPS = 1e-6


def nt_dot(lhs, rhs):
    return lax.dot_general(lhs, rhs, (((1,), (1,)), ((), ())), preferred_element_type=F32)


def tn_dot(lhs, rhs):
    return lax.dot_general(lhs, rhs, (((0,), (0,)), ((), ())), preferred_element_type=F32)


def lanes_of(head, values):
    lane = lax.broadcasted_iota(jnp.int32, values.shape, 1)
    return jnp.where((lane >= LANES // 2) == bool(head), values, jnp.zeros_like(values))


def attention_kernel(x_ref, w_ref, h_ref, qkv_ref, ctx, *, head_dim):
    seq_len, d_model = x_ref.shape[1:]
    n_fsdp, n_ep, rows, half = w_ref.shape
    n_qkv = rows * 3 // 4
    x = x_ref[0].astype(F32)
    normed = (x * lax.rsqrt(jnp.mean(x * x, axis=-1, keepdims=True) + EPS)).astype(BF16)
    for p in range(n_ep):
        part = nt_dot(normed[:, :half], w_ref[0, p, :n_qkv]) + nt_dot(normed[:, half:], w_ref[1, p, :n_qkv])
        qkv_ref[0, :, p * n_qkv:(p + 1) * n_qkv] = part.astype(BF16)
    scale = head_dim ** -0.5 * LOG2E

    def pair(i, carry):
        q2, k2, v2 = (qkv_ref[0, :, pl.ds(pl.multiple_of(t * d_model + i * LANES, LANES), LANES)] for t in range(3))
        for first in range(0, seq_len, BLOCK):
            end = first + BLOCK
            keys, vals = k2[:end], v2[:end]
            causal = lax.broadcasted_iota(jnp.int32, (BLOCK, end), 0) + first >= lax.broadcasted_iota(jnp.int32, (BLOCK, end), 1)
            both = []
            for head in range(2):
                scores = nt_dot(lanes_of(head, q2[first:end]), keys) * scale
                scores = jnp.where(causal, scores, -1e30)
                probs = jnp.exp2(scores - jnp.max(scores, axis=-1, keepdims=True))
                probs = (probs * (1.0 / jnp.sum(probs, axis=-1, keepdims=True))).astype(BF16)
                both.append(jnp.dot(probs, vals, preferred_element_type=F32))
            lane = lax.broadcasted_iota(jnp.int32, (BLOCK, LANES), 1)
            ctx[first:end, pl.ds(pl.multiple_of(i * LANES, LANES), LANES)] = jnp.where(lane < LANES // 2, both[0], both[1]).astype(BF16)
        return carry

    lax.fori_loop(0, d_model // LANES, pair, 0)
    for f in range(n_fsdp):
        w_out = jnp.concatenate([w_ref[f, p, n_qkv:] for p in range(n_ep)], axis=0)
        cols = slice(f * half, (f + 1) * half)
        h_ref[0, :, cols] = (x_ref[0, :, cols].astype(F32) + jnp.dot(ctx[...], w_out, preferred_element_type=F32)).astype(BF16)


def attention(tokens, weights, head_dim):
    n_seq, seq_len, d_model = tokens.shape
    seq_spec = pl.BlockSpec((1, seq_len, d_model), lambda s: (s, 0, 0))
    qkv_spec = pl.BlockSpec((1, seq_len, 3 * d_model), lambda s: (s, 0, 0))
    w_spec = pl.BlockSpec(weights.shape, lambda s: (0, 0, 0, 0))
    return pl.pallas_call(
        functools.partial(attention_kernel, head_dim=head_dim),
        grid=(n_seq,),
        in_specs=[seq_spec, w_spec],
        out_specs=[seq_spec, qkv_spec],
        out_shape=[jax.ShapeDtypeStruct(tokens.shape, BF16), jax.ShapeDtypeStruct((n_seq, seq_len, 3 * d_model), BF16)],
        scratch_shapes=[pltpu.VMEM((seq_len, d_model), BF16)],
        compiler_params=pltpu.CompilerParams(dimension_semantics=('arbitrary',), vmem_limit_bytes=56 * 2 ** 20),
        cost_estimate=pl.CostEstimate(flops=90 * 10 ** 9, bytes_accessed=60 * 10 ** 6, transcendentals=0),
        name='attention',
    )(tokens, weights)


def attention_grad_kernel(dh_ref, x_ref, qkv_ref, w_ref, dx_ref, dctx, dqkv, *, head_dim):
    seq_len, d_model = x_ref.shape[1:]
    n_fsdp, n_ep, rows, half = w_ref.shape
    n_qkv = rows * 3 // 4
    n_out = rows - n_qkv
    dh = dh_ref[0]
    for p in range(n_ep):
        part = nt_dot(dh[:, :half], w_ref[0, p, n_qkv:]) + nt_dot(dh[:, half:], w_ref[1, p, n_qkv:])
        dctx[:, p * n_out:(p + 1) * n_out] = part.astype(BF16)
    scale = head_dim ** -0.5

    def pair(i, carry):
        col = pl.multiple_of(i * LANES, LANES)
        q2, k2, v2 = (qkv_ref[0, :, pl.ds(pl.multiple_of(t * d_model + i * LANES, LANES), LANES)] for t in range(3))
        d2 = dctx[:, pl.ds(col, LANES)]
        dk = [jnp.zeros((BLOCK, LANES), F32)] * (seq_len // BLOCK)
        dv = list(dk)
        for first in range(0, seq_len, BLOCK):
            end = first + BLOCK
            keys, vals = k2[:end], v2[:end]
            causal = lax.broadcasted_iota(jnp.int32, (end, BLOCK), 1) + first >= lax.broadcasted_iota(jnp.int32, (end, BLOCK), 0)
            dq = jnp.zeros((BLOCK, LANES), F32)
            for head in range(2):
                q, d = lanes_of(head, q2[first:end]), lanes_of(head, d2[first:end])
                scores = jnp.where(causal, nt_dot(keys, q) * (scale * LOG2E), -1e30)
                probs = jnp.exp2(scores - jnp.max(scores, axis=0, keepdims=True))
                probs = probs * (1.0 / jnp.sum(probs, axis=0, keepdims=True))
                d_probs = nt_dot(vals, d)
                d_scores = probs * (d_probs - jnp.sum(probs * d_probs, axis=0, keepdims=True))
                d_scores = (d_scores * scale).astype(BF16)
                dv_part = jnp.dot(probs.astype(BF16), d, preferred_element_type=F32)
                dk_part = jnp.dot(d_scores, q, preferred_element_type=F32)
                dq = dq + tn_dot(d_scores, lanes_of(head, keys))
                for n in range(end // BLOCK):
                    dk[n] = dk[n] + dk_part[n * BLOCK:(n + 1) * BLOCK]
                    dv[n] = dv[n] + dv_part[n * BLOCK:(n + 1) * BLOCK]
            dqkv[first:end, pl.ds(col, LANES)] = dq.astype(BF16)
        for n in range(seq_len // BLOCK):
            dqkv[n * BLOCK:(n + 1) * BLOCK, pl.ds(pl.multiple_of(d_model + i * LANES, LANES), LANES)] = dk[n].astype(BF16)
            dqkv[n * BLOCK:(n + 1) * BLOCK, pl.ds(pl.multiple_of(2 * d_model + i * LANES, LANES), LANES)] = dv[n].astype(BF16)
        return carry

    lax.fori_loop(0, d_model // LANES, pair, 0)
    x = x_ref[0].astype(F32)
    d_normed = []
    for f in range(n_fsdp):
        w_qkv = jnp.concatenate([w_ref[f, p, :n_qkv] for p in range(n_ep)], axis=0)
        d_normed.append(jnp.dot(dqkv[...], w_qkv, preferred_element_type=F32).astype(BF16))
    d_normed = jnp.concatenate(d_normed, axis=1).astype(F32)
    inv = lax.rsqrt(jnp.mean(x * x, axis=-1, keepdims=True) + EPS)
    proj = jnp.mean(d_normed * x, axis=-1, keepdims=True)
    d_x = (d_normed * inv - x * (inv * inv * inv * proj)).astype(BF16).astype(F32)
    dx_ref[0] = (dh_ref[0].astype(F32) + d_x).astype(BF16)


def attention_grad(d_h, tokens, qkv, weights, head_dim):
    n_seq, seq_len, d_model = tokens.shape
    seq_spec = pl.BlockSpec((1, seq_len, d_model), lambda s: (s, 0, 0))
    qkv_spec = pl.BlockSpec((1, seq_len, 3 * d_model), lambda s: (s, 0, 0))
    w_spec = pl.BlockSpec(weights.shape, lambda s: (0, 0, 0, 0))
    return pl.pallas_call(
        functools.partial(attention_grad_kernel, head_dim=head_dim),
        grid=(n_seq,),
        in_specs=[seq_spec, seq_spec, qkv_spec, w_spec],
        out_specs=seq_spec,
        out_shape=jax.ShapeDtypeStruct(tokens.shape, BF16),
        scratch_shapes=[pltpu.VMEM((seq_len, d_model), BF16), pltpu.VMEM((seq_len, 3 * d_model), BF16)],
        compiler_params=pltpu.CompilerParams(dimension_semantics=('arbitrary',), vmem_limit_bytes=56 * 2 ** 20),
        cost_estimate=pl.CostEstimate(flops=150 * 10 ** 9, bytes_accessed=70 * 10 ** 6, transcendentals=0),
        name='attention_grad',
    )(d_h, tokens, qkv, weights)


def capacity_of(tok_count, top_k, num_experts):
    return max(8, (5 * tok_count * top_k // (4 * num_experts) + 7) // 8 * 8)


def route_kernel(loc_ref, dest_ref, start_ref, rows_ref, off_ref, total, *, n_local):
    top_k = loc_ref.shape[1]
    ids = lax.broadcasted_iota(jnp.int32, (n_local, BLOCK), 0)
    upper = (lax.broadcasted_iota(jnp.int32, (BLOCK, BLOCK), 0) <= lax.broadcasted_iota(jnp.int32, (BLOCK, BLOCK), 1)).astype(F32).astype(BF16)
    before = (lax.broadcasted_iota(jnp.int32, (n_local, n_local), 0) > lax.broadcasted_iota(jnp.int32, (n_local, n_local), 1)).astype(F32).astype(BF16)

    @pl.when(pl.program_id(0) == 0)
    def _():
        total[...] = jnp.zeros(total.shape, jnp.int32)

    so_far = total[...]
    for s in range(loc_ref.shape[0]):
        for p in range(loc_ref.shape[2] // BLOCK):
            q = s * (loc_ref.shape[2] // BLOCK) + p
            loc = loc_ref[s, :, p * BLOCK:(p + 1) * BLOCK]
            member = jnp.zeros((n_local, BLOCK), F32)
            for j in range(top_k):
                member = jnp.where(loc[j:j + 1] == ids, 1.0, member)
            count = jnp.dot(member.astype(BF16), upper, preferred_element_type=F32)
            units = (count[:, BLOCK - 1:].astype(jnp.int32) + (ALIGN - 1)) // ALIGN
            units = jnp.broadcast_to(units, (n_local, LANES))
            start = jnp.dot(before, units.astype(F32).astype(BF16), preferred_element_type=F32).astype(jnp.int32) * ALIGN
            place = start[:, :1] + count.astype(jnp.int32) - 1
            for j in range(top_k):
                row = jnp.sum(jnp.where(loc[j:j + 1] == ids, place, 0), axis=0, keepdims=True)
                dest_ref[q, j:j + 1, :] = jnp.where(loc[j:j + 1] >= 0, row, -1)
            start_ref[q] = start
            rows_ref[q] = units * ALIGN
            off_ref[q] = so_far
            so_far = so_far + units * ALIGN
    total[...] = so_far


def route(local_ids, n_local):
    n_seq, top_k, seq_len = local_ids.shape
    per_seq = seq_len // BLOCK
    step = 2 if n_seq % 2 == 0 else 1
    n_blocks = n_seq * per_seq
    seg = jax.ShapeDtypeStruct((n_blocks, n_local, LANES), jnp.int32)
    seg_spec = pl.BlockSpec((step * per_seq, n_local, LANES), lambda s: (s, 0, 0))
    dest, *segs = pl.pallas_call(
        functools.partial(route_kernel, n_local=n_local),
        grid=(n_seq // step,),
        in_specs=[pl.BlockSpec((step, top_k, seq_len), lambda s: (s, 0, 0))],
        out_specs=[pl.BlockSpec((step * per_seq, top_k, BLOCK), lambda s: (s, 0, 0)), seg_spec, seg_spec, seg_spec],
        out_shape=[jax.ShapeDtypeStruct((n_blocks, top_k, BLOCK), jnp.int32), seg, seg, seg],
        scratch_shapes=[pltpu.VMEM((n_local, LANES), jnp.int32)],
        compiler_params=pltpu.CompilerParams(dimension_semantics=('arbitrary',)),
        cost_estimate=pl.CostEstimate(flops=10 ** 9, bytes_accessed=3 * 10 ** 6, transcendentals=0),
        name='route',
    )(local_ids)
    return dest, [part[:, :, 0] for part in segs]


def one_hot(dest_ref, gate_ref, first_row):
    rows = lax.broadcasted_iota(jnp.int32, (TILE, BLOCK), 0) + first_row
    dest = dest_ref[0]
    gate = gate_ref[0]
    picked = jnp.zeros((TILE, BLOCK), F32)
    for j in range(dest.shape[0]):
        picked = jnp.where(rows == dest[j:j + 1], gate[j:j + 1], picked)
    return picked


def dispatch_kernel(start_ref, rows_ref, off_ref, h_ref, dout_ref, dest_ref, gate_ref, *refs, base):
    r_hbm, d_hbm, u_s, rbuf, dbuf, sem = refs[-6:]
    step = pl.program_id(0)
    n_blocks = pl.num_programs(0)
    b = step + base
    n_exp = rows_ref.shape[1]
    slot = lax.rem(b, 2)

    def total(blk):
        return start_ref[blk, n_exp - 1] + rows_ref[blk, n_exp - 1]

    def drain(blk, which):
        n = pl.multiple_of(total(blk), ALIGN)

        @pl.when(n > 0)
        def _():
            pltpu.make_async_copy(rbuf.at[which, pl.ds(0, n), :], rbuf.at[which, pl.ds(0, n), :], sem.at[0, which]).wait()
            pltpu.make_async_copy(dbuf.at[which, pl.ds(0, n), :], dbuf.at[which, pl.ds(0, n), :], sem.at[1, which]).wait()

    @pl.when(step >= 2)
    def _():
        drain(b - 2, slot)

    hf = h_ref[...].astype(F32)
    u_s[...] = (hf * lax.rsqrt(jnp.mean(hf * hf, axis=-1, keepdims=True) + EPS)).astype(BF16)

    def tile(i, carry):
        first = pl.multiple_of(i * TILE, TILE)
        picked = one_hot(dest_ref, gate_ref, first)
        ones = jnp.where(picked > 0, 1.0, 0.0).astype(BF16)
        rbuf[slot, pl.ds(first, TILE), :] = jnp.dot(ones, u_s[...], preferred_element_type=F32).astype(BF16)
        dbuf[slot, pl.ds(first, TILE), :] = jnp.dot(picked.astype(BF16), dout_ref[...], preferred_element_type=F32).astype(BF16)
        return carry

    lax.fori_loop(0, (total(b) + (TILE - 1)) // TILE, tile, 0)

    def send(e, carry):
        n = pl.multiple_of(rows_ref[b, e], ALIGN)
        src = pl.multiple_of(start_ref[b, e], ALIGN)
        dst = pl.multiple_of(off_ref[b, e], ALIGN)

        @pl.when(n > 0)
        def _():
            pltpu.make_async_copy(rbuf.at[slot, pl.ds(src, n), :], r_hbm.at[e, pl.ds(dst, n), :], sem.at[0, slot]).start()
            pltpu.make_async_copy(dbuf.at[slot, pl.ds(src, n), :], d_hbm.at[e, pl.ds(dst, n), :], sem.at[1, slot]).start()
        return carry

    lax.fori_loop(0, n_exp, send, 0)

    @pl.when(step == n_blocks - 1)
    def _():
        @pl.when(n_blocks > 1)
        def _():
            drain(b - 1, 1 - slot)
        drain(b, slot)


def block_rows(top_k, n_local):
    return -(-(BLOCK * top_k + n_local * (ALIGN - 1)) // TILE) * TILE


def dispatch(h_tok, dout_tok, dest, gate, segs, base, held, n_local, max_rows):
    tok_count, d_model = h_tok.shape
    top_k = dest.shape[1]
    n_blocks = tok_count // BLOCK
    buf_rows = block_rows(top_k, n_local)
    tok_spec = pl.BlockSpec((BLOCK, d_model), lambda b, *_: (b, 0))
    map_spec = pl.BlockSpec((1, top_k, BLOCK), lambda b, *_: (b + base, 0, 0))
    rows_shape = jax.ShapeDtypeStruct((n_local, max_rows, d_model), BF16)
    hbm = pl.BlockSpec(memory_space=pl.ANY)
    return pl.pallas_call(
        functools.partial(dispatch_kernel, base=base),
        grid_spec=pltpu.PrefetchScalarGridSpec(
            num_scalar_prefetch=3,
            grid=(n_blocks,),
            in_specs=[tok_spec, tok_spec, map_spec, map_spec] + [hbm] * len(held),
            out_specs=[hbm, hbm],
            scratch_shapes=[
                pltpu.VMEM((BLOCK, d_model), BF16),
                pltpu.VMEM((2, buf_rows, d_model), BF16),
                pltpu.VMEM((2, buf_rows, d_model), BF16),
                pltpu.SemaphoreType.DMA((2, 2)),
            ],
        ),
        out_shape=[rows_shape, rows_shape],
        input_output_aliases={7: 0, 8: 1} if held else {},
        compiler_params=pltpu.CompilerParams(dimension_semantics=('arbitrary',), vmem_limit_bytes=60 * 2 ** 20),
        cost_estimate=pl.CostEstimate(flops=40 * 10 ** 9, bytes_accessed=90 * 10 ** 6, transcendentals=0),
        name='dispatch',
    )(*segs, h_tok, dout_tok, dest, gate, *held)


def expert_kernel(count_ref, r_hbm, d_hbm, w_ref, y_hbm, dr_hbm, dw_ref, rbuf, dbuf, ybuf, drbuf, done, in_sem, out_sem, *, expert_of):
    step = pl.program_id(0)
    n_steps = pl.num_programs(0)
    expert = expert_of(step)
    n_rows = count_ref[expert]
    n_tiles = jnp.maximum((n_rows + (TILE - 1)) // TILE, 1)
    half = w_ref.shape[-1]

    def loads(who, i, slot):
        rows = pl.ds(pl.multiple_of(i * TILE, TILE), TILE)
        return (pltpu.make_async_copy(r_hbm.at[who, rows, :], rbuf.at[slot], in_sem.at[0, slot]),
                pltpu.make_async_copy(d_hbm.at[who, rows, :], dbuf.at[slot], in_sem.at[1, slot]))

    def stores(who, i, slot):
        rows = pl.ds(pl.multiple_of(i * TILE, TILE), TILE)
        return (pltpu.make_async_copy(ybuf.at[slot], y_hbm.at[who, rows, :], out_sem.at[0, slot]),
                pltpu.make_async_copy(drbuf.at[slot], dr_hbm.at[who, rows, :], out_sem.at[1, slot]))

    @pl.when(step == 0)
    def _():
        done[0] = 0
        for copy in loads(expert, 0, 0):
            copy.start()

    before = done[0]
    dw_ref[...] = jnp.zeros(dw_ref.shape, F32)

    def tile(i, carry):
        slot = lax.rem(before + i, 2)
        first = i * TILE

        @pl.when(i + 1 < n_tiles)
        def _():
            for copy in loads(expert, i + 1, 1 - slot):
                copy.start()

        @pl.when((i + 1 == n_tiles) & (step + 1 < n_steps))
        def _():
            for copy in loads(expert_of(step + 1), 0, 1 - slot):
                copy.start()

        for copy in loads(expert, i, slot):
            copy.wait()

        @pl.when(before + i >= 2)
        def _():
            for copy in stores(expert, i, slot):
                copy.wait()

        valid = lax.broadcasted_iota(jnp.int32, (TILE, 1), 0) + first < n_rows
        r = jnp.where(valid, rbuf[slot], 0)
        dy = jnp.where(valid, dbuf[slot], 0)
        w1 = jnp.concatenate([w_ref[0, 0, 0, 0], w_ref[1, 0, 0, 0]], axis=0)
        w3 = jnp.concatenate([w_ref[0, 0, 1, 0], w_ref[1, 0, 1, 0]], axis=0)
        w2 = jnp.concatenate([w_ref[0, 0, 2, 0], w_ref[1, 0, 2, 0]], axis=1)
        act_a = jnp.dot(r, w1, preferred_element_type=F32)
        act_b = jnp.dot(r, w3, preferred_element_type=F32)
        d_g = nt_dot(dy, w2)
        sig = 1.0 / (1.0 + jnp.exp(-act_a))
        silu = act_a * sig
        g = (silu * act_b).astype(BF16)
        d_up = (d_g * silu).astype(BF16)
        d_gate = (d_g * act_b * sig * (1.0 + act_a * (1.0 - sig))).astype(BF16)
        ybuf[slot] = jnp.dot(g, w2, preferred_element_type=F32).astype(BF16)
        drbuf[slot] = (nt_dot(d_gate, w1) + nt_dot(d_up, w3)).astype(BF16)
        for copy in stores(expert, i, slot):
            copy.start()
        r_lo, r_hi = r[:, :half], r[:, half:]
        dw_ref[0, 0, 0, 0] += tn_dot(r_lo, d_gate)
        dw_ref[1, 0, 0, 0] += tn_dot(r_hi, d_gate)
        dw_ref[0, 0, 1, 0] += tn_dot(r_lo, d_up)
        dw_ref[1, 0, 1, 0] += tn_dot(r_hi, d_up)
        dw_ref[0, 0, 2, 0] += tn_dot(g, dy[:, :half])
        dw_ref[1, 0, 2, 0] += tn_dot(g, dy[:, half:])
        return carry

    lax.fori_loop(0, n_tiles, tile, 0)
    done[0] = before + n_tiles

    @pl.when(step == n_steps - 1)
    def _():
        last = before + n_tiles - 1
        for copy in stores(expert, 0, lax.rem(last, 2)):
            copy.wait()

        @pl.when(last >= 1)
        def _():
            for copy in stores(expert, 0, lax.rem(last + 1, 2)):
                copy.wait()


def experts(rows, d_rows, weights, counts, first, skip, size, local_experts):
    d_model = rows.shape[2]
    n_fsdp, n_side, three, _, half, _ = weights.shape

    def expert_of(g):
        return g // size * local_experts + first + lax.rem(g, size)

    hbm = pl.BlockSpec(memory_space=pl.ANY)
    w_block = (n_fsdp, 1, three, 1, half, half)
    return pl.pallas_call(
        functools.partial(expert_kernel, expert_of=expert_of),
        grid_spec=pltpu.PrefetchScalarGridSpec(
            num_scalar_prefetch=1,
            grid=(n_side * size,),
            in_specs=[hbm, hbm, pl.BlockSpec(w_block, lambda g, *_: (0, g // size, 0, skip + lax.rem(g, size), 0, 0))],
            out_specs=[hbm, hbm, pl.BlockSpec(w_block, lambda g, *_: (0, g // size, 0, lax.rem(g, size), 0, 0))],
            scratch_shapes=[pltpu.VMEM((2, TILE, d_model), BF16)] * 4 + [
                pltpu.SMEM((1,), jnp.int32),
                pltpu.SemaphoreType.DMA((2, 2)),
                pltpu.SemaphoreType.DMA((2, 2)),
            ],
        ),
        out_shape=[
            jax.ShapeDtypeStruct(rows.shape, BF16),
            jax.ShapeDtypeStruct(rows.shape, BF16),
            jax.ShapeDtypeStruct((n_fsdp, n_side, three, size, half, half), F32),
        ],
        input_output_aliases={1: 0, 2: 1},
        compiler_params=pltpu.CompilerParams(dimension_semantics=('arbitrary',), vmem_limit_bytes=56 * 2 ** 20),
        cost_estimate=pl.CostEstimate(flops=55 * 10 ** 9 * size, bytes_accessed=100 * 10 ** 6 * size, transcendentals=0),
        name='experts',
    )(counts, rows, d_rows, weights)


def combine_kernel(start_ref, rows_ref, off_ref, y_hbm, dr_hbm, dest_ref, gate_ref, *refs, base, own):
    ybuf, dbuf, acc_y, acc_d, sem = refs[-5:]
    step = pl.program_id(0)
    n_blocks = pl.num_programs(0)
    b = step + base
    n_exp = rows_ref.shape[1]
    slot = lax.rem(step, 2)

    def total(blk):
        return start_ref[blk, n_exp - 1] + rows_ref[blk, n_exp - 1]

    def fetch(blk, which):
        def one(e, carry):
            n = pl.multiple_of(rows_ref[blk, e], ALIGN)
            dst = pl.multiple_of(start_ref[blk, e], ALIGN)
            src = pl.multiple_of(off_ref[blk, e], ALIGN)

            @pl.when(n > 0)
            def _():
                pltpu.make_async_copy(y_hbm.at[e, pl.ds(src, n), :], ybuf.at[which, pl.ds(dst, n), :], sem.at[0, which]).start()
                pltpu.make_async_copy(dr_hbm.at[e, pl.ds(src, n), :], dbuf.at[which, pl.ds(dst, n), :], sem.at[1, which]).start()
            return carry

        lax.fori_loop(0, n_exp, one, 0)

    @pl.when(step == 0)
    def _():
        ybuf[...] = jnp.zeros(ybuf.shape, BF16)
        dbuf[...] = jnp.zeros(dbuf.shape, BF16)
        fetch(b, 0)

    @pl.when(step + 1 < n_blocks)
    def _():
        fetch(b + 1, 1 - slot)

    n = pl.multiple_of(total(b), ALIGN)

    @pl.when(n > 0)
    def _():
        pltpu.make_async_copy(ybuf.at[slot, pl.ds(0, n), :], ybuf.at[slot, pl.ds(0, n), :], sem.at[0, slot]).wait()
        pltpu.make_async_copy(dbuf.at[slot, pl.ds(0, n), :], dbuf.at[slot, pl.ds(0, n), :], sem.at[1, slot]).wait()

    acc_y[...] = jnp.zeros(acc_y.shape, F32)
    acc_d[...] = jnp.zeros(acc_d.shape, F32)

    def tile(i, carry):
        first = pl.multiple_of(i * TILE, TILE)
        picked = one_hot(dest_ref, gate_ref, first)
        ones = jnp.where(picked > 0, 1.0, 0.0).astype(BF16)
        acc_y[...] += tn_dot(picked.astype(BF16), ybuf[slot, pl.ds(first, TILE), :])
        acc_d[...] += tn_dot(ones, dbuf[slot, pl.ds(first, TILE), :])
        return carry

    lax.fori_loop(0, (n + (TILE - 1)) // TILE, tile, 0)

    if not own:
        out_y, out_d = refs[:2]
        out_y[...] = acc_y[...]
        out_d[...] = acc_d[...]
        return
    more_y, more_d, h_ref, dout_ref, out_ref, dh_ref = refs[:6]
    hf = h_ref[...].astype(F32)
    out_ref[...] = (hf + (acc_y[...] + more_y[...])).astype(BF16)
    d_u = (acc_d[...] + more_d[...]).astype(BF16).astype(F32)
    inv = lax.rsqrt(jnp.mean(hf * hf, axis=-1, keepdims=True) + EPS)
    proj = jnp.mean(d_u * hf, axis=-1, keepdims=True)
    d_norm = (d_u * inv - hf * (inv * inv * inv * proj)).astype(BF16).astype(F32)
    dh_ref[...] = (dout_ref[...].astype(F32) + d_norm).astype(BF16)


def combine(y_rows, dr_rows, dest, gate, segs, base, n_blocks, extra):
    n_local, _, d_model = y_rows.shape
    top_k = dest.shape[1]
    buf_rows = block_rows(top_k, n_local)
    tok_spec = pl.BlockSpec((BLOCK, d_model), lambda b, *_: (b, 0))
    map_spec = pl.BlockSpec((1, top_k, BLOCK), lambda b, *_: (b + base, 0, 0))
    hbm = pl.BlockSpec(memory_space=pl.ANY)
    out = jax.ShapeDtypeStruct((n_blocks * BLOCK, d_model), BF16 if extra else F32)
    return pl.pallas_call(
        functools.partial(combine_kernel, base=base, own=bool(extra)),
        grid_spec=pltpu.PrefetchScalarGridSpec(
            num_scalar_prefetch=3,
            grid=(n_blocks,),
            in_specs=[hbm, hbm, map_spec, map_spec] + [tok_spec] * len(extra),
            out_specs=[tok_spec, tok_spec],
            scratch_shapes=[
                pltpu.VMEM((2, buf_rows, d_model), BF16),
                pltpu.VMEM((2, buf_rows, d_model), BF16),
                pltpu.VMEM((BLOCK, d_model), F32),
                pltpu.VMEM((BLOCK, d_model), F32),
                pltpu.SemaphoreType.DMA((2, 2)),
            ],
        ),
        out_shape=[out, out],
        compiler_params=pltpu.CompilerParams(dimension_semantics=('arbitrary',), vmem_limit_bytes=60 * 2 ** 20),
        cost_estimate=pl.CostEstimate(flops=45 * 10 ** 9, bytes_accessed=120 * 10 ** 6, transcendentals=0),
        name='combine',
    )(*segs, y_rows, dr_rows, dest, gate, *extra)


def place_kernel(part_ref, *refs):
    for k, out_ref in enumerate(refs[-3:]):
        out_ref[...] = part_ref[k]


def place(part, held, first, n_total):
    three, per_chunk, rows, cols = part.shape
    hbm = pl.BlockSpec(memory_space=pl.ANY)
    return pl.pallas_call(
        place_kernel,
        grid=(per_chunk,),
        in_specs=[pl.BlockSpec((three, 1, rows, cols), lambda i: (0, i, 0, 0))] + [hbm] * len(held),
        out_specs=[pl.BlockSpec((1, rows, cols), lambda i: (first + i, 0, 0))] * three,
        out_shape=[jax.ShapeDtypeStruct((n_total, rows, cols), F32)] * three,
        input_output_aliases={1: 0, 2: 1, 3: 2} if held else {},
        compiler_params=pltpu.CompilerParams(dimension_semantics=('arbitrary',)),
        cost_estimate=pl.CostEstimate(flops=3 * 10 ** 8, bytes_accessed=12 * 10 ** 6, transcendentals=0),
        name='place',
    )(part, *held)


GATHERS = (2, 6)
SCATTERS = (2, 3, 3)
CORES = 2


def solution(mesh):
    ep_size, fsdp_size = mesh.shape['ep'], mesh.shape['fsdp']
    tok_spec = P(('data', 'fsdp', 'ep'))
    in_specs = (tok_spec, P('fsdp'), P(None, None, 'fsdp'), P('ep', 'fsdp'), P('ep', 'fsdp'), P('ep', None, 'fsdp'), tok_spec, tok_spec, tok_spec, tok_spec)
    out_specs = (tok_spec, tok_spec, P(('data', 'ep'), 'fsdp'), P(('data', 'ep'), 'fsdp'), P(('data', 'ep'), None, 'fsdp'))

    def device_fn(tokens, w_qkv, w_out, w_gate, w_up, w_down, expert_idx, expert_slot, gate_wts, d_out):
        n_seq, seq_len, d_model = tokens.shape
        tok_count = n_seq * seq_len
        top_k = expert_idx.shape[2]
        local_experts, half, _ = w_gate.shape
        num_experts = local_experts * ep_size
        n_side = ep_size // CORES
        n_local = local_experts * n_side
        n_blocks = tok_count // BLOCK
        capacity = capacity_of(tok_count, top_k, num_experts)
        max_rows = -(-(CORES * (capacity + n_blocks * (ALIGN - 1))) // TILE) * TILE
        ep = lax.axis_index('ep')
        groups = [[c + CORES * i for i in range(fsdp_size * n_side)] for c in range(CORES)]

        def swap(values):
            return lax.ppermute(values, 'ep', [(i, i ^ 1) for i in range(ep_size)])

        n_heads, head_dim, _ = w_out.shape
        qkv_rows = w_qkv.transpose(1, 2, 3, 0).reshape(-1, half)
        qkv_rows = lax.dynamic_slice_in_dim(qkv_rows, ep * (3 * d_model // ep_size), 3 * d_model // ep_size, axis=0)
        out_rows = lax.dynamic_slice_in_dim(w_out.reshape(-1, half), ep * (d_model // ep_size), d_model // ep_size, axis=0)
        attn_w = lax.all_gather(jnp.concatenate([qkv_rows, out_rows], axis=0), ('fsdp', 'ep'), axis=0, tiled=False)
        attn_w = attn_w.reshape(fsdp_size, ep_size, -1, half)
        weights, held_from, first = [], [], 0
        for size in GATHERS:
            part = slice(first, first + size)
            mine = jnp.stack([w_gate[part], w_up[part], w_down[part]], axis=0)
            full = lax.all_gather(mine, ('fsdp', 'ep'), axis=0, tiled=False, axis_index_groups=groups)
            weights.append(full.reshape(fsdp_size, n_side, *mine.shape))
            held_from.append(first)
            first += size

        dout_tok = d_out.reshape(tok_count, d_model)
        dout_other = swap(dout_tok)
        kept_ids = jnp.where(expert_slot >= 0, expert_idx, -1).transpose(0, 2, 1)
        all_ids = jnp.concatenate([kept_ids, swap(kept_ids)], axis=0)
        owner = all_ids // local_experts
        mine_too = (all_ids >= 0) & (lax.rem(owner, CORES) == lax.rem(ep, CORES))
        local_ids = jnp.where(mine_too, owner // CORES * local_experts + lax.rem(all_ids, local_experts), -1)
        dest, segs = route(local_ids, n_local)
        counts = jnp.sum(segs[1], axis=0)
        gate = gate_wts.transpose(0, 2, 1)
        gate = jnp.concatenate([gate, swap(gate)], axis=0).astype(F32)
        gate = gate.reshape(2 * n_seq, top_k, seq_len // BLOCK, BLOCK).transpose(0, 2, 1, 3).reshape(2 * n_blocks, top_k, BLOCK)

        tokens, dest, segs, counts, gate = lax.optimization_barrier((tokens, dest, segs, counts, gate))
        h_seq, qkv = attention(tokens, attn_w, head_dim)
        h_tok = h_seq.reshape(tok_count, d_model)
        h_other = swap(h_tok)
        held = dispatch(h_tok, dout_tok, dest, gate, segs, 0, [], n_local, max_rows)
        rows, d_rows = dispatch(h_other, dout_other, dest, gate, segs, n_blocks, held, n_local, max_rows)
        d_ws, first = [], 0
        for size in SCATTERS:
            which = max(n for n, start in enumerate(held_from) if start <= first)
            rows, d_rows, d_w = experts(rows, d_rows, weights[which], counts, first, first - held_from[which], size, local_experts)
            d_w = d_w.reshape(fsdp_size * n_side, 3, size, half, half)
            d_w = lax.psum_scatter(d_w, ('fsdp', 'ep'), scatter_dimension=0, tiled=False, axis_index_groups=groups)
            d_ws = place(d_w, d_ws, first, local_experts)
            first += size
        sums = combine(rows, d_rows, dest, gate, segs, n_blocks, n_blocks, [])
        more = [swap(value) for value in sums]
        layer_out, d_h = combine(rows, d_rows, dest, gate, segs, 0, n_blocks, [*more, h_tok, dout_tok])
        d_tokens = attention_grad(d_h.reshape(n_seq, seq_len, d_model), tokens, qkv, attn_w, head_dim)
        return layer_out.reshape(n_seq, seq_len, d_model), d_tokens, *d_ws

    return jax.shard_map(device_fn, mesh=mesh, in_specs=in_specs, out_specs=out_specs, check_vma=False)
```

```python
import functools
import math

import jax
import jax.numpy as jnp
from jax import lax
from jax.experimental import pallas as pl
from jax.experimental.pallas import tpu as pltpu
from jax.sharding import PartitionSpec as P


F32 = jnp.float32
BF16 = jnp.bfloat16
BLOCK = 256
TILE = 256
ALIGN = 16
LANES = 128
LOG2E = math.log2(math.e)
EPS = 1e-6
VMEM_BYTES = 60 * 2 ** 20


def settings(gflop, mbytes):
    return {
        'compiler_params': pltpu.CompilerParams(dimension_semantics=('arbitrary',), vmem_limit_bytes=VMEM_BYTES),
        'cost_estimate': pl.CostEstimate(flops=gflop * 10 ** 9, bytes_accessed=mbytes * 10 ** 6, transcendentals=0),
    }


def nt_dot(lhs, rhs):
    return lax.dot_general(lhs, rhs, (((1,), (1,)), ((), ())), preferred_element_type=F32)


def tn_dot(lhs, rhs):
    return lax.dot_general(lhs, rhs, (((0,), (0,)), ((), ())), preferred_element_type=F32)


def lanes_of(head, values):
    lane = lax.broadcasted_iota(jnp.int32, values.shape, 1)
    return jnp.where((lane >= LANES // 2) == bool(head), values, jnp.zeros_like(values))


def attention_kernel(x_ref, w_ref, h_ref, qkv_ref, ctx, *, head_dim):
    seq_len, d_model = x_ref.shape[1:]
    n_fsdp, n_ep, rows, half = w_ref.shape
    n_qkv = rows * 3 // 4
    x = x_ref[0].astype(F32)
    normed = (x * lax.rsqrt(jnp.mean(x * x, axis=-1, keepdims=True) + EPS)).astype(BF16)
    for p in range(n_ep):
        part = nt_dot(normed[:, :half], w_ref[0, p, :n_qkv]) + nt_dot(normed[:, half:], w_ref[1, p, :n_qkv])
        qkv_ref[0, :, p * n_qkv:(p + 1) * n_qkv] = part.astype(BF16)
    scale = head_dim ** -0.5 * LOG2E

    def pair(i, carry):
        q2, k2, v2 = (qkv_ref[0, :, pl.ds(pl.multiple_of(t * d_model + i * LANES, LANES), LANES)] for t in range(3))
        for first in range(0, seq_len, BLOCK):
            end = first + BLOCK
            keys, vals = k2[:end], v2[:end]
            causal = lax.broadcasted_iota(jnp.int32, (BLOCK, end), 0) + first >= lax.broadcasted_iota(jnp.int32, (BLOCK, end), 1)
            both = []
            for head in range(2):
                scores = nt_dot(lanes_of(head, q2[first:end]), keys) * scale
                scores = jnp.where(causal, scores, -1e30)
                probs = jnp.exp2(scores - jnp.max(scores, axis=-1, keepdims=True))
                probs = (probs * (1.0 / jnp.sum(probs, axis=-1, keepdims=True))).astype(BF16)
                both.append(jnp.dot(probs, vals, preferred_element_type=F32))
            lane = lax.broadcasted_iota(jnp.int32, (BLOCK, LANES), 1)
            ctx[first:end, pl.ds(pl.multiple_of(i * LANES, LANES), LANES)] = jnp.where(lane < LANES // 2, both[0], both[1]).astype(BF16)
        return carry

    lax.fori_loop(0, d_model // LANES, pair, 0)
    for f in range(n_fsdp):
        w_out = jnp.concatenate([w_ref[f, p, n_qkv:] for p in range(n_ep)], axis=0)
        cols = slice(f * half, (f + 1) * half)
        h_ref[0, :, cols] = (x_ref[0, :, cols].astype(F32) + jnp.dot(ctx[...], w_out, preferred_element_type=F32)).astype(BF16)


def attention(tokens, weights, head_dim):
    n_seq, seq_len, d_model = tokens.shape
    seq_spec = pl.BlockSpec((1, seq_len, d_model), lambda s: (s, 0, 0))
    qkv_spec = pl.BlockSpec((1, seq_len, 3 * d_model), lambda s: (s, 0, 0))
    w_spec = pl.BlockSpec(weights.shape, lambda s: (0, 0, 0, 0))
    return pl.pallas_call(
        functools.partial(attention_kernel, head_dim=head_dim),
        grid=(n_seq,),
        in_specs=[seq_spec, w_spec],
        out_specs=[seq_spec, qkv_spec],
        out_shape=[jax.ShapeDtypeStruct(tokens.shape, BF16), jax.ShapeDtypeStruct((n_seq, seq_len, 3 * d_model), BF16)],
        scratch_shapes=[pltpu.VMEM((seq_len, d_model), BF16)],
        name='attention',
        **settings(90, 60),
    )(tokens, weights)


def attention_grad_kernel(dh_ref, x_ref, qkv_ref, w_ref, dx_ref, dctx, dqkv, *, head_dim):
    seq_len, d_model = x_ref.shape[1:]
    n_fsdp, n_ep, rows, half = w_ref.shape
    n_qkv = rows * 3 // 4
    n_out = rows - n_qkv
    dh = dh_ref[0]
    for p in range(n_ep):
        part = nt_dot(dh[:, :half], w_ref[0, p, n_qkv:]) + nt_dot(dh[:, half:], w_ref[1, p, n_qkv:])
        dctx[:, p * n_out:(p + 1) * n_out] = part.astype(BF16)
    scale = head_dim ** -0.5

    def pair(i, carry):
        col = pl.multiple_of(i * LANES, LANES)
        q2, k2, v2 = (qkv_ref[0, :, pl.ds(pl.multiple_of(t * d_model + i * LANES, LANES), LANES)] for t in range(3))
        d2 = dctx[:, pl.ds(col, LANES)]
        dk = [jnp.zeros((BLOCK, LANES), F32)] * (seq_len // BLOCK)
        dv = list(dk)
        for first in range(0, seq_len, BLOCK):
            end = first + BLOCK
            keys, vals = k2[:end], v2[:end]
            causal = lax.broadcasted_iota(jnp.int32, (end, BLOCK), 1) + first >= lax.broadcasted_iota(jnp.int32, (end, BLOCK), 0)
            dq = jnp.zeros((BLOCK, LANES), F32)
            for head in range(2):
                q, d = lanes_of(head, q2[first:end]), lanes_of(head, d2[first:end])
                scores = jnp.where(causal, nt_dot(keys, q) * (scale * LOG2E), -1e30)
                probs = jnp.exp2(scores - jnp.max(scores, axis=0, keepdims=True))
                probs = probs * (1.0 / jnp.sum(probs, axis=0, keepdims=True))
                d_probs = nt_dot(vals, d)
                d_scores = probs * (d_probs - jnp.sum(probs * d_probs, axis=0, keepdims=True))
                d_scores = (d_scores * scale).astype(BF16)
                dv_part = jnp.dot(probs.astype(BF16), d, preferred_element_type=F32)
                dk_part = jnp.dot(d_scores, q, preferred_element_type=F32)
                dq = dq + tn_dot(d_scores, lanes_of(head, keys))
                for n in range(end // BLOCK):
                    dk[n] = dk[n] + dk_part[n * BLOCK:(n + 1) * BLOCK]
                    dv[n] = dv[n] + dv_part[n * BLOCK:(n + 1) * BLOCK]
            dqkv[first:end, pl.ds(col, LANES)] = dq.astype(BF16)
        for n in range(seq_len // BLOCK):
            dqkv[n * BLOCK:(n + 1) * BLOCK, pl.ds(pl.multiple_of(d_model + i * LANES, LANES), LANES)] = dk[n].astype(BF16)
            dqkv[n * BLOCK:(n + 1) * BLOCK, pl.ds(pl.multiple_of(2 * d_model + i * LANES, LANES), LANES)] = dv[n].astype(BF16)
        return carry

    lax.fori_loop(0, d_model // LANES, pair, 0)
    x = x_ref[0].astype(F32)
    d_normed = []
    for f in range(n_fsdp):
        w_qkv = jnp.concatenate([w_ref[f, p, :n_qkv] for p in range(n_ep)], axis=0)
        d_normed.append(jnp.dot(dqkv[...], w_qkv, preferred_element_type=F32).astype(BF16))
    d_normed = jnp.concatenate(d_normed, axis=1).astype(F32)
    inv = lax.rsqrt(jnp.mean(x * x, axis=-1, keepdims=True) + EPS)
    proj = jnp.mean(d_normed * x, axis=-1, keepdims=True)
    d_x = (d_normed * inv - x * (inv * inv * inv * proj)).astype(BF16).astype(F32)
    dx_ref[0] = (dh_ref[0].astype(F32) + d_x).astype(BF16)


def attention_grad(d_h, tokens, qkv, weights, head_dim):
    n_seq, seq_len, d_model = tokens.shape
    seq_spec = pl.BlockSpec((1, seq_len, d_model), lambda s: (s, 0, 0))
    qkv_spec = pl.BlockSpec((1, seq_len, 3 * d_model), lambda s: (s, 0, 0))
    w_spec = pl.BlockSpec(weights.shape, lambda s: (0, 0, 0, 0))
    return pl.pallas_call(
        functools.partial(attention_grad_kernel, head_dim=head_dim),
        grid=(n_seq,),
        in_specs=[seq_spec, seq_spec, qkv_spec, w_spec],
        out_specs=seq_spec,
        out_shape=jax.ShapeDtypeStruct(tokens.shape, BF16),
        scratch_shapes=[pltpu.VMEM((seq_len, d_model), BF16), pltpu.VMEM((seq_len, 3 * d_model), BF16)],
        name='attention_grad',
        **settings(150, 70),
    )(d_h, tokens, qkv, weights)


def capacity_of(tok_count, top_k, num_experts):
    return max(8, (5 * tok_count * top_k // (4 * num_experts) + 7) // 8 * 8)


def route_kernel(loc_ref, dest_ref, start_ref, rows_ref, off_ref, total, *, n_local):
    top_k = loc_ref.shape[1]
    ids = lax.broadcasted_iota(jnp.int32, (n_local, BLOCK), 0)
    upper = (lax.broadcasted_iota(jnp.int32, (BLOCK, BLOCK), 0) <= lax.broadcasted_iota(jnp.int32, (BLOCK, BLOCK), 1)).astype(F32).astype(BF16)
    before = (lax.broadcasted_iota(jnp.int32, (n_local, n_local), 0) > lax.broadcasted_iota(jnp.int32, (n_local, n_local), 1)).astype(F32).astype(BF16)

    @pl.when(pl.program_id(0) == 0)
    def _():
        total[...] = jnp.zeros(total.shape, jnp.int32)

    so_far = total[...]
    for s in range(loc_ref.shape[0]):
        for p in range(loc_ref.shape[2] // BLOCK):
            q = s * (loc_ref.shape[2] // BLOCK) + p
            loc = loc_ref[s, :, p * BLOCK:(p + 1) * BLOCK]
            member = jnp.zeros((n_local, BLOCK), F32)
            for j in range(top_k):
                member = jnp.where(loc[j:j + 1] == ids, 1.0, member)
            count = jnp.dot(member.astype(BF16), upper, preferred_element_type=F32)
            units = (count[:, BLOCK - 1:].astype(jnp.int32) + (ALIGN - 1)) // ALIGN
            units = jnp.broadcast_to(units, (n_local, LANES))
            start = jnp.dot(before, units.astype(F32).astype(BF16), preferred_element_type=F32).astype(jnp.int32) * ALIGN
            place = start[:, :1] + count.astype(jnp.int32) - 1
            for j in range(top_k):
                row = jnp.sum(jnp.where(loc[j:j + 1] == ids, place, 0), axis=0, keepdims=True)
                dest_ref[q, j:j + 1, :] = jnp.where(loc[j:j + 1] >= 0, row, -1)
            start_ref[q] = start
            rows_ref[q] = units * ALIGN
            off_ref[q] = so_far
            so_far = so_far + units * ALIGN
    total[...] = so_far


def route(local_ids, n_local):
    n_seq, top_k, seq_len = local_ids.shape
    per_seq = seq_len // BLOCK
    step = 2 if n_seq % 2 == 0 else 1
    n_blocks = n_seq * per_seq
    seg = jax.ShapeDtypeStruct((n_blocks, n_local, LANES), jnp.int32)
    seg_spec = pl.BlockSpec((step * per_seq, n_local, LANES), lambda s: (s, 0, 0))
    dest, *segs = pl.pallas_call(
        functools.partial(route_kernel, n_local=n_local),
        grid=(n_seq // step,),
        in_specs=[pl.BlockSpec((step, top_k, seq_len), lambda s: (s, 0, 0))],
        out_specs=[pl.BlockSpec((step * per_seq, top_k, BLOCK), lambda s: (s, 0, 0)), seg_spec, seg_spec, seg_spec],
        out_shape=[jax.ShapeDtypeStruct((n_blocks, top_k, BLOCK), jnp.int32), seg, seg, seg],
        scratch_shapes=[pltpu.VMEM((n_local, LANES), jnp.int32)],
        name='route',
        **settings(1, 3),
    )(local_ids)
    return dest, [part[:, :, 0] for part in segs]


def one_hot(dest_ref, gate_ref, first_row):
    rows = lax.broadcasted_iota(jnp.int32, (TILE, BLOCK), 0) + first_row
    dest = dest_ref[0]
    gate = gate_ref[0]
    picked = jnp.zeros((TILE, BLOCK), F32)
    for j in range(dest.shape[0]):
        picked = jnp.where(rows == dest[j:j + 1], gate[j:j + 1], picked)
    return picked


def dispatch_kernel(start_ref, rows_ref, off_ref, h_ref, dout_ref, dest_ref, gate_ref, *refs, base):
    r_hbm, d_hbm, u_s, rbuf, dbuf, sem = refs[-6:]
    step = pl.program_id(0)
    n_blocks = pl.num_programs(0)
    b = step + base
    n_exp = rows_ref.shape[1]
    slot = lax.rem(b, 2)

    def total(blk):
        return start_ref[blk, n_exp - 1] + rows_ref[blk, n_exp - 1]

    def drain(blk, which):
        n = pl.multiple_of(total(blk), ALIGN)

        @pl.when(n > 0)
        def _():
            pltpu.make_async_copy(rbuf.at[which, pl.ds(0, n), :], rbuf.at[which, pl.ds(0, n), :], sem.at[0, which]).wait()
            pltpu.make_async_copy(dbuf.at[which, pl.ds(0, n), :], dbuf.at[which, pl.ds(0, n), :], sem.at[1, which]).wait()

    @pl.when(step >= 2)
    def _():
        drain(b - 2, slot)

    hf = h_ref[...].astype(F32)
    u_s[...] = (hf * lax.rsqrt(jnp.mean(hf * hf, axis=-1, keepdims=True) + EPS)).astype(BF16)

    def tile(i, carry):
        first = pl.multiple_of(i * TILE, TILE)
        picked = one_hot(dest_ref, gate_ref, first)
        ones = jnp.where(picked > 0, 1.0, 0.0).astype(BF16)
        rbuf[slot, pl.ds(first, TILE), :] = jnp.dot(ones, u_s[...], preferred_element_type=F32).astype(BF16)
        dbuf[slot, pl.ds(first, TILE), :] = jnp.dot(picked.astype(BF16), dout_ref[...], preferred_element_type=F32).astype(BF16)
        return carry

    lax.fori_loop(0, (total(b) + (TILE - 1)) // TILE, tile, 0)

    def send(e, carry):
        n = pl.multiple_of(rows_ref[b, e], ALIGN)
        src = pl.multiple_of(start_ref[b, e], ALIGN)
        dst = pl.multiple_of(off_ref[b, e], ALIGN)

        @pl.when(n > 0)
        def _():
            pltpu.make_async_copy(rbuf.at[slot, pl.ds(src, n), :], r_hbm.at[e, pl.ds(dst, n), :], sem.at[0, slot]).start()
            pltpu.make_async_copy(dbuf.at[slot, pl.ds(src, n), :], d_hbm.at[e, pl.ds(dst, n), :], sem.at[1, slot]).start()

        return carry

    lax.fori_loop(0, n_exp, send, 0)

    @pl.when(step == n_blocks - 1)
    def _():
        @pl.when(n_blocks > 1)
        def _():
            drain(b - 1, 1 - slot)

        drain(b, slot)


def block_rows(top_k, n_local):
    return -(-(BLOCK * top_k + n_local * (ALIGN - 1)) // TILE) * TILE


def dispatch(h_tok, dout_tok, dest, gate, segs, base, held, n_local, max_rows):
    tok_count, d_model = h_tok.shape
    top_k = dest.shape[1]
    n_blocks = tok_count // BLOCK
    buf_rows = block_rows(top_k, n_local)
    tok_spec = pl.BlockSpec((BLOCK, d_model), lambda b, *_: (b, 0))
    map_spec = pl.BlockSpec((1, top_k, BLOCK), lambda b, *_: (b + base, 0, 0))
    rows_shape = jax.ShapeDtypeStruct((n_local, max_rows, d_model), BF16)
    hbm = pl.BlockSpec(memory_space=pl.ANY)
    return pl.pallas_call(
        functools.partial(dispatch_kernel, base=base),
        grid_spec=pltpu.PrefetchScalarGridSpec(
            num_scalar_prefetch=3,
            grid=(n_blocks,),
            in_specs=[tok_spec, tok_spec, map_spec, map_spec] + [hbm] * len(held),
            out_specs=[hbm, hbm],
            scratch_shapes=[
                pltpu.VMEM((BLOCK, d_model), BF16),
                pltpu.VMEM((2, buf_rows, d_model), BF16),
                pltpu.VMEM((2, buf_rows, d_model), BF16),
                pltpu.SemaphoreType.DMA((2, 2)),
            ],
        ),
        out_shape=[rows_shape, rows_shape],
        input_output_aliases={7: 0, 8: 1} if held else {},
        name='dispatch',
        **settings(40, 90),
    )(*segs, h_tok, dout_tok, dest, gate, *held)


def expert_kernel(count_ref, flip_ref, r_hbm, d_hbm, w_lo, w_hi, y_hbm, dr_hbm, dw_ref, rbuf, dbuf, ybuf, drbuf, done, in_sem, out_sem, *, expert_of):
    step = pl.program_id(0)
    n_steps = pl.num_programs(0)
    expert = expert_of(step)
    n_rows = count_ref[expert]
    n_tiles = jnp.maximum((n_rows + (TILE - 1)) // TILE, 1)
    half = dw_ref.shape[-1]

    def copies(who, i, slot, load):
        rows = pl.ds(pl.multiple_of(i * TILE, TILE), TILE)
        pairs = ((r_hbm, rbuf), (d_hbm, dbuf)) if load else ((ybuf, y_hbm), (drbuf, dr_hbm))
        for k, (src, dst) in enumerate(pairs):
            src = src.at[who, rows, :] if load else src.at[slot]
            dst = dst.at[slot] if load else dst.at[who, rows, :]
            yield pltpu.make_async_copy(src, dst, (in_sem if load else out_sem).at[k, slot])

    def start(*args):
        for copy in copies(*args):
            copy.start()

    def wait(*args):
        for copy in copies(*args):
            copy.wait()

    @pl.when(step == 0)
    def _():
        done[0] = 0
        start(expert, 0, 0, True)

    before = done[0]
    dw_ref[...] = jnp.zeros(dw_ref.shape, F32)

    def tile(i, carry):
        slot = lax.rem(before + i, 2)

        @pl.when(i + 1 < n_tiles)
        def _():
            start(expert, i + 1, 1 - slot, True)

        @pl.when((i + 1 == n_tiles) & (step + 1 < n_steps))
        def _():
            start(expert_of(step + 1), 0, 1 - slot, True)

        wait(expert, i, slot, True)

        @pl.when(before + i >= 2)
        def _():
            wait(expert, i, slot, False)

        valid = lax.broadcasted_iota(jnp.int32, (TILE, 1), 0) + i * TILE < n_rows
        r = jnp.where(valid, rbuf[slot], 0)
        dy = jnp.where(valid, dbuf[slot], 0)
        w1, w3, w2 = (jnp.concatenate([w[0, 0, t, 0] for w in (w_lo, w_hi)], axis=t // 2) for t in range(3))
        act_a = jnp.dot(r, w1, preferred_element_type=F32)
        act_b = jnp.dot(r, w3, preferred_element_type=F32)
        d_g = nt_dot(dy, w2)
        sig = 1.0 / (1.0 + jnp.exp(-act_a))
        silu = act_a * sig
        g = (silu * act_b).astype(BF16)
        d_up = (d_g * silu).astype(BF16)
        d_gate = (d_g * act_b * sig * (1.0 + act_a * (1.0 - sig))).astype(BF16)
        ybuf[slot] = jnp.dot(g, w2, preferred_element_type=F32).astype(BF16)
        drbuf[slot] = (nt_dot(d_gate, w1) + nt_dot(d_up, w3)).astype(BF16)
        start(expert, i, slot, False)
        for f in range(2):
            part = slice(f * half, (f + 1) * half)
            to = lax.rem(f + flip_ref[0], 2)
            for t, (lhs, rhs) in enumerate(((r[:, part], d_gate), (r[:, part], d_up), (g, dy[:, part]))):
                dw_ref[to, 0, t, 0] += tn_dot(lhs, rhs)
        return carry

    lax.fori_loop(0, n_tiles, tile, 0)
    done[0] = before + n_tiles

    @pl.when(step == n_steps - 1)
    def _():
        last = before + n_tiles - 1
        wait(expert, 0, lax.rem(last, 2), False)

        @pl.when(last >= 1)
        def _():
            wait(expert, 0, lax.rem(last + 1, 2), False)


def experts(rows, d_rows, weights, counts, flips, first, local_experts):
    d_model = rows.shape[2]
    n_fsdp, n_side, three, size, half, _ = weights.shape

    def expert_of(g):
        return g // size * local_experts + first + lax.rem(g, size)

    def side(g, flip):
        return lax.rem(g // size + flip[1], n_side)

    def w_spec(f):
        return pl.BlockSpec((1, 1, three, 1, half, half), lambda g, _, flip: (lax.rem(f + flip[0], n_fsdp), side(g, flip), 0, lax.rem(g, size), 0, 0))

    hbm = pl.BlockSpec(memory_space=pl.ANY)
    return pl.pallas_call(
        functools.partial(expert_kernel, expert_of=expert_of),
        grid_spec=pltpu.PrefetchScalarGridSpec(
            num_scalar_prefetch=2,
            grid=(n_side * size,),
            in_specs=[hbm, hbm, w_spec(0), w_spec(1)],
            out_specs=[hbm, hbm, pl.BlockSpec((n_fsdp, 1, three, 1, half, half), lambda g, _, flip: (0, side(g, flip), 0, lax.rem(g, size), 0, 0))],
            scratch_shapes=[pltpu.VMEM((2, TILE, d_model), BF16)] * 4 + [pltpu.SMEM((1,), jnp.int32)] + [pltpu.SemaphoreType.DMA((2, 2))] * 2,
        ),
        out_shape=[jax.ShapeDtypeStruct(rows.shape, BF16)] * 2 + [jax.ShapeDtypeStruct(weights.shape, F32)],
        input_output_aliases={2: 0, 3: 1},
        name='experts',
        **settings(56 * size, 100 * size),
    )(counts, flips, rows, d_rows, weights, weights)


def combine_kernel(start_ref, rows_ref, off_ref, y_hbm, dr_hbm, dest_ref, gate_ref, *refs, base, own):
    ybuf, dbuf, acc_y, acc_d, sem = refs[-5:]
    step = pl.program_id(0)
    n_blocks = pl.num_programs(0)
    b = step + base
    n_exp = rows_ref.shape[1]
    slot = lax.rem(step, 2)

    def total(blk):
        return start_ref[blk, n_exp - 1] + rows_ref[blk, n_exp - 1]

    def fetch(blk, which):
        def one(e, carry):
            n = pl.multiple_of(rows_ref[blk, e], ALIGN)
            dst = pl.multiple_of(start_ref[blk, e], ALIGN)
            src = pl.multiple_of(off_ref[blk, e], ALIGN)

            @pl.when(n > 0)
            def _():
                pltpu.make_async_copy(y_hbm.at[e, pl.ds(src, n), :], ybuf.at[which, pl.ds(dst, n), :], sem.at[0, which]).start()
                pltpu.make_async_copy(dr_hbm.at[e, pl.ds(src, n), :], dbuf.at[which, pl.ds(dst, n), :], sem.at[1, which]).start()

            return carry

        lax.fori_loop(0, n_exp, one, 0)

    @pl.when(step == 0)
    def _():
        ybuf[...] = jnp.zeros(ybuf.shape, BF16)
        dbuf[...] = jnp.zeros(dbuf.shape, BF16)
        fetch(b, 0)

    @pl.when(step + 1 < n_blocks)
    def _():
        fetch(b + 1, 1 - slot)

    n = pl.multiple_of(total(b), ALIGN)

    @pl.when(n > 0)
    def _():
        pltpu.make_async_copy(ybuf.at[slot, pl.ds(0, n), :], ybuf.at[slot, pl.ds(0, n), :], sem.at[0, slot]).wait()
        pltpu.make_async_copy(dbuf.at[slot, pl.ds(0, n), :], dbuf.at[slot, pl.ds(0, n), :], sem.at[1, slot]).wait()

    acc_y[...] = jnp.zeros(acc_y.shape, F32)
    acc_d[...] = jnp.zeros(acc_d.shape, F32)

    def tile(i, carry):
        first = pl.multiple_of(i * TILE, TILE)
        picked = one_hot(dest_ref, gate_ref, first)
        ones = jnp.where(picked > 0, 1.0, 0.0).astype(BF16)
        acc_y[...] += tn_dot(picked.astype(BF16), ybuf[slot, pl.ds(first, TILE), :])
        acc_d[...] += tn_dot(ones, dbuf[slot, pl.ds(first, TILE), :])
        return carry

    lax.fori_loop(0, (n + (TILE - 1)) // TILE, tile, 0)

    if not own:
        out_y, out_d = refs[:2]
        out_y[...] = acc_y[...]
        out_d[...] = acc_d[...]
        return
    more_y, more_d, h_ref, dout_ref, out_ref, dh_ref = refs[:6]
    hf = h_ref[...].astype(F32)
    out_ref[...] = (hf + (acc_y[...] + more_y[...])).astype(BF16)
    d_u = (acc_d[...] + more_d[...]).astype(BF16).astype(F32)
    inv = lax.rsqrt(jnp.mean(hf * hf, axis=-1, keepdims=True) + EPS)
    proj = jnp.mean(d_u * hf, axis=-1, keepdims=True)
    d_norm = (d_u * inv - hf * (inv * inv * inv * proj)).astype(BF16).astype(F32)
    dh_ref[...] = (dout_ref[...].astype(F32) + d_norm).astype(BF16)


def combine(y_rows, dr_rows, dest, gate, segs, base, n_blocks, extra):
    n_local, _, d_model = y_rows.shape
    top_k = dest.shape[1]
    buf_rows = block_rows(top_k, n_local)
    tok_spec = pl.BlockSpec((BLOCK, d_model), lambda b, *_: (b, 0))
    map_spec = pl.BlockSpec((1, top_k, BLOCK), lambda b, *_: (b + base, 0, 0))
    hbm = pl.BlockSpec(memory_space=pl.ANY)
    out = jax.ShapeDtypeStruct((n_blocks * BLOCK, d_model), BF16 if extra else F32)
    return pl.pallas_call(
        functools.partial(combine_kernel, base=base, own=bool(extra)),
        grid_spec=pltpu.PrefetchScalarGridSpec(
            num_scalar_prefetch=3,
            grid=(n_blocks,),
            in_specs=[hbm, hbm, map_spec, map_spec] + [tok_spec] * len(extra),
            out_specs=[tok_spec, tok_spec],
            scratch_shapes=[
                pltpu.VMEM((2, buf_rows, d_model), BF16),
                pltpu.VMEM((2, buf_rows, d_model), BF16),
                pltpu.VMEM((BLOCK, d_model), F32),
                pltpu.VMEM((BLOCK, d_model), F32),
                pltpu.SemaphoreType.DMA((2, 2)),
            ],
        ),
        out_shape=[out, out],
        name='combine',
        **settings(45, 120),
    )(*segs, y_rows, dr_rows, dest, gate, *extra)


def place_kernel(*refs, n_parts):
    for k, out_ref in enumerate(refs[-3:]):
        value = refs[0][k]
        for part_ref in refs[1:n_parts]:
            value = value + part_ref[k]
        out_ref[...] = value


def place(parts, held, first, n_total):
    three, size, rows, cols = parts[0].shape
    hbm = pl.BlockSpec(memory_space=pl.ANY)
    return pl.pallas_call(
        functools.partial(place_kernel, n_parts=len(parts)),
        grid=(size,),
        in_specs=[pl.BlockSpec((three, 1, rows, cols), lambda i: (0, i, 0, 0))] * len(parts) + [hbm] * len(held),
        out_specs=[pl.BlockSpec((1, rows, cols), lambda i: (first + i, 0, 0))] * three,
        out_shape=[jax.ShapeDtypeStruct((n_total, rows, cols), F32)] * three,
        input_output_aliases={len(parts) + k: k for k in range(len(held))},
        name='place',
        **settings(1, 12),
    )(*parts, *held)


CHUNKS = (3, 3)
CORES = 2


def solution(mesh):
    ep_size, fsdp_size = mesh.shape['ep'], mesh.shape['fsdp']
    tok_spec = P(('data', 'fsdp', 'ep'))
    in_specs = (tok_spec, P('fsdp'), P(None, None, 'fsdp'), P('ep', 'fsdp'), P('ep', 'fsdp'), P('ep', None, 'fsdp'), tok_spec, tok_spec, tok_spec, tok_spec)
    out_specs = (tok_spec, tok_spec, P(('data', 'ep'), 'fsdp'), P(('data', 'ep'), 'fsdp'), P(('data', 'ep'), None, 'fsdp'))

    def device_fn(tokens, w_qkv, w_out, w_gate, w_up, w_down, expert_idx, expert_slot, gate_wts, d_out):
        n_seq, seq_len, d_model = tokens.shape
        tok_count = n_seq * seq_len
        top_k = expert_idx.shape[2]
        local_experts, half, _ = w_gate.shape
        num_experts = local_experts * ep_size
        n_side = ep_size // CORES
        n_local = local_experts * n_side
        n_blocks = tok_count // BLOCK
        capacity = capacity_of(tok_count, top_k, num_experts)
        max_rows = -(-(CORES * (capacity + n_blocks * (ALIGN - 1))) // TILE) * TILE
        ep = lax.axis_index('ep')
        groups = [[c + CORES * i for i in range(fsdp_size * n_side)] for c in range(CORES)]

        fsdp, side = lax.axis_index('fsdp'), ep // CORES
        flips = jnp.stack([fsdp, side]).astype(jnp.int32)

        def swap(values):
            return lax.ppermute(values, 'ep', [(i, i ^ 1) for i in range(ep_size)])

        def swap_x(values):
            return lax.ppermute(values, 'ep', [(i, i ^ CORES) for i in range(ep_size)])

        def swap_y(values):
            return lax.ppermute(values, 'fsdp', [(i, i ^ 1) for i in range(fsdp_size)])

        def own_weights(part):
            return jnp.stack([w_gate[part], w_up[part], w_down[part]], axis=0)

        _, head_dim, _ = w_out.shape
        qkv_rows = w_qkv.transpose(1, 2, 3, 0).reshape(-1, half)
        qkv_rows = lax.dynamic_slice_in_dim(qkv_rows, ep * (3 * d_model // ep_size), 3 * d_model // ep_size, axis=0)
        out_rows = lax.dynamic_slice_in_dim(w_out.reshape(-1, half), ep * (d_model // ep_size), d_model // ep_size, axis=0)
        attn_w = lax.all_gather(jnp.concatenate([qkv_rows, out_rows], axis=0), ('fsdp', 'ep'), axis=0, tiled=False)
        attn_w = attn_w.reshape(fsdp_size, ep_size, -1, half)
        weights, first = [], 0
        for size in CHUNKS:
            mine = own_weights(slice(first, first + size))
            full = lax.all_gather(mine, ('fsdp', 'ep'), axis=0, tiled=False, axis_index_groups=groups)
            weights.append(full.reshape(fsdp_size, n_side, *mine.shape))
            first += size
        mid = first + (local_experts - first) // 2
        attn_w, w_a, w_b = lax.optimization_barrier((attn_w, own_weights(slice(first, mid)), own_weights(slice(mid, local_experts))))
        w_ax, w_ay, w_bx, w_by = swap_x(w_a), swap_y(w_a), swap_x(w_b), swap_y(w_b)

        dout_tok = d_out.reshape(tok_count, d_model)
        dout_other = swap(dout_tok)
        kept_ids = jnp.where(expert_slot >= 0, expert_idx, -1).transpose(0, 2, 1)
        all_ids = jnp.concatenate([kept_ids, swap(kept_ids)], axis=0)
        owner = all_ids // local_experts
        mine_too = (all_ids >= 0) & (lax.rem(owner, CORES) == lax.rem(ep, CORES))
        local_ids = jnp.where(mine_too, owner // CORES * local_experts + lax.rem(all_ids, local_experts), -1)
        dest, segs = route(local_ids, n_local)
        counts = jnp.sum(segs[1], axis=0)
        gate = gate_wts.transpose(0, 2, 1)
        gate = jnp.concatenate([gate, swap(gate)], axis=0).astype(F32)
        gate = gate.reshape(2 * n_seq, top_k, seq_len // BLOCK, BLOCK).transpose(0, 2, 1, 3).reshape(2 * n_blocks, top_k, BLOCK)

        tokens, dest, segs, counts, gate = lax.optimization_barrier((tokens, dest, segs, counts, gate))
        h_seq, qkv = attention(tokens, attn_w, head_dim)
        w_axy, w_byx = swap_y(w_ax), swap_x(w_by)
        w_rest = jnp.stack([jnp.concatenate(pair, axis=1) for pair in ((w_a, w_b), (w_ax, w_bx), (w_ay, w_by), (w_axy, w_byx))])
        w_rest = w_rest.reshape(fsdp_size, n_side, *w_rest.shape[1:])
        h_tok = h_seq.reshape(tok_count, d_model)
        h_other = swap(h_tok)
        held = dispatch(h_tok, dout_tok, dest, gate, segs, 0, [], n_local, max_rows)
        rows, d_rows = dispatch(h_other, dout_other, dest, gate, segs, n_blocks, held, n_local, max_rows)
        done, start = [], 0
        for n, size in enumerate(CHUNKS):
            rows, d_rows, d_w = experts(rows, d_rows, weights[n], counts, jnp.zeros_like(flips), start, local_experts)
            d_w = d_w.reshape(fsdp_size * n_side, *d_w.shape[2:])
            d_w = lax.psum_scatter(d_w, ('fsdp', 'ep'), scatter_dimension=0, tiled=False, axis_index_groups=groups)
            done.append(([d_w], start))
            start += size
            if n == 0:
                rows, d_rows, d_rest = experts(rows, d_rows, w_rest, counts, flips, first, local_experts)
                d_a, d_b = d_rest[:, :, :, :mid - first], d_rest[:, :, :, mid - first:]
                more_a, more_b = swap_x(d_a[:, 1]), swap_y(d_b[1])
                d_a, d_b = d_a[:, 0] + more_a, d_b[0] + more_b
                more_a, more_b = swap_y(d_a[1]), swap_x(d_b[1])
                done += [([d_a[0], more_a], first), ([d_b[0], more_b], mid)]
        sums = combine(rows, d_rows, dest, gate, segs, n_blocks, n_blocks, [])
        more = [swap(value) for value in sums]
        layer_out, d_h = combine(rows, d_rows, dest, gate, segs, 0, n_blocks, [*more, h_tok, dout_tok])
        d_tokens = attention_grad(d_h.reshape(n_seq, seq_len, d_model), tokens, qkv, attn_w, head_dim)
        d_ws = []
        for parts, where in done:
            d_ws = place(parts, d_ws, where, local_experts)
        return layer_out.reshape(n_seq, seq_len, d_model), d_tokens, *d_ws

    return jax.shard_map(device_fn, mesh=mesh, in_specs=in_specs, out_specs=out_specs, check_vma=False)
```

```python
import functools
import math

import jax
import jax.numpy as jnp
from jax import lax
from jax.experimental import pallas as pl
from jax.experimental.pallas import tpu as pltpu
from jax.sharding import PartitionSpec as P


F32 = jnp.float32
BF16 = jnp.bfloat16
BLOCK = 256
TILE = 256
ALIGN = 16
LANES = 128
LOG2E = math.log2(math.e)
EPS = 1e-6
VMEM_BYTES = 60 * 2 ** 20


def settings(gflop, mbytes):
    return {
        'compiler_params': pltpu.CompilerParams(dimension_semantics=('arbitrary',), vmem_limit_bytes=VMEM_BYTES),
        'cost_estimate': pl.CostEstimate(flops=gflop * 10 ** 9, bytes_accessed=mbytes * 10 ** 6, transcendentals=0),
    }


def nt_dot(lhs, rhs):
    return lax.dot_general(lhs, rhs, (((1,), (1,)), ((), ())), preferred_element_type=F32)


def tn_dot(lhs, rhs):
    return lax.dot_general(lhs, rhs, (((0,), (0,)), ((), ())), preferred_element_type=F32)


def lanes_of(head, values):
    lane = lax.broadcasted_iota(jnp.int32, values.shape, 1)
    return jnp.where((lane >= LANES // 2) == bool(head), values, jnp.zeros_like(values))


def attention_kernel(x_ref, w_ref, h_ref, qkv_ref, ctx, *, head_dim):
    seq_len, d_model = x_ref.shape[1:]
    n_fsdp, n_ep, rows, half = w_ref.shape
    n_qkv = rows * 3 // 4
    x = x_ref[0].astype(F32)
    normed = (x * lax.rsqrt(jnp.mean(x * x, axis=-1, keepdims=True) + EPS)).astype(BF16)
    for p in range(n_ep):
        part = nt_dot(normed[:, :half], w_ref[0, p, :n_qkv]) + nt_dot(normed[:, half:], w_ref[1, p, :n_qkv])
        qkv_ref[0, :, p * n_qkv:(p + 1) * n_qkv] = part.astype(BF16)
    scale = head_dim ** -0.5 * LOG2E

    def pair(i, carry):
        q2, k2, v2 = (qkv_ref[0, :, pl.ds(pl.multiple_of(t * d_model + i * LANES, LANES), LANES)] for t in range(3))
        for first in range(0, seq_len, BLOCK):
            end = first + BLOCK
            keys, vals = k2[:end], v2[:end]
            causal = lax.broadcasted_iota(jnp.int32, (BLOCK, end), 0) + first >= lax.broadcasted_iota(jnp.int32, (BLOCK, end), 1)
            both = []
            for head in range(2):
                scores = nt_dot(lanes_of(head, q2[first:end]), keys) * scale
                scores = jnp.where(causal, scores, -1e30)
                probs = jnp.exp2(scores - jnp.max(scores, axis=-1, keepdims=True))
                probs = (probs * (1.0 / jnp.sum(probs, axis=-1, keepdims=True))).astype(BF16)
                both.append(jnp.dot(probs, vals, preferred_element_type=F32))
            lane = lax.broadcasted_iota(jnp.int32, (BLOCK, LANES), 1)
            ctx[first:end, pl.ds(pl.multiple_of(i * LANES, LANES), LANES)] = jnp.where(lane < LANES // 2, both[0], both[1]).astype(BF16)
        return carry

    lax.fori_loop(0, d_model // LANES, pair, 0)
    for f in range(n_fsdp):
        w_out = jnp.concatenate([w_ref[f, p, n_qkv:] for p in range(n_ep)], axis=0)
        cols = slice(f * half, (f + 1) * half)
        h_ref[0, :, cols] = (x_ref[0, :, cols].astype(F32) + jnp.dot(ctx[...], w_out, preferred_element_type=F32)).astype(BF16)


def attention(tokens, weights, head_dim):
    n_seq, seq_len, d_model = tokens.shape
    seq_spec = pl.BlockSpec((1, seq_len, d_model), lambda s: (s, 0, 0))
    qkv_spec = pl.BlockSpec((1, seq_len, 3 * d_model), lambda s: (s, 0, 0))
    w_spec = pl.BlockSpec(weights.shape, lambda s: (0, 0, 0, 0))
    return pl.pallas_call(
        functools.partial(attention_kernel, head_dim=head_dim),
        grid=(n_seq,),
        in_specs=[seq_spec, w_spec],
        out_specs=[seq_spec, qkv_spec],
        out_shape=[jax.ShapeDtypeStruct(tokens.shape, BF16), jax.ShapeDtypeStruct((n_seq, seq_len, 3 * d_model), BF16)],
        scratch_shapes=[pltpu.VMEM((seq_len, d_model), BF16)],
        name='attention',
        **settings(90, 60),
    )(tokens, weights)


def attention_grad_kernel(dh_ref, x_ref, qkv_ref, w_ref, dx_ref, dctx, dqkv, *, head_dim):
    seq_len, d_model = x_ref.shape[1:]
    n_fsdp, n_ep, rows, half = w_ref.shape
    n_qkv = rows * 3 // 4
    n_out = rows - n_qkv
    dh = dh_ref[0]
    for p in range(n_ep):
        part = nt_dot(dh[:, :half], w_ref[0, p, n_qkv:]) + nt_dot(dh[:, half:], w_ref[1, p, n_qkv:])
        dctx[:, p * n_out:(p + 1) * n_out] = part.astype(BF16)
    scale = head_dim ** -0.5

    def pair(i, carry):
        col = pl.multiple_of(i * LANES, LANES)
        q2, k2, v2 = (qkv_ref[0, :, pl.ds(pl.multiple_of(t * d_model + i * LANES, LANES), LANES)] for t in range(3))
        d2 = dctx[:, pl.ds(col, LANES)]
        dk = [jnp.zeros((BLOCK, LANES), F32)] * (seq_len // BLOCK)
        dv = list(dk)
        for first in range(0, seq_len, BLOCK):
            end = first + BLOCK
            keys, vals = k2[:end], v2[:end]
            causal = lax.broadcasted_iota(jnp.int32, (end, BLOCK), 1) + first >= lax.broadcasted_iota(jnp.int32, (end, BLOCK), 0)
            dq = jnp.zeros((BLOCK, LANES), F32)
            for head in range(2):
                q, d = lanes_of(head, q2[first:end]), lanes_of(head, d2[first:end])
                scores = jnp.where(causal, nt_dot(keys, q) * (scale * LOG2E), -1e30)
                probs = jnp.exp2(scores - jnp.max(scores, axis=0, keepdims=True))
                probs = probs * (1.0 / jnp.sum(probs, axis=0, keepdims=True))
                d_probs = nt_dot(vals, d)
                d_scores = probs * (d_probs - jnp.sum(probs * d_probs, axis=0, keepdims=True))
                d_scores = (d_scores * scale).astype(BF16)
                dv_part = jnp.dot(probs.astype(BF16), d, preferred_element_type=F32)
                dk_part = jnp.dot(d_scores, q, preferred_element_type=F32)
                dq = dq + tn_dot(d_scores, lanes_of(head, keys))
                for n in range(end // BLOCK):
                    dk[n] = dk[n] + dk_part[n * BLOCK:(n + 1) * BLOCK]
                    dv[n] = dv[n] + dv_part[n * BLOCK:(n + 1) * BLOCK]
            dqkv[first:end, pl.ds(col, LANES)] = dq.astype(BF16)
        for n in range(seq_len // BLOCK):
            dqkv[n * BLOCK:(n + 1) * BLOCK, pl.ds(pl.multiple_of(d_model + i * LANES, LANES), LANES)] = dk[n].astype(BF16)
            dqkv[n * BLOCK:(n + 1) * BLOCK, pl.ds(pl.multiple_of(2 * d_model + i * LANES, LANES), LANES)] = dv[n].astype(BF16)
        return carry

    lax.fori_loop(0, d_model // LANES, pair, 0)
    x = x_ref[0].astype(F32)
    d_normed = []
    for f in range(n_fsdp):
        w_qkv = jnp.concatenate([w_ref[f, p, :n_qkv] for p in range(n_ep)], axis=0)
        d_normed.append(jnp.dot(dqkv[...], w_qkv, preferred_element_type=F32).astype(BF16))
    d_normed = jnp.concatenate(d_normed, axis=1).astype(F32)
    inv = lax.rsqrt(jnp.mean(x * x, axis=-1, keepdims=True) + EPS)
    proj = jnp.mean(d_normed * x, axis=-1, keepdims=True)
    d_x = (d_normed * inv - x * (inv * inv * inv * proj)).astype(BF16).astype(F32)
    dx_ref[0] = (dh_ref[0].astype(F32) + d_x).astype(BF16)


def attention_grad(d_h, tokens, qkv, weights, head_dim):
    n_seq, seq_len, d_model = tokens.shape
    seq_spec = pl.BlockSpec((1, seq_len, d_model), lambda s: (s, 0, 0))
    qkv_spec = pl.BlockSpec((1, seq_len, 3 * d_model), lambda s: (s, 0, 0))
    w_spec = pl.BlockSpec(weights.shape, lambda s: (0, 0, 0, 0))
    return pl.pallas_call(
        functools.partial(attention_grad_kernel, head_dim=head_dim),
        grid=(n_seq,),
        in_specs=[seq_spec, seq_spec, qkv_spec, w_spec],
        out_specs=seq_spec,
        out_shape=jax.ShapeDtypeStruct(tokens.shape, BF16),
        scratch_shapes=[pltpu.VMEM((seq_len, d_model), BF16), pltpu.VMEM((seq_len, 3 * d_model), BF16)],
        name='attention_grad',
        **settings(150, 70),
    )(d_h, tokens, qkv, weights)


def capacity_of(tok_count, top_k, num_experts):
    return max(8, (5 * tok_count * top_k // (4 * num_experts) + 7) // 8 * 8)


def route_kernel(loc_ref, dest_ref, start_ref, rows_ref, off_ref, total, *, n_local):
    top_k = loc_ref.shape[1]
    ids = lax.broadcasted_iota(jnp.int32, (n_local, BLOCK), 0)
    upper = (lax.broadcasted_iota(jnp.int32, (BLOCK, BLOCK), 0) <= lax.broadcasted_iota(jnp.int32, (BLOCK, BLOCK), 1)).astype(F32).astype(BF16)
    before = (lax.broadcasted_iota(jnp.int32, (n_local, n_local), 0) > lax.broadcasted_iota(jnp.int32, (n_local, n_local), 1)).astype(F32).astype(BF16)

    @pl.when(pl.program_id(0) == 0)
    def _():
        total[...] = jnp.zeros(total.shape, jnp.int32)

    so_far = total[...]
    for s in range(loc_ref.shape[0]):
        for p in range(loc_ref.shape[2] // BLOCK):
            q = s * (loc_ref.shape[2] // BLOCK) + p
            loc = loc_ref[s, :, p * BLOCK:(p + 1) * BLOCK]
            member = jnp.zeros((n_local, BLOCK), F32)
            for j in range(top_k):
                member = jnp.where(loc[j:j + 1] == ids, 1.0, member)
            count = jnp.dot(member.astype(BF16), upper, preferred_element_type=F32)
            units = (count[:, BLOCK - 1:].astype(jnp.int32) + (ALIGN - 1)) // ALIGN
            units = jnp.broadcast_to(units, (n_local, LANES))
            start = jnp.dot(before, units.astype(F32).astype(BF16), preferred_element_type=F32).astype(jnp.int32) * ALIGN
            place = start[:, :1] + count.astype(jnp.int32) - 1
            for j in range(top_k):
                row = jnp.sum(jnp.where(loc[j:j + 1] == ids, place, 0), axis=0, keepdims=True)
                dest_ref[q, j:j + 1, :] = jnp.where(loc[j:j + 1] >= 0, row, -1)
            start_ref[q] = start
            rows_ref[q] = units * ALIGN
            off_ref[q] = so_far
            so_far = so_far + units * ALIGN
    total[...] = so_far


def route(local_ids, n_local):
    n_seq, top_k, seq_len = local_ids.shape
    per_seq = seq_len // BLOCK
    step = 2 if n_seq % 2 == 0 else 1
    n_blocks = n_seq * per_seq
    seg = jax.ShapeDtypeStruct((n_blocks, n_local, LANES), jnp.int32)
    seg_spec = pl.BlockSpec((step * per_seq, n_local, LANES), lambda s: (s, 0, 0))
    dest, *segs = pl.pallas_call(
        functools.partial(route_kernel, n_local=n_local),
        grid=(n_seq // step,),
        in_specs=[pl.BlockSpec((step, top_k, seq_len), lambda s: (s, 0, 0))],
        out_specs=[pl.BlockSpec((step * per_seq, top_k, BLOCK), lambda s: (s, 0, 0)), seg_spec, seg_spec, seg_spec],
        out_shape=[jax.ShapeDtypeStruct((n_blocks, top_k, BLOCK), jnp.int32), seg, seg, seg],
        scratch_shapes=[pltpu.VMEM((n_local, LANES), jnp.int32)],
        name='route',
        **settings(1, 3),
    )(local_ids)
    return dest, [part[:, :, 0] for part in segs]


def one_hot(dest_ref, gate_ref, first_row):
    rows = lax.broadcasted_iota(jnp.int32, (TILE, BLOCK), 0) + first_row
    dest = dest_ref[0]
    gate = gate_ref[0]
    picked = jnp.zeros((TILE, BLOCK), F32)
    for j in range(dest.shape[0]):
        picked = jnp.where(rows == dest[j:j + 1], gate[j:j + 1], picked)
    return picked


def dispatch_kernel(start_ref, rows_ref, off_ref, h_ref, dout_ref, dest_ref, gate_ref, *refs, base):
    r_hbm, d_hbm, u_s, rbuf, dbuf, sem = refs[-6:]
    step = pl.program_id(0)
    n_blocks = pl.num_programs(0)
    b = step + base
    n_exp = rows_ref.shape[1]
    slot = lax.rem(b, 2)

    def total(blk):
        return start_ref[blk, n_exp - 1] + rows_ref[blk, n_exp - 1]

    def drain(blk, which):
        n = pl.multiple_of(total(blk), ALIGN)

        @pl.when(n > 0)
        def _():
            pltpu.make_async_copy(rbuf.at[which, pl.ds(0, n), :], rbuf.at[which, pl.ds(0, n), :], sem.at[0, which]).wait()
            pltpu.make_async_copy(dbuf.at[which, pl.ds(0, n), :], dbuf.at[which, pl.ds(0, n), :], sem.at[1, which]).wait()

    @pl.when(step >= 2)
    def _():
        drain(b - 2, slot)

    hf = h_ref[...].astype(F32)
    u_s[...] = (hf * lax.rsqrt(jnp.mean(hf * hf, axis=-1, keepdims=True) + EPS)).astype(BF16)

    def tile(i, carry):
        first = pl.multiple_of(i * TILE, TILE)
        picked = one_hot(dest_ref, gate_ref, first)
        ones = jnp.where(picked > 0, 1.0, 0.0).astype(BF16)
        rbuf[slot, pl.ds(first, TILE), :] = jnp.dot(ones, u_s[...], preferred_element_type=F32).astype(BF16)
        dbuf[slot, pl.ds(first, TILE), :] = jnp.dot(picked.astype(BF16), dout_ref[...], preferred_element_type=F32).astype(BF16)
        return carry

    lax.fori_loop(0, (total(b) + (TILE - 1)) // TILE, tile, 0)

    def send(e, carry):
        n = pl.multiple_of(rows_ref[b, e], ALIGN)
        src = pl.multiple_of(start_ref[b, e], ALIGN)
        dst = pl.multiple_of(off_ref[b, e], ALIGN)

        @pl.when(n > 0)
        def _():
            pltpu.make_async_copy(rbuf.at[slot, pl.ds(src, n), :], r_hbm.at[e, pl.ds(dst, n), :], sem.at[0, slot]).start()
            pltpu.make_async_copy(dbuf.at[slot, pl.ds(src, n), :], d_hbm.at[e, pl.ds(dst, n), :], sem.at[1, slot]).start()

        return carry

    lax.fori_loop(0, n_exp, send, 0)

    @pl.when(step == n_blocks - 1)
    def _():
        @pl.when(n_blocks > 1)
        def _():
            drain(b - 1, 1 - slot)

        drain(b, slot)


def block_rows(top_k, n_local):
    return -(-(BLOCK * top_k + n_local * (ALIGN - 1)) // TILE) * TILE


def dispatch(h_tok, dout_tok, dest, gate, segs, base, held, n_local, max_rows):
    tok_count, d_model = h_tok.shape
    top_k = dest.shape[1]
    n_blocks = tok_count // BLOCK
    buf_rows = block_rows(top_k, n_local)
    tok_spec = pl.BlockSpec((BLOCK, d_model), lambda b, *_: (b, 0))
    map_spec = pl.BlockSpec((1, top_k, BLOCK), lambda b, *_: (b + base, 0, 0))
    rows_shape = jax.ShapeDtypeStruct((n_local, max_rows, d_model), BF16)
    hbm = pl.BlockSpec(memory_space=pl.ANY)
    return pl.pallas_call(
        functools.partial(dispatch_kernel, base=base),
        grid_spec=pltpu.PrefetchScalarGridSpec(
            num_scalar_prefetch=3,
            grid=(n_blocks,),
            in_specs=[tok_spec, tok_spec, map_spec, map_spec] + [hbm] * len(held),
            out_specs=[hbm, hbm],
            scratch_shapes=[
                pltpu.VMEM((BLOCK, d_model), BF16),
                pltpu.VMEM((2, buf_rows, d_model), BF16),
                pltpu.VMEM((2, buf_rows, d_model), BF16),
                pltpu.SemaphoreType.DMA((2, 2)),
            ],
        ),
        out_shape=[rows_shape, rows_shape],
        input_output_aliases={7: 0, 8: 1} if held else {},
        name='dispatch',
        **settings(40, 90),
    )(*segs, h_tok, dout_tok, dest, gate, *held)


def expert_kernel(count_ref, flip_ref, r_hbm, d_hbm, w_lo, w_hi, y_hbm, dr_hbm, dw_ref, rbuf, dbuf, ybuf, drbuf, done, in_sem, out_sem, *, expert_of):
    step = pl.program_id(0)
    n_steps = pl.num_programs(0)
    expert = expert_of(step)
    n_rows = count_ref[expert]
    n_tiles = jnp.maximum((n_rows + (TILE - 1)) // TILE, 1)
    half = dw_ref.shape[-1]

    def copies(who, i, slot, load):
        rows = pl.ds(pl.multiple_of(i * TILE, TILE), TILE)
        pairs = ((r_hbm, rbuf), (d_hbm, dbuf)) if load else ((ybuf, y_hbm), (drbuf, dr_hbm))
        for k, (src, dst) in enumerate(pairs):
            src = src.at[who, rows, :] if load else src.at[slot]
            dst = dst.at[slot] if load else dst.at[who, rows, :]
            yield pltpu.make_async_copy(src, dst, (in_sem if load else out_sem).at[k, slot])

    def start(*args):
        for copy in copies(*args):
            copy.start()

    def wait(*args):
        for copy in copies(*args):
            copy.wait()

    @pl.when(step == 0)
    def _():
        done[0] = 0
        start(expert, 0, 0, True)

    before = done[0]
    dw_ref[...] = jnp.zeros(dw_ref.shape, F32)

    def tile(i, carry):
        slot = lax.rem(before + i, 2)

        @pl.when(i + 1 < n_tiles)
        def _():
            start(expert, i + 1, 1 - slot, True)

        @pl.when((i + 1 == n_tiles) & (step + 1 < n_steps))
        def _():
            start(expert_of(step + 1), 0, 1 - slot, True)

        wait(expert, i, slot, True)

        @pl.when(before + i >= 2)
        def _():
            wait(expert, i, slot, False)

        valid = lax.broadcasted_iota(jnp.int32, (TILE, 1), 0) + i * TILE < n_rows
        r = jnp.where(valid, rbuf[slot], 0)
        dy = jnp.where(valid, dbuf[slot], 0)
        w1, w3, w2 = (jnp.concatenate([w[0, 0, t, 0] for w in (w_lo, w_hi)], axis=t // 2) for t in range(3))
        act_a = jnp.dot(r, w1, preferred_element_type=F32)
        act_b = jnp.dot(r, w3, preferred_element_type=F32)
        d_g = nt_dot(dy, w2)
        sig = 1.0 / (1.0 + jnp.exp(-act_a))
        silu = act_a * sig
        g = (silu * act_b).astype(BF16)
        d_up = (d_g * silu).astype(BF16)
        d_gate = (d_g * act_b * sig * (1.0 + act_a * (1.0 - sig))).astype(BF16)
        ybuf[slot] = jnp.dot(g, w2, preferred_element_type=F32).astype(BF16)
        drbuf[slot] = (nt_dot(d_gate, w1) + nt_dot(d_up, w3)).astype(BF16)
        start(expert, i, slot, False)
        for f in range(2):
            part = slice(f * half, (f + 1) * half)
            to = lax.rem(f + flip_ref[0], 2)
            for t, (lhs, rhs) in enumerate(((r[:, part], d_gate), (r[:, part], d_up), (g, dy[:, part]))):
                dw_ref[to, 0, t, 0] += tn_dot(lhs, rhs)
        return carry

    lax.fori_loop(0, n_tiles, tile, 0)
    done[0] = before + n_tiles

    @pl.when(step == n_steps - 1)
    def _():
        last = before + n_tiles - 1
        wait(expert, 0, lax.rem(last, 2), False)

        @pl.when(last >= 1)
        def _():
            wait(expert, 0, lax.rem(last + 1, 2), False)


def experts(rows, d_rows, weights, counts, flips, first, local_experts):
    d_model = rows.shape[2]
    n_fsdp, n_side, three, size, half, _ = weights.shape

    def expert_of(g):
        return g // size * local_experts + first + lax.rem(g, size)

    def side(g, flip):
        return lax.rem(g // size + flip[1], n_side)

    def w_spec(f):
        return pl.BlockSpec((1, 1, three, 1, half, half), lambda g, _, flip: (lax.rem(f + flip[0], n_fsdp), side(g, flip), 0, lax.rem(g, size), 0, 0))

    hbm = pl.BlockSpec(memory_space=pl.ANY)
    return pl.pallas_call(
        functools.partial(expert_kernel, expert_of=expert_of),
        grid_spec=pltpu.PrefetchScalarGridSpec(
            num_scalar_prefetch=2,
            grid=(n_side * size,),
            in_specs=[hbm, hbm, w_spec(0), w_spec(1)],
            out_specs=[hbm, hbm, pl.BlockSpec((n_fsdp, 1, three, 1, half, half), lambda g, _, flip: (0, side(g, flip), 0, lax.rem(g, size), 0, 0))],
            scratch_shapes=[pltpu.VMEM((2, TILE, d_model), BF16)] * 4 + [pltpu.SMEM((1,), jnp.int32)] + [pltpu.SemaphoreType.DMA((2, 2))] * 2,
        ),
        out_shape=[jax.ShapeDtypeStruct(rows.shape, BF16)] * 2 + [jax.ShapeDtypeStruct(weights.shape, F32)],
        input_output_aliases={2: 0, 3: 1},
        name='experts',
        **settings(56 * size, 100 * size),
    )(counts, flips, rows, d_rows, weights, weights)


def combine_kernel(start_ref, rows_ref, off_ref, y_hbm, dr_hbm, dest_ref, gate_ref, *refs, base, own):
    ybuf, dbuf, acc_y, acc_d, sem = refs[-5:]
    step = pl.program_id(0)
    n_blocks = pl.num_programs(0)
    b = step + base
    n_exp = rows_ref.shape[1]
    slot = lax.rem(step, 2)

    def total(blk):
        return start_ref[blk, n_exp - 1] + rows_ref[blk, n_exp - 1]

    def fetch(blk, which):
        def one(e, carry):
            n = pl.multiple_of(rows_ref[blk, e], ALIGN)
            dst = pl.multiple_of(start_ref[blk, e], ALIGN)
            src = pl.multiple_of(off_ref[blk, e], ALIGN)

            @pl.when(n > 0)
            def _():
                pltpu.make_async_copy(y_hbm.at[e, pl.ds(src, n), :], ybuf.at[which, pl.ds(dst, n), :], sem.at[0, which]).start()
                pltpu.make_async_copy(dr_hbm.at[e, pl.ds(src, n), :], dbuf.at[which, pl.ds(dst, n), :], sem.at[1, which]).start()

            return carry

        lax.fori_loop(0, n_exp, one, 0)

    @pl.when(step == 0)
    def _():
        ybuf[...] = jnp.zeros(ybuf.shape, BF16)
        dbuf[...] = jnp.zeros(dbuf.shape, BF16)
        fetch(b, 0)

    @pl.when(step + 1 < n_blocks)
    def _():
        fetch(b + 1, 1 - slot)

    n = pl.multiple_of(total(b), ALIGN)

    @pl.when(n > 0)
    def _():
        pltpu.make_async_copy(ybuf.at[slot, pl.ds(0, n), :], ybuf.at[slot, pl.ds(0, n), :], sem.at[0, slot]).wait()
        pltpu.make_async_copy(dbuf.at[slot, pl.ds(0, n), :], dbuf.at[slot, pl.ds(0, n), :], sem.at[1, slot]).wait()

    acc_y[...] = jnp.zeros(acc_y.shape, F32)
    acc_d[...] = jnp.zeros(acc_d.shape, F32)

    def tile(i, carry):
        first = pl.multiple_of(i * TILE, TILE)
        picked = one_hot(dest_ref, gate_ref, first)
        ones = jnp.where(picked > 0, 1.0, 0.0).astype(BF16)
        acc_y[...] += tn_dot(picked.astype(BF16), ybuf[slot, pl.ds(first, TILE), :])
        acc_d[...] += tn_dot(ones, dbuf[slot, pl.ds(first, TILE), :])
        return carry

    lax.fori_loop(0, (n + (TILE - 1)) // TILE, tile, 0)

    if not own:
        out_y, out_d = refs[:2]
        out_y[...] = acc_y[...]
        out_d[...] = acc_d[...]
        return
    more_y, more_d, h_ref, dout_ref, out_ref, dh_ref = refs[:6]
    hf = h_ref[...].astype(F32)
    out_ref[...] = (hf + (acc_y[...] + more_y[...])).astype(BF16)
    d_u = (acc_d[...] + more_d[...]).astype(BF16).astype(F32)
    inv = lax.rsqrt(jnp.mean(hf * hf, axis=-1, keepdims=True) + EPS)
    proj = jnp.mean(d_u * hf, axis=-1, keepdims=True)
    d_norm = (d_u * inv - hf * (inv * inv * inv * proj)).astype(BF16).astype(F32)
    dh_ref[...] = (dout_ref[...].astype(F32) + d_norm).astype(BF16)


def combine(y_rows, dr_rows, dest, gate, segs, base, n_blocks, extra):
    n_local, _, d_model = y_rows.shape
    top_k = dest.shape[1]
    buf_rows = block_rows(top_k, n_local)
    tok_spec = pl.BlockSpec((BLOCK, d_model), lambda b, *_: (b, 0))
    map_spec = pl.BlockSpec((1, top_k, BLOCK), lambda b, *_: (b + base, 0, 0))
    hbm = pl.BlockSpec(memory_space=pl.ANY)
    out = jax.ShapeDtypeStruct((n_blocks * BLOCK, d_model), BF16 if extra else F32)
    return pl.pallas_call(
        functools.partial(combine_kernel, base=base, own=bool(extra)),
        grid_spec=pltpu.PrefetchScalarGridSpec(
            num_scalar_prefetch=3,
            grid=(n_blocks,),
            in_specs=[hbm, hbm, map_spec, map_spec] + [tok_spec] * len(extra),
            out_specs=[tok_spec, tok_spec],
            scratch_shapes=[
                pltpu.VMEM((2, buf_rows, d_model), BF16),
                pltpu.VMEM((2, buf_rows, d_model), BF16),
                pltpu.VMEM((BLOCK, d_model), F32),
                pltpu.VMEM((BLOCK, d_model), F32),
                pltpu.SemaphoreType.DMA((2, 2)),
            ],
        ),
        out_shape=[out, out],
        name='combine',
        **settings(45, 120),
    )(*segs, y_rows, dr_rows, dest, gate, *extra)


def place_kernel(*refs, n_parts):
    for k, out_ref in enumerate(refs[-3:]):
        value = refs[0][k]
        for part_ref in refs[1:n_parts]:
            value = value + part_ref[k]
        out_ref[...] = value


def place(parts, held, first, n_total):
    three, size, rows, cols = parts[0].shape
    hbm = pl.BlockSpec(memory_space=pl.ANY)
    return pl.pallas_call(
        functools.partial(place_kernel, n_parts=len(parts)),
        grid=(size,),
        in_specs=[pl.BlockSpec((three, 1, rows, cols), lambda i: (0, i, 0, 0))] * len(parts) + [hbm] * len(held),
        out_specs=[pl.BlockSpec((1, rows, cols), lambda i: (first + i, 0, 0))] * three,
        out_shape=[jax.ShapeDtypeStruct((n_total, rows, cols), F32)] * three,
        input_output_aliases={len(parts) + k: k for k in range(len(held))},
        name='place',
        **settings(1, 12),
    )(*parts, *held)


CHUNKS = (3, 3)
CORES = 2


def solution(mesh):
    ep_size, fsdp_size = mesh.shape['ep'], mesh.shape['fsdp']
    tok_spec = P(('data', 'fsdp', 'ep'))
    in_specs = (tok_spec, P('fsdp'), P(None, None, 'fsdp'), P('ep', 'fsdp'), P('ep', 'fsdp'), P('ep', None, 'fsdp'), tok_spec, tok_spec, tok_spec, tok_spec)
    out_specs = (tok_spec, tok_spec, P(('data', 'ep'), 'fsdp'), P(('data', 'ep'), 'fsdp'), P(('data', 'ep'), None, 'fsdp'))

    def device_fn(tokens, w_qkv, w_out, w_gate, w_up, w_down, expert_idx, expert_slot, gate_wts, d_out):
        n_seq, seq_len, d_model = tokens.shape
        tok_count = n_seq * seq_len
        top_k = expert_idx.shape[2]
        local_experts, half, _ = w_gate.shape
        num_experts = local_experts * ep_size
        n_side = ep_size // CORES
        n_local = local_experts * n_side
        n_blocks = tok_count // BLOCK
        capacity = capacity_of(tok_count, top_k, num_experts)
        max_rows = -(-(CORES * (capacity + n_blocks * (ALIGN - 1))) // TILE) * TILE
        ep = lax.axis_index('ep')
        groups = [[c + CORES * i for i in range(fsdp_size * n_side)] for c in range(CORES)]

        fsdp, side = lax.axis_index('fsdp'), ep // CORES
        flips = jnp.stack([fsdp, side]).astype(jnp.int32)

        def swap(values):
            return lax.ppermute(values, 'ep', [(i, i ^ 1) for i in range(ep_size)])

        def swap_x(values):
            return lax.ppermute(values, 'ep', [(i, i ^ CORES) for i in range(ep_size)])

        def swap_y(values):
            return lax.ppermute(values, 'fsdp', [(i, i ^ 1) for i in range(fsdp_size)])

        def own_weights(part):
            return jnp.stack([w_gate[part], w_up[part], w_down[part]], axis=0)

        _, head_dim, _ = w_out.shape
        qkv_rows = w_qkv.transpose(1, 2, 3, 0).reshape(-1, half)
        qkv_rows = lax.dynamic_slice_in_dim(qkv_rows, ep * (3 * d_model // ep_size), 3 * d_model // ep_size, axis=0)
        out_rows = lax.dynamic_slice_in_dim(w_out.reshape(-1, half), ep * (d_model // ep_size), d_model // ep_size, axis=0)
        attn_w = lax.all_gather(jnp.concatenate([qkv_rows, out_rows], axis=0), ('fsdp', 'ep'), axis=0, tiled=False)
        attn_w = attn_w.reshape(fsdp_size, ep_size, -1, half)
        weights, first = [], 0
        for size in CHUNKS:
            mine = own_weights(slice(first, first + size))
            full = lax.all_gather(mine, ('fsdp', 'ep'), axis=0, tiled=False, axis_index_groups=groups)
            weights.append(full.reshape(fsdp_size, n_side, *mine.shape))
            first += size
        mid = first + (local_experts - first) // 2
        attn_w, w_a, w_b = lax.optimization_barrier((attn_w, own_weights(slice(first, mid)), own_weights(slice(mid, local_experts))))
        w_ax, w_ay, w_bx, w_by = swap_x(w_a), swap_y(w_a), swap_x(w_b), swap_y(w_b)

        dout_tok = d_out.reshape(tok_count, d_model)
        dout_other = swap(dout_tok)
        kept_ids = jnp.where(expert_slot >= 0, expert_idx, -1).transpose(0, 2, 1)
        all_ids = jnp.concatenate([kept_ids, swap(kept_ids)], axis=0)
        owner = all_ids // local_experts
        mine_too = (all_ids >= 0) & (lax.rem(owner, CORES) == lax.rem(ep, CORES))
        local_ids = jnp.where(mine_too, owner // CORES * local_experts + lax.rem(all_ids, local_experts), -1)
        dest, segs = route(local_ids, n_local)
        counts = jnp.sum(segs[1], axis=0)
        gate = gate_wts.transpose(0, 2, 1)
        gate = jnp.concatenate([gate, swap(gate)], axis=0).astype(F32)
        gate = gate.reshape(2 * n_seq, top_k, seq_len // BLOCK, BLOCK).transpose(0, 2, 1, 3).reshape(2 * n_blocks, top_k, BLOCK)

        tokens, dest, segs, counts, gate = lax.optimization_barrier((tokens, dest, segs, counts, gate))
        h_seq, qkv = attention(tokens, attn_w, head_dim)
        w_axy, w_byx = swap_y(w_ax), swap_x(w_by)
        w_rest = jnp.stack([jnp.concatenate(pair, axis=1) for pair in ((w_a, w_b), (w_ax, w_bx), (w_ay, w_by), (w_axy, w_byx))])
        w_rest = w_rest.reshape(fsdp_size, n_side, *w_rest.shape[1:])
        h_tok = h_seq.reshape(tok_count, d_model)
        h_other = swap(h_tok)
        held = dispatch(h_tok, dout_tok, dest, gate, segs, 0, [], n_local, max_rows)
        rows, d_rows = dispatch(h_other, dout_other, dest, gate, segs, n_blocks, held, n_local, max_rows)
        rows, d_rows, d_rest = experts(rows, d_rows, w_rest, counts, flips, first, local_experts)
        d_a, d_b = d_rest[:, :, :, :mid - first], d_rest[:, :, :, mid - first:]
        more_a, more_b = swap_x(d_a[:, 1]), swap_y(d_b[1])
        d_a, d_b = d_a[:, 0] + more_a, d_b[0] + more_b
        more_a, more_b = swap_y(d_a[1]), swap_x(d_b[1])
        done, start = [([d_a[0], more_a], first), ([d_b[0], more_b], mid)], 0
        for n, size in enumerate(CHUNKS):
            rows, d_rows, d_w = experts(rows, d_rows, weights[n], counts, jnp.zeros_like(flips), start, local_experts)
            d_w = d_w.reshape(fsdp_size * n_side, *d_w.shape[2:])
            d_w = lax.psum_scatter(d_w, ('fsdp', 'ep'), scatter_dimension=0, tiled=False, axis_index_groups=groups)
            done.insert(0 if n == 0 else len(done), ([d_w], start))
            start += size
        sums = combine(rows, d_rows, dest, gate, segs, n_blocks, n_blocks, [])
        more = [swap(value) for value in sums]
        layer_out, d_h = combine(rows, d_rows, dest, gate, segs, 0, n_blocks, [*more, h_tok, dout_tok])
        d_tokens = attention_grad(d_h.reshape(n_seq, seq_len, d_model), tokens, qkv, attn_w, head_dim)
        d_ws = []
        for parts, where in done:
            d_ws = place(parts, d_ws, where, local_experts)
        return layer_out.reshape(n_seq, seq_len, d_model), d_tokens, *d_ws

    return jax.shard_map(device_fn, mesh=mesh, in_specs=in_specs, out_specs=out_specs, check_vma=False)
```

```python
import functools
import math

import jax
import jax.numpy as jnp
from jax import lax
from jax.experimental import pallas as pl
from jax.experimental.pallas import tpu as pltpu
from jax.sharding import PartitionSpec as P


F32 = jnp.float32
BF16 = jnp.bfloat16
BLOCK = 256
TILE = 256
ALIGN = 16
LANES = 128
LOG2E = math.log2(math.e)
EPS = 1e-6
VMEM_BYTES = 60 * 2 ** 20


def settings(gflop, mbytes):
    return {
        'compiler_params': pltpu.CompilerParams(dimension_semantics=('arbitrary',), vmem_limit_bytes=VMEM_BYTES),
        'cost_estimate': pl.CostEstimate(flops=gflop * 10 ** 9, bytes_accessed=mbytes * 10 ** 6, transcendentals=0),
    }


def nt_dot(lhs, rhs):
    return lax.dot_general(lhs, rhs, (((1,), (1,)), ((), ())), preferred_element_type=F32)


def tn_dot(lhs, rhs):
    return lax.dot_general(lhs, rhs, (((0,), (0,)), ((), ())), preferred_element_type=F32)


def lanes_of(head, values):
    lane = lax.broadcasted_iota(jnp.int32, values.shape, 1)
    return jnp.where((lane >= LANES // 2) == bool(head), values, jnp.zeros_like(values))


def attention_kernel(x_ref, w_ref, h_ref, qkv_ref, ctx, *, head_dim):
    seq_len, d_model = x_ref.shape[1:]
    n_fsdp, n_ep, rows, half = w_ref.shape
    n_qkv = rows * 3 // 4
    x = x_ref[0].astype(F32)
    normed = (x * lax.rsqrt(jnp.mean(x * x, axis=-1, keepdims=True) + EPS)).astype(BF16)
    for p in range(n_ep):
        part = nt_dot(normed[:, :half], w_ref[0, p, :n_qkv]) + nt_dot(normed[:, half:], w_ref[1, p, :n_qkv])
        qkv_ref[0, :, p * n_qkv:(p + 1) * n_qkv] = part.astype(BF16)
    scale = head_dim ** -0.5 * LOG2E

    def pair(i, carry):
        q2, k2, v2 = (qkv_ref[0, :, pl.ds(pl.multiple_of(t * d_model + i * LANES, LANES), LANES)] for t in range(3))
        for first in range(0, seq_len, BLOCK):
            end = first + BLOCK
            keys, vals = k2[:end], v2[:end]
            causal = lax.broadcasted_iota(jnp.int32, (BLOCK, end), 0) + first >= lax.broadcasted_iota(jnp.int32, (BLOCK, end), 1)
            both = []
            for head in range(2):
                scores = nt_dot(lanes_of(head, q2[first:end]), keys) * scale
                scores = jnp.where(causal, scores, -1e30)
                probs = jnp.exp2(scores - jnp.max(scores, axis=-1, keepdims=True))
                probs = (probs * (1.0 / jnp.sum(probs, axis=-1, keepdims=True))).astype(BF16)
                both.append(jnp.dot(probs, vals, preferred_element_type=F32))
            lane = lax.broadcasted_iota(jnp.int32, (BLOCK, LANES), 1)
            ctx[first:end, pl.ds(pl.multiple_of(i * LANES, LANES), LANES)] = jnp.where(lane < LANES // 2, both[0], both[1]).astype(BF16)
        return carry

    lax.fori_loop(0, d_model // LANES, pair, 0)
    for f in range(n_fsdp):
        w_out = jnp.concatenate([w_ref[f, p, n_qkv:] for p in range(n_ep)], axis=0)
        cols = slice(f * half, (f + 1) * half)
        h_ref[0, :, cols] = (x_ref[0, :, cols].astype(F32) + jnp.dot(ctx[...], w_out, preferred_element_type=F32)).astype(BF16)


def attention(tokens, weights, head_dim):
    n_seq, seq_len, d_model = tokens.shape
    seq_spec = pl.BlockSpec((1, seq_len, d_model), lambda s: (s, 0, 0))
    qkv_spec = pl.BlockSpec((1, seq_len, 3 * d_model), lambda s: (s, 0, 0))
    w_spec = pl.BlockSpec(weights.shape, lambda s: (0, 0, 0, 0))
    return pl.pallas_call(
        functools.partial(attention_kernel, head_dim=head_dim),
        grid=(n_seq,),
        in_specs=[seq_spec, w_spec],
        out_specs=[seq_spec, qkv_spec],
        out_shape=[jax.ShapeDtypeStruct(tokens.shape, BF16), jax.ShapeDtypeStruct((n_seq, seq_len, 3 * d_model), BF16)],
        scratch_shapes=[pltpu.VMEM((seq_len, d_model), BF16)],
        name='attention',
        **settings(90, 60),
    )(tokens, weights)


def attention_grad_kernel(dh_ref, x_ref, qkv_ref, w_ref, dx_ref, dctx, dqkv, *, head_dim):
    seq_len, d_model = x_ref.shape[1:]
    n_fsdp, n_ep, rows, half = w_ref.shape
    n_qkv = rows * 3 // 4
    n_out = rows - n_qkv
    dh = dh_ref[0]
    for p in range(n_ep):
        part = nt_dot(dh[:, :half], w_ref[0, p, n_qkv:]) + nt_dot(dh[:, half:], w_ref[1, p, n_qkv:])
        dctx[:, p * n_out:(p + 1) * n_out] = part.astype(BF16)
    scale = head_dim ** -0.5

    def pair(i, carry):
        col = pl.multiple_of(i * LANES, LANES)
        q2, k2, v2 = (qkv_ref[0, :, pl.ds(pl.multiple_of(t * d_model + i * LANES, LANES), LANES)] for t in range(3))
        d2 = dctx[:, pl.ds(col, LANES)]
        dk = [jnp.zeros((BLOCK, LANES), F32)] * (seq_len // BLOCK)
        dv = list(dk)
        for first in range(0, seq_len, BLOCK):
            end = first + BLOCK
            keys, vals = k2[:end], v2[:end]
            causal = lax.broadcasted_iota(jnp.int32, (end, BLOCK), 1) + first >= lax.broadcasted_iota(jnp.int32, (end, BLOCK), 0)
            dq = jnp.zeros((BLOCK, LANES), F32)
            for head in range(2):
                q, d = lanes_of(head, q2[first:end]), lanes_of(head, d2[first:end])
                scores = jnp.where(causal, nt_dot(keys, q) * (scale * LOG2E), -1e30)
                probs = jnp.exp2(scores - jnp.max(scores, axis=0, keepdims=True))
                probs = probs * (1.0 / jnp.sum(probs, axis=0, keepdims=True))
                d_probs = nt_dot(vals, d)
                d_scores = probs * (d_probs - jnp.sum(probs * d_probs, axis=0, keepdims=True))
                d_scores = (d_scores * scale).astype(BF16)
                dv_part = jnp.dot(probs.astype(BF16), d, preferred_element_type=F32)
                dk_part = jnp.dot(d_scores, q, preferred_element_type=F32)
                dq = dq + tn_dot(d_scores, lanes_of(head, keys))
                for n in range(end // BLOCK):
                    dk[n] = dk[n] + dk_part[n * BLOCK:(n + 1) * BLOCK]
                    dv[n] = dv[n] + dv_part[n * BLOCK:(n + 1) * BLOCK]
            dqkv[first:end, pl.ds(col, LANES)] = dq.astype(BF16)
        for n in range(seq_len // BLOCK):
            dqkv[n * BLOCK:(n + 1) * BLOCK, pl.ds(pl.multiple_of(d_model + i * LANES, LANES), LANES)] = dk[n].astype(BF16)
            dqkv[n * BLOCK:(n + 1) * BLOCK, pl.ds(pl.multiple_of(2 * d_model + i * LANES, LANES), LANES)] = dv[n].astype(BF16)
        return carry

    lax.fori_loop(0, d_model // LANES, pair, 0)
    x = x_ref[0].astype(F32)
    d_normed = []
    for f in range(n_fsdp):
        w_qkv = jnp.concatenate([w_ref[f, p, :n_qkv] for p in range(n_ep)], axis=0)
        d_normed.append(jnp.dot(dqkv[...], w_qkv, preferred_element_type=F32).astype(BF16))
    d_normed = jnp.concatenate(d_normed, axis=1).astype(F32)
    inv = lax.rsqrt(jnp.mean(x * x, axis=-1, keepdims=True) + EPS)
    proj = jnp.mean(d_normed * x, axis=-1, keepdims=True)
    d_x = (d_normed * inv - x * (inv * inv * inv * proj)).astype(BF16).astype(F32)
    dx_ref[0] = (dh_ref[0].astype(F32) + d_x).astype(BF16)


def attention_grad(d_h, tokens, qkv, weights, head_dim):
    n_seq, seq_len, d_model = tokens.shape
    seq_spec = pl.BlockSpec((1, seq_len, d_model), lambda s: (s, 0, 0))
    qkv_spec = pl.BlockSpec((1, seq_len, 3 * d_model), lambda s: (s, 0, 0))
    w_spec = pl.BlockSpec(weights.shape, lambda s: (0, 0, 0, 0))
    return pl.pallas_call(
        functools.partial(attention_grad_kernel, head_dim=head_dim),
        grid=(n_seq,),
        in_specs=[seq_spec, seq_spec, qkv_spec, w_spec],
        out_specs=seq_spec,
        out_shape=jax.ShapeDtypeStruct(tokens.shape, BF16),
        scratch_shapes=[pltpu.VMEM((seq_len, d_model), BF16), pltpu.VMEM((seq_len, 3 * d_model), BF16)],
        name='attention_grad',
        **settings(150, 70),
    )(d_h, tokens, qkv, weights)


def capacity_of(tok_count, top_k, num_experts):
    return max(8, (5 * tok_count * top_k // (4 * num_experts) + 7) // 8 * 8)


def route_kernel(loc_ref, dest_ref, start_ref, rows_ref, off_ref, total, *, n_local):
    top_k = loc_ref.shape[1]
    ids = lax.broadcasted_iota(jnp.int32, (n_local, BLOCK), 0)
    upper = (lax.broadcasted_iota(jnp.int32, (BLOCK, BLOCK), 0) <= lax.broadcasted_iota(jnp.int32, (BLOCK, BLOCK), 1)).astype(F32).astype(BF16)
    before = (lax.broadcasted_iota(jnp.int32, (n_local, n_local), 0) > lax.broadcasted_iota(jnp.int32, (n_local, n_local), 1)).astype(F32).astype(BF16)

    @pl.when(pl.program_id(0) == 0)
    def _():
        total[...] = jnp.zeros(total.shape, jnp.int32)

    so_far = total[...]
    for s in range(loc_ref.shape[0]):
        for p in range(loc_ref.shape[2] // BLOCK):
            q = s * (loc_ref.shape[2] // BLOCK) + p
            loc = loc_ref[s, :, p * BLOCK:(p + 1) * BLOCK]
            member = jnp.zeros((n_local, BLOCK), F32)
            for j in range(top_k):
                member = jnp.where(loc[j:j + 1] == ids, 1.0, member)
            count = jnp.dot(member.astype(BF16), upper, preferred_element_type=F32)
            units = (count[:, BLOCK - 1:].astype(jnp.int32) + (ALIGN - 1)) // ALIGN
            units = jnp.broadcast_to(units, (n_local, LANES))
            start = jnp.dot(before, units.astype(F32).astype(BF16), preferred_element_type=F32).astype(jnp.int32) * ALIGN
            place = start[:, :1] + count.astype(jnp.int32) - 1
            for j in range(top_k):
                row = jnp.sum(jnp.where(loc[j:j + 1] == ids, place, 0), axis=0, keepdims=True)
                dest_ref[q, j:j + 1, :] = jnp.where(loc[j:j + 1] >= 0, row, -1)
            start_ref[q] = start
            rows_ref[q] = units * ALIGN
            off_ref[q] = so_far
            so_far = so_far + units * ALIGN
    total[...] = so_far


def route(local_ids, n_local):
    n_seq, top_k, seq_len = local_ids.shape
    per_seq = seq_len // BLOCK
    step = 2 if n_seq % 2 == 0 else 1
    n_blocks = n_seq * per_seq
    seg = jax.ShapeDtypeStruct((n_blocks, n_local, LANES), jnp.int32)
    seg_spec = pl.BlockSpec((step * per_seq, n_local, LANES), lambda s: (s, 0, 0))
    dest, *segs = pl.pallas_call(
        functools.partial(route_kernel, n_local=n_local),
        grid=(n_seq // step,),
        in_specs=[pl.BlockSpec((step, top_k, seq_len), lambda s: (s, 0, 0))],
        out_specs=[pl.BlockSpec((step * per_seq, top_k, BLOCK), lambda s: (s, 0, 0)), seg_spec, seg_spec, seg_spec],
        out_shape=[jax.ShapeDtypeStruct((n_blocks, top_k, BLOCK), jnp.int32), seg, seg, seg],
        scratch_shapes=[pltpu.VMEM((n_local, LANES), jnp.int32)],
        name='route',
        **settings(1, 3),
    )(local_ids)
    return dest, [part[:, :, 0] for part in segs]


def one_hot(dest_ref, gate_ref, first_row):
    rows = lax.broadcasted_iota(jnp.int32, (TILE, BLOCK), 0).astype(F32).astype(BF16)
    dest = jnp.clip(dest_ref[0] - first_row, -1, TILE).astype(F32).astype(BF16)
    gate = gate_ref[0]
    picked = jnp.zeros((TILE, BLOCK), BF16)
    for j in range(dest.shape[0]):
        picked = jnp.where(rows == dest[j:j + 1], gate[j:j + 1], picked)
    return picked, jnp.where(picked > 0, jnp.ones_like(picked), jnp.zeros_like(picked))


def dispatch_kernel(start_ref, rows_ref, off_ref, h_ref, dout_ref, dest_ref, gate_ref, *refs, base):
    r_hbm, d_hbm, u_s, rbuf, dbuf, sem = refs[-6:]
    step = pl.program_id(0)
    n_blocks = pl.num_programs(0)
    b = step + base
    n_exp = rows_ref.shape[1]
    slot = lax.rem(b, 2)

    def total(blk):
        return start_ref[blk, n_exp - 1] + rows_ref[blk, n_exp - 1]

    def drain(blk, which):
        n = pl.multiple_of(total(blk), ALIGN)

        @pl.when(n > 0)
        def _():
            pltpu.make_async_copy(rbuf.at[which, pl.ds(0, n), :], rbuf.at[which, pl.ds(0, n), :], sem.at[0, which]).wait()
            pltpu.make_async_copy(dbuf.at[which, pl.ds(0, n), :], dbuf.at[which, pl.ds(0, n), :], sem.at[1, which]).wait()

    @pl.when(step >= 2)
    def _():
        drain(b - 2, slot)

    hf = h_ref[...].astype(F32)
    u_s[...] = (hf * lax.rsqrt(jnp.mean(hf * hf, axis=-1, keepdims=True) + EPS)).astype(BF16)

    def tile(i, carry):
        first = pl.multiple_of(i * TILE, TILE)
        picked, ones = one_hot(dest_ref, gate_ref, first)
        rbuf[slot, pl.ds(first, TILE), :] = jnp.dot(ones, u_s[...], preferred_element_type=F32).astype(BF16)
        dbuf[slot, pl.ds(first, TILE), :] = jnp.dot(picked, dout_ref[...], preferred_element_type=F32).astype(BF16)
        return carry

    lax.fori_loop(0, (total(b) + (TILE - 1)) // TILE, tile, 0)

    def send(e, carry):
        n = pl.multiple_of(rows_ref[b, e], ALIGN)
        src = pl.multiple_of(start_ref[b, e], ALIGN)
        dst = pl.multiple_of(off_ref[b, e], ALIGN)

        @pl.when(n > 0)
        def _():
            pltpu.make_async_copy(rbuf.at[slot, pl.ds(src, n), :], r_hbm.at[e, pl.ds(dst, n), :], sem.at[0, slot]).start()
            pltpu.make_async_copy(dbuf.at[slot, pl.ds(src, n), :], d_hbm.at[e, pl.ds(dst, n), :], sem.at[1, slot]).start()

        return carry

    lax.fori_loop(0, n_exp, send, 0)

    @pl.when(step == n_blocks - 1)
    def _():
        @pl.when(n_blocks > 1)
        def _():
            drain(b - 1, 1 - slot)

        drain(b, slot)


def block_rows(top_k, n_local):
    return -(-(BLOCK * top_k + n_local * (ALIGN - 1)) // TILE) * TILE


def dispatch(h_tok, dout_tok, dest, gate, segs, base, held, n_local, max_rows):
    tok_count, d_model = h_tok.shape
    top_k = dest.shape[1]
    n_blocks = tok_count // BLOCK
    buf_rows = block_rows(top_k, n_local)
    tok_spec = pl.BlockSpec((BLOCK, d_model), lambda b, *_: (b, 0))
    map_spec = pl.BlockSpec((1, top_k, BLOCK), lambda b, *_: (b + base, 0, 0))
    rows_shape = jax.ShapeDtypeStruct((n_local, max_rows, d_model), BF16)
    hbm = pl.BlockSpec(memory_space=pl.ANY)
    return pl.pallas_call(
        functools.partial(dispatch_kernel, base=base),
        grid_spec=pltpu.PrefetchScalarGridSpec(
            num_scalar_prefetch=3,
            grid=(n_blocks,),
            in_specs=[tok_spec, tok_spec, map_spec, map_spec] + [hbm] * len(held),
            out_specs=[hbm, hbm],
            scratch_shapes=[
                pltpu.VMEM((BLOCK, d_model), BF16),
                pltpu.VMEM((2, buf_rows, d_model), BF16),
                pltpu.VMEM((2, buf_rows, d_model), BF16),
                pltpu.SemaphoreType.DMA((2, 2)),
            ],
        ),
        out_shape=[rows_shape, rows_shape],
        input_output_aliases={7: 0, 8: 1} if held else {},
        name='dispatch',
        **settings(40, 90),
    )(*segs, h_tok, dout_tok, dest, gate, *held)


def expert_kernel(count_ref, flip_ref, r_hbm, d_hbm, w_lo, w_hi, y_hbm, dr_hbm, dw_ref, rbuf, dbuf, ybuf, drbuf, done, in_sem, out_sem, *, expert_of, x_first):
    step = pl.program_id(0)
    n_steps = pl.num_programs(0)
    expert = expert_of(step)
    n_rows = count_ref[expert]
    n_tiles = jnp.maximum((n_rows + (TILE - 1)) // TILE, 1)
    half = dw_ref.shape[-1]

    def copies(who, i, slot, load):
        rows = pl.ds(pl.multiple_of(i * TILE, TILE), TILE)
        pairs = ((r_hbm, rbuf), (d_hbm, dbuf)) if load else ((ybuf, y_hbm), (drbuf, dr_hbm))
        for k, (src, dst) in enumerate(pairs):
            src = src.at[who, rows, :] if load else src.at[slot]
            dst = dst.at[slot] if load else dst.at[who, rows, :]
            yield pltpu.make_async_copy(src, dst, (in_sem if load else out_sem).at[k, slot])

    def start(*args):
        for copy in copies(*args):
            copy.start()

    def wait(*args):
        for copy in copies(*args):
            copy.wait()

    @pl.when(step == 0)
    def _():
        done[0] = 0
        start(expert, 0, 0, True)

    before = done[0]
    dw_ref[...] = jnp.zeros(dw_ref.shape, F32)

    def tile(i, carry):
        slot = lax.rem(before + i, 2)

        @pl.when(i + 1 < n_tiles)
        def _():
            start(expert, i + 1, 1 - slot, True)

        @pl.when((i + 1 == n_tiles) & (step + 1 < n_steps))
        def _():
            start(expert_of(step + 1), 0, 1 - slot, True)

        wait(expert, i, slot, True)

        @pl.when(before + i >= 2)
        def _():
            wait(expert, i, slot, False)

        valid = lax.broadcasted_iota(jnp.int32, (TILE, 1), 0) + i * TILE < n_rows
        r = jnp.where(valid, rbuf[slot], 0)
        dy = jnp.where(valid, dbuf[slot], 0)
        w1, w3, w2 = (jnp.concatenate([w[0, t, 0] for w in (w_lo, w_hi)], axis=t // 2) for t in range(3))
        act_a = jnp.dot(r, w1, preferred_element_type=F32)
        act_b = jnp.dot(r, w3, preferred_element_type=F32)
        d_g = nt_dot(dy, w2)
        sig = 1.0 / (1.0 + jnp.exp(-act_a))
        silu = act_a * sig
        g = (silu * act_b).astype(BF16)
        d_up = (d_g * silu).astype(BF16)
        d_gate = (d_g * act_b * sig * (1.0 + act_a * (1.0 - sig))).astype(BF16)
        ybuf[slot] = jnp.dot(g, w2, preferred_element_type=F32).astype(BF16)
        drbuf[slot] = (nt_dot(d_gate, w1) + nt_dot(d_up, w3)).astype(BF16)
        start(expert, i, slot, False)
        for f in range(2):
            part = slice(f * half, (f + 1) * half)
            to = lax.rem(f + flip_ref[0], 2)
            for t, (lhs, rhs) in enumerate(((r[:, part], d_gate), (r[:, part], d_up), (g, dy[:, part]))):
                dw_ref[(0, to, t, 0) if x_first else (to, 0, t, 0)] += tn_dot(lhs, rhs)
        return carry

    lax.fori_loop(0, n_tiles, tile, 0)
    done[0] = before + n_tiles

    @pl.when(step == n_steps - 1)
    def _():
        last = before + n_tiles - 1
        wait(expert, 0, lax.rem(last, 2), False)

        @pl.when(last >= 1)
        def _():
            wait(expert, 0, lax.rem(last + 1, 2), False)


def experts(rows, d_rows, weights, counts, flips, first, local_experts, x_first=False):
    d_model = rows.shape[2]
    n_owners, three, size, half, _ = weights.shape
    n_fsdp = d_model // half
    n_side = n_owners // n_fsdp

    def expert_of(g):
        return g // size * local_experts + first + lax.rem(g, size)

    def side(g, flip):
        return lax.rem(g // size + flip[1], n_side)

    def w_spec(f):
        return pl.BlockSpec((1, three, 1, half, half), lambda g, _, flip: (lax.rem(f + flip[0], n_fsdp) * n_side + side(g, flip), 0, lax.rem(g, size), 0, 0))

    def dw_index(g, _, flip):
        place = (side(g, flip), 0) if x_first else (0, side(g, flip))
        return (*place, 0, lax.rem(g, size), 0, 0)

    hbm = pl.BlockSpec(memory_space=pl.ANY)
    grads = (n_side, n_fsdp) if x_first else (n_fsdp, n_side)
    dw_block = (1, n_fsdp) if x_first else (n_fsdp, 1)
    return pl.pallas_call(
        functools.partial(expert_kernel, expert_of=expert_of, x_first=x_first),
        grid_spec=pltpu.PrefetchScalarGridSpec(
            num_scalar_prefetch=2,
            grid=(n_side * size,),
            in_specs=[hbm, hbm, w_spec(0), w_spec(1)],
            out_specs=[hbm, hbm, pl.BlockSpec((*dw_block, three, 1, half, half), dw_index)],
            scratch_shapes=[pltpu.VMEM((2, TILE, d_model), BF16)] * 4 + [pltpu.SMEM((1,), jnp.int32)] + [pltpu.SemaphoreType.DMA((2, 2))] * 2,
        ),
        out_shape=[jax.ShapeDtypeStruct(rows.shape, BF16)] * 2 + [jax.ShapeDtypeStruct((*grads, three, size, half, half), F32)],
        input_output_aliases={2: 0, 3: 1},
        name='experts',
        **settings(56 * size, 100 * size),
    )(counts, flips, rows, d_rows, weights, weights)


def combine_kernel(start_ref, rows_ref, off_ref, y_hbm, dr_hbm, dest_ref, gate_ref, *refs, base, own):
    ybuf, dbuf, acc_y, acc_d, sem = refs[-5:]
    step = pl.program_id(0)
    n_blocks = pl.num_programs(0)
    b = step + base
    n_exp = rows_ref.shape[1]
    slot = lax.rem(step, 2)

    def total(blk):
        return start_ref[blk, n_exp - 1] + rows_ref[blk, n_exp - 1]

    def fetch(blk, which):
        def one(e, carry):
            n = pl.multiple_of(rows_ref[blk, e], ALIGN)
            dst = pl.multiple_of(start_ref[blk, e], ALIGN)
            src = pl.multiple_of(off_ref[blk, e], ALIGN)

            @pl.when(n > 0)
            def _():
                pltpu.make_async_copy(y_hbm.at[e, pl.ds(src, n), :], ybuf.at[which, pl.ds(dst, n), :], sem.at[0, which]).start()
                pltpu.make_async_copy(dr_hbm.at[e, pl.ds(src, n), :], dbuf.at[which, pl.ds(dst, n), :], sem.at[1, which]).start()

            return carry

        lax.fori_loop(0, n_exp, one, 0)

    @pl.when(step == 0)
    def _():
        ybuf[...] = jnp.zeros(ybuf.shape, BF16)
        dbuf[...] = jnp.zeros(dbuf.shape, BF16)
        fetch(b, 0)

    @pl.when(step + 1 < n_blocks)
    def _():
        fetch(b + 1, 1 - slot)

    n = pl.multiple_of(total(b), ALIGN)

    @pl.when(n > 0)
    def _():
        pltpu.make_async_copy(ybuf.at[slot, pl.ds(0, n), :], ybuf.at[slot, pl.ds(0, n), :], sem.at[0, slot]).wait()
        pltpu.make_async_copy(dbuf.at[slot, pl.ds(0, n), :], dbuf.at[slot, pl.ds(0, n), :], sem.at[1, slot]).wait()

    acc_y[...] = jnp.zeros(acc_y.shape, F32)
    acc_d[...] = jnp.zeros(acc_d.shape, F32)

    def tile(i, carry):
        first = pl.multiple_of(i * TILE, TILE)
        picked, ones = one_hot(dest_ref, gate_ref, first)
        acc_y[...] += tn_dot(picked, ybuf[slot, pl.ds(first, TILE), :])
        acc_d[...] += tn_dot(ones, dbuf[slot, pl.ds(first, TILE), :])
        return carry

    lax.fori_loop(0, (n + (TILE - 1)) // TILE, tile, 0)

    if not own:
        out_y, out_d = refs[:2]
        out_y[...] = acc_y[...]
        out_d[...] = acc_d[...]
        return
    more_y, more_d, h_ref, dout_ref, out_ref, dh_ref = refs[:6]
    hf = h_ref[...].astype(F32)
    out_ref[...] = (hf + (acc_y[...] + more_y[...])).astype(BF16)
    d_u = (acc_d[...] + more_d[...]).astype(BF16).astype(F32)
    inv = lax.rsqrt(jnp.mean(hf * hf, axis=-1, keepdims=True) + EPS)
    proj = jnp.mean(d_u * hf, axis=-1, keepdims=True)
    d_norm = (d_u * inv - hf * (inv * inv * inv * proj)).astype(BF16).astype(F32)
    dh_ref[...] = (dout_ref[...].astype(F32) + d_norm).astype(BF16)


def combine(y_rows, dr_rows, dest, gate, segs, base, n_blocks, extra):
    n_local, _, d_model = y_rows.shape
    top_k = dest.shape[1]
    buf_rows = block_rows(top_k, n_local)
    tok_spec = pl.BlockSpec((BLOCK, d_model), lambda b, *_: (b, 0))
    map_spec = pl.BlockSpec((1, top_k, BLOCK), lambda b, *_: (b + base, 0, 0))
    hbm = pl.BlockSpec(memory_space=pl.ANY)
    out = jax.ShapeDtypeStruct((n_blocks * BLOCK, d_model), BF16 if extra else F32)
    return pl.pallas_call(
        functools.partial(combine_kernel, base=base, own=bool(extra)),
        grid_spec=pltpu.PrefetchScalarGridSpec(
            num_scalar_prefetch=3,
            grid=(n_blocks,),
            in_specs=[hbm, hbm, map_spec, map_spec] + [tok_spec] * len(extra),
            out_specs=[tok_spec, tok_spec],
            scratch_shapes=[
                pltpu.VMEM((2, buf_rows, d_model), BF16),
                pltpu.VMEM((2, buf_rows, d_model), BF16),
                pltpu.VMEM((BLOCK, d_model), F32),
                pltpu.VMEM((BLOCK, d_model), F32),
                pltpu.SemaphoreType.DMA((2, 2)),
            ],
        ),
        out_shape=[out, out],
        name='combine',
        **settings(45, 120),
    )(*segs, y_rows, dr_rows, dest, gate, *extra)


def place_kernel(*refs, n_parts):
    for k, out_ref in enumerate(refs[-3:]):
        value = refs[0][k]
        for part_ref in refs[1:n_parts]:
            value = value + part_ref[k]
        out_ref[...] = value


def place(parts, held, first, n_total):
    three, size, rows, cols = parts[0].shape
    hbm = pl.BlockSpec(memory_space=pl.ANY)
    return pl.pallas_call(
        functools.partial(place_kernel, n_parts=len(parts)),
        grid=(size,),
        in_specs=[pl.BlockSpec((three, 1, rows, cols), lambda i: (0, i, 0, 0))] * len(parts) + [hbm] * len(held),
        out_specs=[pl.BlockSpec((1, rows, cols), lambda i: (first + i, 0, 0))] * three,
        out_shape=[jax.ShapeDtypeStruct((n_total, rows, cols), F32)] * three,
        input_output_aliases={len(parts) + k: k for k in range(len(held))},
        name='place',
        **settings(1, 12),
    )(*parts, *held)


CHUNKS = (2, 4)
CORES = 2


def solution(mesh):
    ep_size, fsdp_size = mesh.shape['ep'], mesh.shape['fsdp']
    tok_spec = P(('data', 'fsdp', 'ep'))
    in_specs = (tok_spec, P('fsdp'), P(None, None, 'fsdp'), P('ep', 'fsdp'), P('ep', 'fsdp'), P('ep', None, 'fsdp'), tok_spec, tok_spec, tok_spec, tok_spec)
    out_specs = (tok_spec, tok_spec, P(('data', 'ep'), 'fsdp'), P(('data', 'ep'), 'fsdp'), P(('data', 'ep'), None, 'fsdp'))

    def device_fn(tokens, w_qkv, w_out, w_gate, w_up, w_down, expert_idx, expert_slot, gate_wts, d_out):
        n_seq, seq_len, d_model = tokens.shape
        tok_count = n_seq * seq_len
        top_k = expert_idx.shape[2]
        local_experts, half, _ = w_gate.shape
        num_experts = local_experts * ep_size
        n_side = ep_size // CORES
        n_local = local_experts * n_side
        n_blocks = tok_count // BLOCK
        capacity = capacity_of(tok_count, top_k, num_experts)
        max_rows = -(-(CORES * (capacity + n_blocks * (ALIGN - 1))) // TILE) * TILE
        ep = lax.axis_index('ep')
        groups = [[c + CORES * i for i in range(fsdp_size * n_side)] for c in range(CORES)]

        fsdp, side = lax.axis_index('fsdp'), ep // CORES
        flips = jnp.stack([fsdp, side]).astype(jnp.int32)

        def swap(values):
            return lax.ppermute(values, 'ep', [(i, i ^ 1) for i in range(ep_size)])

        def swap_x(values):
            return lax.ppermute(values, 'ep', [(i, i ^ CORES) for i in range(ep_size)])

        def swap_y(values):
            return lax.ppermute(values, 'fsdp', [(i, i ^ 1) for i in range(fsdp_size)])

        def own_weights(part):
            return jnp.stack([w_gate[part], w_up[part], w_down[part]], axis=0)

        _, head_dim, _ = w_out.shape
        qkv_rows = w_qkv.transpose(1, 2, 3, 0).reshape(-1, half)
        qkv_rows = lax.dynamic_slice_in_dim(qkv_rows, ep * (3 * d_model // ep_size), 3 * d_model // ep_size, axis=0)
        out_rows = lax.dynamic_slice_in_dim(w_out.reshape(-1, half), ep * (d_model // ep_size), d_model // ep_size, axis=0)
        attn_w = lax.all_gather(jnp.concatenate([qkv_rows, out_rows], axis=0), ('fsdp', 'ep'), axis=0, tiled=False)
        attn_w = attn_w.reshape(fsdp_size, ep_size, -1, half)
        weights, first = [], 0
        for size in CHUNKS:
            mine = own_weights(slice(first, first + size))
            full = lax.all_gather(mine, ('fsdp', 'ep'), axis=0, tiled=False, axis_index_groups=groups)
            weights.append(full)
            first += size
        mid = first + (local_experts - first) // 2
        attn_w, w_a, w_b = lax.optimization_barrier((attn_w, own_weights(slice(first, mid)), own_weights(slice(mid, local_experts))))
        w_ax, w_ay, w_bx, w_by = swap_x(w_a), swap_y(w_a), swap_x(w_b), swap_y(w_b)

        dout_tok = d_out.reshape(tok_count, d_model)
        dout_other = swap(dout_tok)
        kept_ids = jnp.where(expert_slot >= 0, expert_idx, -1).transpose(0, 2, 1)
        all_ids = jnp.concatenate([kept_ids, swap(kept_ids)], axis=0)
        owner = all_ids // local_experts
        mine_too = (all_ids >= 0) & (lax.rem(owner, CORES) == lax.rem(ep, CORES))
        local_ids = jnp.where(mine_too, owner // CORES * local_experts + lax.rem(all_ids, local_experts), -1)
        dest, segs = route(local_ids, n_local)
        counts = jnp.sum(segs[1], axis=0)
        gate = gate_wts.transpose(0, 2, 1)
        gate = jnp.concatenate([gate, swap(gate)], axis=0)
        gate = gate.reshape(2 * n_seq, top_k, seq_len // BLOCK, BLOCK).transpose(0, 2, 1, 3).reshape(2 * n_blocks, top_k, BLOCK)

        tokens, dest, segs, counts, gate = lax.optimization_barrier((tokens, dest, segs, counts, gate))
        h_seq, qkv = attention(tokens, attn_w, head_dim)
        w_axy, w_byx = swap_y(w_ax), swap_x(w_by)
        w_a = jnp.stack([w_a, w_ax, w_ay, w_axy])
        w_b = jnp.stack([w_b, w_bx, w_by, w_byx])
        h_tok = h_seq.reshape(tok_count, d_model)
        h_other = swap(h_tok)
        held = dispatch(h_tok, dout_tok, dest, gate, segs, 0, [], n_local, max_rows)
        rows, d_rows = dispatch(h_other, dout_other, dest, gate, segs, n_blocks, held, n_local, max_rows)
        rows, d_rows, d_a = experts(rows, d_rows, w_a, counts, flips, first, local_experts, x_first=True)
        more_a = swap_x(d_a[1])
        rows, d_rows, d_b = experts(rows, d_rows, w_b, counts, flips, mid, local_experts)
        more_b = swap_y(d_b[1])
        d_a, d_b = d_a[0] + more_a, d_b[0] + more_b
        more_a, more_b = swap_y(d_a[1]), swap_x(d_b[1])
        done, start = [([d_a[0], more_a], first), ([d_b[0], more_b], mid)], 0
        for n, size in enumerate(CHUNKS):
            rows, d_rows, d_w = experts(rows, d_rows, weights[n], counts, jnp.zeros_like(flips), start, local_experts)
            d_w = d_w.reshape(fsdp_size * n_side, *d_w.shape[2:])
            d_w = lax.psum_scatter(d_w, ('fsdp', 'ep'), scatter_dimension=0, tiled=False, axis_index_groups=groups)
            done.insert(0 if n == 0 else len(done), ([d_w], start))
            start += size
        sums = combine(rows, d_rows, dest, gate, segs, n_blocks, n_blocks, [])
        more = [swap(value) for value in sums]
        layer_out, d_h = combine(rows, d_rows, dest, gate, segs, 0, n_blocks, [*more, h_tok, dout_tok])
        d_tokens = attention_grad(d_h.reshape(n_seq, seq_len, d_model), tokens, qkv, attn_w, head_dim)
        d_ws = []
        for parts, where in done:
            d_ws = place(parts, d_ws, where, local_experts)
        return layer_out.reshape(n_seq, seq_len, d_model), d_tokens, *d_ws

    return jax.shard_map(device_fn, mesh=mesh, in_specs=in_specs, out_specs=out_specs, check_vma=False)
```

```python
import functools
import math

import jax
import jax.numpy as jnp
from jax import lax
from jax.experimental import pallas as pl
from jax.experimental.pallas import tpu as pltpu
from jax.sharding import PartitionSpec as P


F32 = jnp.float32
BF16 = jnp.bfloat16
BLOCK = 256
TILE = 256
ALIGN = 16
LANES = 128
LOG2E = math.log2(math.e)
EPS = 1e-6
VMEM_BYTES = 60 * 2 ** 20


def settings(gflop, mbytes):
    return {
        'compiler_params': pltpu.CompilerParams(dimension_semantics=('arbitrary',), vmem_limit_bytes=VMEM_BYTES),
        'cost_estimate': pl.CostEstimate(flops=gflop * 10 ** 9, bytes_accessed=mbytes * 10 ** 6, transcendentals=0),
    }


def nt_dot(lhs, rhs):
    return lax.dot_general(lhs, rhs, (((1,), (1,)), ((), ())), preferred_element_type=F32)


def tn_dot(lhs, rhs):
    return lax.dot_general(lhs, rhs, (((0,), (0,)), ((), ())), preferred_element_type=F32)


def lanes_of(head, values):
    lane = lax.broadcasted_iota(jnp.int32, values.shape, 1)
    return jnp.where((lane >= LANES // 2) == bool(head), values, jnp.zeros_like(values))


def attention_kernel(x_ref, w_ref, h_ref, qkv_ref, ctx, *, head_dim):
    seq_len, d_model = x_ref.shape[1:]
    n_fsdp, n_ep, rows, half = w_ref.shape
    n_qkv = rows * 3 // 4
    x = x_ref[0].astype(F32)
    normed = (x * lax.rsqrt(jnp.mean(x * x, axis=-1, keepdims=True) + EPS)).astype(BF16)
    for p in range(n_ep):
        part = nt_dot(normed[:, :half], w_ref[0, p, :n_qkv]) + nt_dot(normed[:, half:], w_ref[1, p, :n_qkv])
        qkv_ref[0, :, p * n_qkv:(p + 1) * n_qkv] = part.astype(BF16)
    scale = head_dim ** -0.5 * LOG2E

    def pair(i, carry):
        q2, k2, v2 = (qkv_ref[0, :, pl.ds(pl.multiple_of(t * d_model + i * LANES, LANES), LANES)] for t in range(3))
        for first in range(0, seq_len, BLOCK):
            end = first + BLOCK
            keys, vals = k2[:end], v2[:end]
            causal = lax.broadcasted_iota(jnp.int32, (BLOCK, end), 0) + first >= lax.broadcasted_iota(jnp.int32, (BLOCK, end), 1)
            both = []
            for head in range(2):
                scores = nt_dot(lanes_of(head, q2[first:end]), keys) * scale
                scores = jnp.where(causal, scores, -1e30)
                probs = jnp.exp2(scores - jnp.max(scores, axis=-1, keepdims=True))
                probs = (probs * (1.0 / jnp.sum(probs, axis=-1, keepdims=True))).astype(BF16)
                both.append(jnp.dot(probs, vals, preferred_element_type=F32))
            lane = lax.broadcasted_iota(jnp.int32, (BLOCK, LANES), 1)
            ctx[first:end, pl.ds(pl.multiple_of(i * LANES, LANES), LANES)] = jnp.where(lane < LANES // 2, both[0], both[1]).astype(BF16)
        return carry

    lax.fori_loop(0, d_model // LANES, pair, 0)
    for f in range(n_fsdp):
        w_out = jnp.concatenate([w_ref[f, p, n_qkv:] for p in range(n_ep)], axis=0)
        cols = slice(f * half, (f + 1) * half)
        h_ref[0, :, cols] = (x_ref[0, :, cols].astype(F32) + jnp.dot(ctx[...], w_out, preferred_element_type=F32)).astype(BF16)


def attention(tokens, weights, head_dim):
    n_seq, seq_len, d_model = tokens.shape
    seq_spec = pl.BlockSpec((1, seq_len, d_model), lambda s: (s, 0, 0))
    qkv_spec = pl.BlockSpec((1, seq_len, 3 * d_model), lambda s: (s, 0, 0))
    w_spec = pl.BlockSpec(weights.shape, lambda s: (0, 0, 0, 0))
    return pl.pallas_call(
        functools.partial(attention_kernel, head_dim=head_dim),
        grid=(n_seq,),
        in_specs=[seq_spec, w_spec],
        out_specs=[seq_spec, qkv_spec],
        out_shape=[jax.ShapeDtypeStruct(tokens.shape, BF16), jax.ShapeDtypeStruct((n_seq, seq_len, 3 * d_model), BF16)],
        scratch_shapes=[pltpu.VMEM((seq_len, d_model), BF16)],
        name='attention',
        **settings(90, 60),
    )(tokens, weights)


def attention_grad_kernel(dh_ref, x_ref, qkv_ref, w_ref, dx_ref, dctx, dqkv, *, head_dim):
    seq_len, d_model = x_ref.shape[1:]
    n_fsdp, n_ep, rows, half = w_ref.shape
    n_qkv = rows * 3 // 4
    n_out = rows - n_qkv
    dh = dh_ref[0]
    for p in range(n_ep):
        part = nt_dot(dh[:, :half], w_ref[0, p, n_qkv:]) + nt_dot(dh[:, half:], w_ref[1, p, n_qkv:])
        dctx[:, p * n_out:(p + 1) * n_out] = part.astype(BF16)
    scale = head_dim ** -0.5

    def pair(i, carry):
        col = pl.multiple_of(i * LANES, LANES)
        q2, k2, v2 = (qkv_ref[0, :, pl.ds(pl.multiple_of(t * d_model + i * LANES, LANES), LANES)] for t in range(3))
        d2 = dctx[:, pl.ds(col, LANES)]
        dk = [jnp.zeros((BLOCK, LANES), F32)] * (seq_len // BLOCK)
        dv = list(dk)
        for first in range(0, seq_len, BLOCK):
            end = first + BLOCK
            keys, vals = k2[:end], v2[:end]
            causal = lax.broadcasted_iota(jnp.int32, (end, BLOCK), 1) + first >= lax.broadcasted_iota(jnp.int32, (end, BLOCK), 0)
            dq = jnp.zeros((BLOCK, LANES), F32)
            for head in range(2):
                q, d = lanes_of(head, q2[first:end]), lanes_of(head, d2[first:end])
                scores = jnp.where(causal, nt_dot(keys, q) * (scale * LOG2E), -1e30)
                probs = jnp.exp2(scores - jnp.max(scores, axis=0, keepdims=True))
                probs = probs * (1.0 / jnp.sum(probs, axis=0, keepdims=True))
                d_probs = nt_dot(vals, d)
                d_scores = probs * (d_probs - jnp.sum(probs * d_probs, axis=0, keepdims=True))
                d_scores = (d_scores * scale).astype(BF16)
                dv_part = jnp.dot(probs.astype(BF16), d, preferred_element_type=F32)
                dk_part = jnp.dot(d_scores, q, preferred_element_type=F32)
                dq = dq + tn_dot(d_scores, lanes_of(head, keys))
                for n in range(end // BLOCK):
                    dk[n] = dk[n] + dk_part[n * BLOCK:(n + 1) * BLOCK]
                    dv[n] = dv[n] + dv_part[n * BLOCK:(n + 1) * BLOCK]
            dqkv[first:end, pl.ds(col, LANES)] = dq.astype(BF16)
        for n in range(seq_len // BLOCK):
            dqkv[n * BLOCK:(n + 1) * BLOCK, pl.ds(pl.multiple_of(d_model + i * LANES, LANES), LANES)] = dk[n].astype(BF16)
            dqkv[n * BLOCK:(n + 1) * BLOCK, pl.ds(pl.multiple_of(2 * d_model + i * LANES, LANES), LANES)] = dv[n].astype(BF16)
        return carry

    lax.fori_loop(0, d_model // LANES, pair, 0)
    x = x_ref[0].astype(F32)
    d_normed = []
    for f in range(n_fsdp):
        w_qkv = jnp.concatenate([w_ref[f, p, :n_qkv] for p in range(n_ep)], axis=0)
        d_normed.append(jnp.dot(dqkv[...], w_qkv, preferred_element_type=F32).astype(BF16))
    d_normed = jnp.concatenate(d_normed, axis=1).astype(F32)
    inv = lax.rsqrt(jnp.mean(x * x, axis=-1, keepdims=True) + EPS)
    proj = jnp.mean(d_normed * x, axis=-1, keepdims=True)
    d_x = (d_normed * inv - x * (inv * inv * inv * proj)).astype(BF16).astype(F32)
    dx_ref[0] = (dh_ref[0].astype(F32) + d_x).astype(BF16)


def attention_grad(d_h, tokens, qkv, weights, head_dim):
    n_seq, seq_len, d_model = tokens.shape
    seq_spec = pl.BlockSpec((1, seq_len, d_model), lambda s: (s, 0, 0))
    qkv_spec = pl.BlockSpec((1, seq_len, 3 * d_model), lambda s: (s, 0, 0))
    w_spec = pl.BlockSpec(weights.shape, lambda s: (0, 0, 0, 0))
    return pl.pallas_call(
        functools.partial(attention_grad_kernel, head_dim=head_dim),
        grid=(n_seq,),
        in_specs=[seq_spec, seq_spec, qkv_spec, w_spec],
        out_specs=seq_spec,
        out_shape=jax.ShapeDtypeStruct(tokens.shape, BF16),
        scratch_shapes=[pltpu.VMEM((seq_len, d_model), BF16), pltpu.VMEM((seq_len, 3 * d_model), BF16)],
        name='attention_grad',
        **settings(150, 70),
    )(d_h, tokens, qkv, weights)


def capacity_of(tok_count, top_k, num_experts):
    return max(8, (5 * tok_count * top_k // (4 * num_experts) + 7) // 8 * 8)


def route_kernel(loc_ref, dest_ref, start_ref, rows_ref, off_ref, total, *, n_local):
    top_k = loc_ref.shape[1]
    ids = lax.broadcasted_iota(jnp.int32, (n_local, BLOCK), 0)
    upper = (lax.broadcasted_iota(jnp.int32, (BLOCK, BLOCK), 0) <= lax.broadcasted_iota(jnp.int32, (BLOCK, BLOCK), 1)).astype(F32).astype(BF16)
    before = (lax.broadcasted_iota(jnp.int32, (n_local, n_local), 0) > lax.broadcasted_iota(jnp.int32, (n_local, n_local), 1)).astype(F32).astype(BF16)

    @pl.when(pl.program_id(0) == 0)
    def _():
        total[...] = jnp.zeros(total.shape, jnp.int32)

    so_far = total[...]
    for s in range(loc_ref.shape[0]):
        for p in range(loc_ref.shape[2] // BLOCK):
            q = s * (loc_ref.shape[2] // BLOCK) + p
            loc = loc_ref[s, :, p * BLOCK:(p + 1) * BLOCK]
            member = jnp.zeros((n_local, BLOCK), F32)
            for j in range(top_k):
                member = jnp.where(loc[j:j + 1] == ids, 1.0, member)
            count = jnp.dot(member.astype(BF16), upper, preferred_element_type=F32)
            units = (count[:, BLOCK - 1:].astype(jnp.int32) + (ALIGN - 1)) // ALIGN
            units = jnp.broadcast_to(units, (n_local, LANES))
            start = jnp.dot(before, units.astype(F32).astype(BF16), preferred_element_type=F32).astype(jnp.int32) * ALIGN
            place = start[:, :1] + count.astype(jnp.int32) - 1
            for j in range(top_k):
                row = jnp.sum(jnp.where(loc[j:j + 1] == ids, place, 0), axis=0, keepdims=True)
                dest_ref[q, j:j + 1, :] = jnp.where(loc[j:j + 1] >= 0, row, -1)
            start_ref[q] = start
            rows_ref[q] = units * ALIGN
            off_ref[q] = so_far
            so_far = so_far + units * ALIGN
    total[...] = so_far


def route(local_ids, n_local):
    n_seq, top_k, seq_len = local_ids.shape
    per_seq = seq_len // BLOCK
    step = 2 if n_seq % 2 == 0 else 1
    n_blocks = n_seq * per_seq
    seg = jax.ShapeDtypeStruct((n_blocks, n_local, LANES), jnp.int32)
    seg_spec = pl.BlockSpec((step * per_seq, n_local, LANES), lambda s: (s, 0, 0))
    dest, *segs = pl.pallas_call(
        functools.partial(route_kernel, n_local=n_local),
        grid=(n_seq // step,),
        in_specs=[pl.BlockSpec((step, top_k, seq_len), lambda s: (s, 0, 0))],
        out_specs=[pl.BlockSpec((step * per_seq, top_k, BLOCK), lambda s: (s, 0, 0)), seg_spec, seg_spec, seg_spec],
        out_shape=[jax.ShapeDtypeStruct((n_blocks, top_k, BLOCK), jnp.int32), seg, seg, seg],
        scratch_shapes=[pltpu.VMEM((n_local, LANES), jnp.int32)],
        name='route',
        **settings(1, 3),
    )(local_ids)
    return dest, [part[:, :, 0] for part in segs]


def one_hot(dest_ref, gate_ref, first_row):
    rows = lax.broadcasted_iota(jnp.int32, (TILE, BLOCK), 0).astype(F32).astype(BF16)
    dest = jnp.clip(dest_ref[0] - first_row, -1, TILE).astype(F32).astype(BF16)
    gate = gate_ref[0]
    picked = jnp.zeros((TILE, BLOCK), BF16)
    for j in range(dest.shape[0]):
        picked = jnp.where(rows == dest[j:j + 1], gate[j:j + 1], picked)
    return picked, jnp.where(picked > 0, jnp.ones_like(picked), jnp.zeros_like(picked))


def dispatch_kernel(start_ref, rows_ref, off_ref, h_ref, dout_ref, dest_ref, gate_ref, *refs, base):
    r_hbm, d_hbm, u_s, rbuf, dbuf, sem = refs[-6:]
    step = pl.program_id(0)
    n_blocks = pl.num_programs(0)
    b = step + base
    n_exp = rows_ref.shape[1]
    slot = lax.rem(b, 2)

    def total(blk):
        return start_ref[blk, n_exp - 1] + rows_ref[blk, n_exp - 1]

    def drain(blk, which):
        n = pl.multiple_of(total(blk), ALIGN)

        @pl.when(n > 0)
        def _():
            pltpu.make_async_copy(rbuf.at[which, pl.ds(0, n), :], rbuf.at[which, pl.ds(0, n), :], sem.at[0, which]).wait()
            pltpu.make_async_copy(dbuf.at[which, pl.ds(0, n), :], dbuf.at[which, pl.ds(0, n), :], sem.at[1, which]).wait()

    @pl.when(step >= 2)
    def _():
        drain(b - 2, slot)

    hf = h_ref[...].astype(F32)
    u_s[...] = (hf * lax.rsqrt(jnp.mean(hf * hf, axis=-1, keepdims=True) + EPS)).astype(BF16)

    def tile(i, carry):
        first = pl.multiple_of(i * TILE, TILE)
        picked, ones = one_hot(dest_ref, gate_ref, first)
        rbuf[slot, pl.ds(first, TILE), :] = jnp.dot(ones, u_s[...], preferred_element_type=F32).astype(BF16)
        dbuf[slot, pl.ds(first, TILE), :] = jnp.dot(picked, dout_ref[...], preferred_element_type=F32).astype(BF16)
        return carry

    lax.fori_loop(0, (total(b) + (TILE - 1)) // TILE, tile, 0)

    def send(e, carry):
        n = pl.multiple_of(rows_ref[b, e], ALIGN)
        src = pl.multiple_of(start_ref[b, e], ALIGN)
        dst = pl.multiple_of(off_ref[b, e], ALIGN)

        @pl.when(n > 0)
        def _():
            pltpu.make_async_copy(rbuf.at[slot, pl.ds(src, n), :], r_hbm.at[e, pl.ds(dst, n), :], sem.at[0, slot]).start()
            pltpu.make_async_copy(dbuf.at[slot, pl.ds(src, n), :], d_hbm.at[e, pl.ds(dst, n), :], sem.at[1, slot]).start()

        return carry

    lax.fori_loop(0, n_exp, send, 0)

    @pl.when(step == n_blocks - 1)
    def _():
        @pl.when(n_blocks > 1)
        def _():
            drain(b - 1, 1 - slot)

        drain(b, slot)


def block_rows(top_k, n_local):
    return -(-(BLOCK * top_k + n_local * (ALIGN - 1)) // TILE) * TILE


def dispatch(h_tok, dout_tok, dest, gate, segs, base, held, n_local, max_rows):
    tok_count, d_model = h_tok.shape
    top_k = dest.shape[1]
    n_blocks = tok_count // BLOCK
    buf_rows = block_rows(top_k, n_local)
    tok_spec = pl.BlockSpec((BLOCK, d_model), lambda b, *_: (b, 0))
    map_spec = pl.BlockSpec((1, top_k, BLOCK), lambda b, *_: (b + base, 0, 0))
    rows_shape = jax.ShapeDtypeStruct((n_local, max_rows, d_model), BF16)
    hbm = pl.BlockSpec(memory_space=pl.ANY)
    return pl.pallas_call(
        functools.partial(dispatch_kernel, base=base),
        grid_spec=pltpu.PrefetchScalarGridSpec(
            num_scalar_prefetch=3,
            grid=(n_blocks,),
            in_specs=[tok_spec, tok_spec, map_spec, map_spec] + [hbm] * len(held),
            out_specs=[hbm, hbm],
            scratch_shapes=[
                pltpu.VMEM((BLOCK, d_model), BF16),
                pltpu.VMEM((2, buf_rows, d_model), BF16),
                pltpu.VMEM((2, buf_rows, d_model), BF16),
                pltpu.SemaphoreType.DMA((2, 2)),
            ],
        ),
        out_shape=[rows_shape, rows_shape],
        input_output_aliases={7: 0, 8: 1} if held else {},
        name='dispatch',
        **settings(40, 90),
    )(*segs, h_tok, dout_tok, dest, gate, *held)


def expert_kernel(count_ref, flip_ref, r_hbm, d_hbm, w_lo, w_hi, y_hbm, dr_hbm, dw_ref, rbuf, dbuf, ybuf, drbuf, done, in_sem, out_sem, *, expert_of, x_first):
    step = pl.program_id(0)
    n_steps = pl.num_programs(0)
    expert = expert_of(step)
    n_rows = count_ref[expert]
    n_tiles = jnp.maximum((n_rows + (TILE - 1)) // TILE, 1)
    half = dw_ref.shape[-1]

    def copies(who, i, slot, load):
        rows = pl.ds(pl.multiple_of(i * TILE, TILE), TILE)
        pairs = ((r_hbm, rbuf), (d_hbm, dbuf)) if load else ((ybuf, y_hbm), (drbuf, dr_hbm))
        for k, (src, dst) in enumerate(pairs):
            src = src.at[who, rows, :] if load else src.at[slot]
            dst = dst.at[slot] if load else dst.at[who, rows, :]
            yield pltpu.make_async_copy(src, dst, (in_sem if load else out_sem).at[k, slot])

    def start(*args):
        for copy in copies(*args):
            copy.start()

    def wait(*args):
        for copy in copies(*args):
            copy.wait()

    @pl.when(step == 0)
    def _():
        done[0] = 0
        start(expert, 0, 0, True)

    before = done[0]
    for p in range(dw_ref.shape[0]):
        for q in range(dw_ref.shape[1]):
            for t in range(dw_ref.shape[2]):
                clear(dw_ref.at[p, q, t, 0])

    def tile(i, carry):
        slot = lax.rem(before + i, 2)

        @pl.when(i + 1 < n_tiles)
        def _():
            start(expert, i + 1, 1 - slot, True)

        @pl.when((i + 1 == n_tiles) & (step + 1 < n_steps))
        def _():
            start(expert_of(step + 1), 0, 1 - slot, True)

        wait(expert, i, slot, True)

        @pl.when(before + i >= 2)
        def _():
            wait(expert, i, slot, False)

        valid = lax.broadcasted_iota(jnp.int32, (TILE, 1), 0) + i * TILE < n_rows
        r = jnp.where(valid, rbuf[slot], 0)
        dy = jnp.where(valid, dbuf[slot], 0)
        w1, w3, w2 = (jnp.concatenate([w[0, t, 0] for w in (w_lo, w_hi)], axis=t // 2) for t in range(3))
        act_a = jnp.dot(r, w1, preferred_element_type=F32)
        act_b = jnp.dot(r, w3, preferred_element_type=F32)
        d_g = nt_dot(dy, w2)
        sig = 1.0 / (1.0 + jnp.exp(-act_a))
        silu = act_a * sig
        g = (silu * act_b).astype(BF16)
        d_up = (d_g * silu).astype(BF16)
        d_gate = (d_g * act_b * sig * (1.0 + act_a * (1.0 - sig))).astype(BF16)
        ybuf[slot] = jnp.dot(g, w2, preferred_element_type=F32).astype(BF16)
        drbuf[slot] = (nt_dot(d_gate, w1) + nt_dot(d_up, w3)).astype(BF16)
        start(expert, i, slot, False)
        for f in range(2):
            part = slice(f * half, (f + 1) * half)
            to = lax.rem(f + flip_ref[0], 2)
            for t, (lhs, rhs) in enumerate(((r[:, part], d_gate), (r[:, part], d_up), (g, dy[:, part]))):
                dw_ref[(0, to, t, 0) if x_first else (to, 0, t, 0)] += tn_dot(lhs, rhs)
        return carry

    lax.fori_loop(0, n_tiles, tile, 0)
    done[0] = before + n_tiles

    @pl.when(step == n_steps - 1)
    def _():
        last = before + n_tiles - 1
        wait(expert, 0, lax.rem(last, 2), False)

        @pl.when(last >= 1)
        def _():
            wait(expert, 0, lax.rem(last + 1, 2), False)


def experts(rows, d_rows, weights, counts, flips, first, local_experts, x_first=False):
    d_model = rows.shape[2]
    n_owners, three, size, half, _ = weights.shape
    n_fsdp = d_model // half
    n_side = n_owners // n_fsdp

    def expert_of(g):
        return g // size * local_experts + first + lax.rem(g, size)

    def side(g, flip):
        return lax.rem(g // size + flip[1], n_side)

    def w_spec(f):
        return pl.BlockSpec((1, three, 1, half, half), lambda g, _, flip: (lax.rem(f + flip[0], n_fsdp) * n_side + side(g, flip), 0, lax.rem(g, size), 0, 0))

    def dw_index(g, _, flip):
        place = (side(g, flip), 0) if x_first else (0, side(g, flip))
        return (*place, 0, lax.rem(g, size), 0, 0)

    hbm = pl.BlockSpec(memory_space=pl.ANY)
    grads = (n_side, n_fsdp) if x_first else (n_fsdp, n_side)
    dw_block = (1, n_fsdp) if x_first else (n_fsdp, 1)
    return pl.pallas_call(
        functools.partial(expert_kernel, expert_of=expert_of, x_first=x_first),
        grid_spec=pltpu.PrefetchScalarGridSpec(
            num_scalar_prefetch=2,
            grid=(n_side * size,),
            in_specs=[hbm, hbm, w_spec(0), w_spec(1)],
            out_specs=[hbm, hbm, pl.BlockSpec((*dw_block, three, 1, half, half), dw_index)],
            scratch_shapes=[pltpu.VMEM((2, TILE, d_model), BF16)] * 4 + [pltpu.SMEM((1,), jnp.int32)] + [pltpu.SemaphoreType.DMA((2, 2))] * 2,
        ),
        out_shape=[jax.ShapeDtypeStruct(rows.shape, BF16)] * 2 + [jax.ShapeDtypeStruct((*grads, three, size, half, half), F32)],
        input_output_aliases={2: 0, 3: 1},
        name='experts',
        **settings(56 * size, 100 * size),
    )(counts, flips, rows, d_rows, weights, weights)


def clear(ref):
    def rows(i, carry):
        ref[pl.ds(pl.multiple_of(i * LANES, LANES), LANES), :] = jnp.zeros((LANES, ref.shape[1]), ref.dtype)
        return carry

    lax.fori_loop(0, ref.shape[0] // LANES, rows, 0)


def combine_kernel(start_ref, rows_ref, off_ref, y_hbm, dr_hbm, dest_ref, gate_ref, *refs, base, own):
    ybuf, dbuf, acc_y, acc_d, sem = refs[-5:]
    step = pl.program_id(0)
    n_blocks = pl.num_programs(0)
    b = step + base
    n_exp = rows_ref.shape[1]
    slot = lax.rem(step, 2)

    def total(blk):
        return start_ref[blk, n_exp - 1] + rows_ref[blk, n_exp - 1]

    def fetch(blk, which):
        def one(e, carry):
            n = pl.multiple_of(rows_ref[blk, e], ALIGN)
            dst = pl.multiple_of(start_ref[blk, e], ALIGN)
            src = pl.multiple_of(off_ref[blk, e], ALIGN)

            @pl.when(n > 0)
            def _():
                pltpu.make_async_copy(y_hbm.at[e, pl.ds(src, n), :], ybuf.at[which, pl.ds(dst, n), :], sem.at[0, which]).start()
                pltpu.make_async_copy(dr_hbm.at[e, pl.ds(src, n), :], dbuf.at[which, pl.ds(dst, n), :], sem.at[1, which]).start()

            return carry

        lax.fori_loop(0, n_exp, one, 0)

    @pl.when(step == 0)
    def _():
        for which in range(2):
            clear(ybuf.at[which])
            clear(dbuf.at[which])
        fetch(b, 0)

    @pl.when(step + 1 < n_blocks)
    def _():
        fetch(b + 1, 1 - slot)

    n = pl.multiple_of(total(b), ALIGN)

    @pl.when(n > 0)
    def _():
        pltpu.make_async_copy(ybuf.at[slot, pl.ds(0, n), :], ybuf.at[slot, pl.ds(0, n), :], sem.at[0, slot]).wait()
        pltpu.make_async_copy(dbuf.at[slot, pl.ds(0, n), :], dbuf.at[slot, pl.ds(0, n), :], sem.at[1, slot]).wait()

    acc_y[...] = jnp.zeros(acc_y.shape, F32)
    acc_d[...] = jnp.zeros(acc_d.shape, F32)

    def tile(i, carry):
        first = pl.multiple_of(i * TILE, TILE)
        picked, ones = one_hot(dest_ref, gate_ref, first)
        acc_y[...] += tn_dot(picked, ybuf[slot, pl.ds(first, TILE), :])
        acc_d[...] += tn_dot(ones, dbuf[slot, pl.ds(first, TILE), :])
        return carry

    lax.fori_loop(0, (n + (TILE - 1)) // TILE, tile, 0)

    if not own:
        out_y, out_d = refs[:2]
        out_y[...] = acc_y[...]
        out_d[...] = acc_d[...]
        return
    more_y, more_d, h_ref, dout_ref, out_ref, dh_ref = refs[:6]
    hf = h_ref[...].astype(F32)
    out_ref[...] = (hf + (acc_y[...] + more_y[...])).astype(BF16)
    d_u = (acc_d[...] + more_d[...]).astype(BF16).astype(F32)
    inv = lax.rsqrt(jnp.mean(hf * hf, axis=-1, keepdims=True) + EPS)
    proj = jnp.mean(d_u * hf, axis=-1, keepdims=True)
    d_norm = (d_u * inv - hf * (inv * inv * inv * proj)).astype(BF16).astype(F32)
    dh_ref[...] = (dout_ref[...].astype(F32) + d_norm).astype(BF16)


def combine(y_rows, dr_rows, dest, gate, segs, base, n_blocks, extra):
    n_local, _, d_model = y_rows.shape
    top_k = dest.shape[1]
    buf_rows = block_rows(top_k, n_local)
    tok_spec = pl.BlockSpec((BLOCK, d_model), lambda b, *_: (b, 0))
    map_spec = pl.BlockSpec((1, top_k, BLOCK), lambda b, *_: (b + base, 0, 0))
    hbm = pl.BlockSpec(memory_space=pl.ANY)
    out = jax.ShapeDtypeStruct((n_blocks * BLOCK, d_model), BF16 if extra else F32)
    return pl.pallas_call(
        functools.partial(combine_kernel, base=base, own=bool(extra)),
        grid_spec=pltpu.PrefetchScalarGridSpec(
            num_scalar_prefetch=3,
            grid=(n_blocks,),
            in_specs=[hbm, hbm, map_spec, map_spec] + [tok_spec] * len(extra),
            out_specs=[tok_spec, tok_spec],
            scratch_shapes=[
                pltpu.VMEM((2, buf_rows, d_model), BF16),
                pltpu.VMEM((2, buf_rows, d_model), BF16),
                pltpu.VMEM((BLOCK, d_model), F32),
                pltpu.VMEM((BLOCK, d_model), F32),
                pltpu.SemaphoreType.DMA((2, 2)),
            ],
        ),
        out_shape=[out, out],
        name='combine',
        **settings(45, 120),
    )(*segs, y_rows, dr_rows, dest, gate, *extra)


def place_kernel(*refs, n_parts):
    for k, out_ref in enumerate(refs[-3:]):
        value = refs[0][k]
        for part_ref in refs[1:n_parts]:
            value = value + part_ref[k]
        out_ref[...] = value


def place(parts, held, first, n_total):
    three, size, rows, cols = parts[0].shape
    hbm = pl.BlockSpec(memory_space=pl.ANY)
    return pl.pallas_call(
        functools.partial(place_kernel, n_parts=len(parts)),
        grid=(size,),
        in_specs=[pl.BlockSpec((three, 1, rows, cols), lambda i: (0, i, 0, 0))] * len(parts) + [hbm] * len(held),
        out_specs=[pl.BlockSpec((1, rows, cols), lambda i: (first + i, 0, 0))] * three,
        out_shape=[jax.ShapeDtypeStruct((n_total, rows, cols), F32)] * three,
        input_output_aliases={len(parts) + k: k for k in range(len(held))},
        name='place',
        **settings(1, 12),
    )(*parts, *held)


CHUNKS = (2, 4)
CORES = 2


def solution(mesh):
    ep_size, fsdp_size = mesh.shape['ep'], mesh.shape['fsdp']
    tok_spec = P(('data', 'fsdp', 'ep'))
    in_specs = (tok_spec, P('fsdp'), P(None, None, 'fsdp'), P('ep', 'fsdp'), P('ep', 'fsdp'), P('ep', None, 'fsdp'), tok_spec, tok_spec, tok_spec, tok_spec)
    out_specs = (tok_spec, tok_spec, P(('data', 'ep'), 'fsdp'), P(('data', 'ep'), 'fsdp'), P(('data', 'ep'), None, 'fsdp'))

    def device_fn(tokens, w_qkv, w_out, w_gate, w_up, w_down, expert_idx, expert_slot, gate_wts, d_out):
        n_seq, seq_len, d_model = tokens.shape
        tok_count = n_seq * seq_len
        top_k = expert_idx.shape[2]
        local_experts, half, _ = w_gate.shape
        num_experts = local_experts * ep_size
        n_side = ep_size // CORES
        n_local = local_experts * n_side
        n_blocks = tok_count // BLOCK
        capacity = capacity_of(tok_count, top_k, num_experts)
        max_rows = -(-(CORES * (capacity + n_blocks * (ALIGN - 1))) // TILE) * TILE
        ep = lax.axis_index('ep')
        groups = [[c + CORES * i for i in range(fsdp_size * n_side)] for c in range(CORES)]

        fsdp, side = lax.axis_index('fsdp'), ep // CORES
        flips = jnp.stack([fsdp, side]).astype(jnp.int32)

        def swap(values):
            return lax.ppermute(values, 'ep', [(i, i ^ 1) for i in range(ep_size)])

        def swap_x(values):
            return lax.ppermute(values, 'ep', [(i, i ^ CORES) for i in range(ep_size)])

        def swap_y(values):
            return lax.ppermute(values, 'fsdp', [(i, i ^ 1) for i in range(fsdp_size)])

        def own_weights(part):
            return jnp.stack([w_gate[part], w_up[part], w_down[part]], axis=0)

        _, head_dim, _ = w_out.shape
        qkv_rows = w_qkv.transpose(1, 2, 3, 0).reshape(-1, half)
        qkv_rows = lax.dynamic_slice_in_dim(qkv_rows, ep * (3 * d_model // ep_size), 3 * d_model // ep_size, axis=0)
        out_rows = lax.dynamic_slice_in_dim(w_out.reshape(-1, half), ep * (d_model // ep_size), d_model // ep_size, axis=0)
        attn_w = lax.all_gather(jnp.concatenate([qkv_rows, out_rows], axis=0), ('fsdp', 'ep'), axis=0, tiled=False)
        attn_w = attn_w.reshape(fsdp_size, ep_size, -1, half)
        weights, first = [], 0
        for size in CHUNKS:
            mine = own_weights(slice(first, first + size))
            full = lax.all_gather(mine, ('fsdp', 'ep'), axis=0, tiled=False, axis_index_groups=groups)
            weights.append(full)
            first += size
        mid = first + (local_experts - first) // 2
        w_a, w_b = own_weights(slice(first, mid)), own_weights(slice(mid, local_experts))
        w_ax, w_ay, w_bx, w_by = swap_x(w_a), swap_y(w_a), swap_x(w_b), swap_y(w_b)

        dout_tok = d_out.reshape(tok_count, d_model)
        dout_other = swap(dout_tok)
        kept_ids = jnp.where(expert_slot >= 0, expert_idx, -1).transpose(0, 2, 1)
        all_ids = jnp.concatenate([kept_ids, swap(kept_ids)], axis=0)
        owner = all_ids // local_experts
        mine_too = (all_ids >= 0) & (lax.rem(owner, CORES) == lax.rem(ep, CORES))
        local_ids = jnp.where(mine_too, owner // CORES * local_experts + lax.rem(all_ids, local_experts), -1)
        dest, segs = route(local_ids, n_local)
        counts = jnp.sum(segs[1], axis=0)
        gate = gate_wts.transpose(0, 2, 1)
        gate = jnp.concatenate([gate, swap(gate)], axis=0)
        gate = gate.reshape(2 * n_seq, top_k, seq_len // BLOCK, BLOCK).transpose(0, 2, 1, 3).reshape(2 * n_blocks, top_k, BLOCK)

        tokens, dest, segs, counts, gate = lax.optimization_barrier((tokens, dest, segs, counts, gate))
        h_seq, qkv = attention(tokens, attn_w, head_dim)
        w_axy, w_byx = swap_y(w_ax), swap_x(w_by)
        w_a = jnp.stack([w_a, w_ax, w_ay, w_axy])
        w_b = jnp.stack([w_b, w_bx, w_by, w_byx])
        h_tok = h_seq.reshape(tok_count, d_model)
        h_other = swap(h_tok)
        held = dispatch(h_tok, dout_tok, dest, gate, segs, 0, [], n_local, max_rows)
        rows, d_rows = dispatch(h_other, dout_other, dest, gate, segs, n_blocks, held, n_local, max_rows)
        rows, d_rows, d_a = experts(rows, d_rows, w_a, counts, flips, first, local_experts, x_first=True)
        more_a = swap_x(d_a[1])
        rows, d_rows, d_b = experts(rows, d_rows, w_b, counts, flips, mid, local_experts)
        more_b = swap_y(d_b[1])
        d_a, d_b = d_a[0] + more_a, d_b[0] + more_b
        more_a, more_b = swap_y(d_a[1]), swap_x(d_b[1])
        done, start = [([d_a[0], more_a], first), ([d_b[0], more_b], mid)], 0
        for n, size in enumerate(CHUNKS):
            rows, d_rows, d_w = experts(rows, d_rows, weights[n], counts, jnp.zeros_like(flips), start, local_experts)
            d_w = d_w.reshape(fsdp_size * n_side, *d_w.shape[2:])
            d_w = lax.psum_scatter(d_w, ('fsdp', 'ep'), scatter_dimension=0, tiled=False, axis_index_groups=groups)
            done.insert(0 if n == 0 else len(done), ([d_w], start))
            start += size
        sums = combine(rows, d_rows, dest, gate, segs, n_blocks, n_blocks, [])
        more = [swap(value) for value in sums]
        layer_out, d_h = combine(rows, d_rows, dest, gate, segs, 0, n_blocks, [*more, h_tok, dout_tok])
        d_tokens = attention_grad(d_h.reshape(n_seq, seq_len, d_model), tokens, qkv, attn_w, head_dim)
        d_ws = []
        for parts, where in done:
            d_ws = place(parts, d_ws, where, local_experts)
        return layer_out.reshape(n_seq, seq_len, d_model), d_tokens, *d_ws

    return jax.shard_map(device_fn, mesh=mesh, in_specs=in_specs, out_specs=out_specs, check_vma=False)
```

```python
import functools
import math

import jax
import jax.numpy as jnp
from jax import lax
from jax.experimental import pallas as pl
from jax.experimental.pallas import tpu as pltpu
from jax.sharding import PartitionSpec as P


F32 = jnp.float32
BF16 = jnp.bfloat16
BLOCK = 256
TILE = 256
ALIGN = 16
LANES = 128
LOG2E = math.log2(math.e)
EPS = 1e-6
VMEM_BYTES = 60 * 2 ** 20


def settings(gflop, mbytes):
    return {
        'compiler_params': pltpu.CompilerParams(dimension_semantics=('arbitrary',), vmem_limit_bytes=VMEM_BYTES),
        'cost_estimate': pl.CostEstimate(flops=gflop * 10 ** 9, bytes_accessed=mbytes * 10 ** 6, transcendentals=0),
    }


def nt_dot(lhs, rhs):
    return lax.dot_general(lhs, rhs, (((1,), (1,)), ((), ())), preferred_element_type=F32)


def tn_dot(lhs, rhs):
    return lax.dot_general(lhs, rhs, (((0,), (0,)), ((), ())), preferred_element_type=F32)


def lanes_of(head, values):
    lane = lax.broadcasted_iota(jnp.int32, values.shape, 1)
    return jnp.where((lane >= LANES // 2) == bool(head), values, jnp.zeros_like(values))


def attention_kernel(x_ref, w_ref, h_ref, qkv_ref, ctx, *, head_dim):
    seq_len, d_model = x_ref.shape[1:]
    n_fsdp, n_ep, rows, half = w_ref.shape
    n_qkv = rows * 3 // 4
    x = x_ref[0].astype(F32)
    normed = (x * lax.rsqrt(jnp.mean(x * x, axis=-1, keepdims=True) + EPS)).astype(BF16)
    for p in range(n_ep):
        part = nt_dot(normed[:, :half], w_ref[0, p, :n_qkv]) + nt_dot(normed[:, half:], w_ref[1, p, :n_qkv])
        qkv_ref[0, :, p * n_qkv:(p + 1) * n_qkv] = part.astype(BF16)
    scale = head_dim ** -0.5 * LOG2E

    diagonal = lax.broadcasted_iota(jnp.int32, (BLOCK, BLOCK), 1) >= lax.broadcasted_iota(jnp.int32, (BLOCK, BLOCK), 0)

    def pair(i, carry):
        q2, k2, v2 = (qkv_ref[0, :, pl.ds(pl.multiple_of(t * d_model + i * LANES, LANES), LANES)] for t in range(3))
        for first in range(0, seq_len, BLOCK):
            both = []
            for head in range(2):
                query = lanes_of(head, q2[first:first + BLOCK])
                parts = [nt_dot(k2[at:at + BLOCK], query) * scale for at in range(0, first + BLOCK, BLOCK)]
                parts[-1] = jnp.where(diagonal, parts[-1], -1e30)
                top = functools.reduce(jnp.maximum, [jnp.max(part, axis=0, keepdims=True) for part in parts])
                parts = [jnp.exp2(part - top) for part in parts]
                inverse = 1.0 / sum(jnp.sum(part, axis=0, keepdims=True) for part in parts)
                probs = jnp.concatenate([(part * inverse).astype(BF16) for part in parts], axis=0)
                both.append(tn_dot(v2[:first + BLOCK], probs))
            row = lax.broadcasted_iota(jnp.int32, (LANES, BLOCK), 0)
            ctx[pl.ds(pl.multiple_of(i * LANES, LANES), LANES), first:first + BLOCK] = jnp.where(row < LANES // 2, both[0], both[1]).astype(BF16)
        return carry

    lax.fori_loop(0, d_model // LANES, pair, 0)
    for f in range(n_fsdp):
        w_out = jnp.concatenate([w_ref[f, p, n_qkv:] for p in range(n_ep)], axis=0)
        cols = slice(f * half, (f + 1) * half)
        h_ref[0, :, cols] = (x_ref[0, :, cols].astype(F32) + tn_dot(ctx[...], w_out)).astype(BF16)


def attention(tokens, weights, head_dim):
    n_seq, seq_len, d_model = tokens.shape
    seq_spec = pl.BlockSpec((1, seq_len, d_model), lambda s: (s, 0, 0))
    qkv_spec = pl.BlockSpec((1, seq_len, 3 * d_model), lambda s: (s, 0, 0))
    w_spec = pl.BlockSpec(weights.shape, lambda s: (0, 0, 0, 0))
    return pl.pallas_call(
        functools.partial(attention_kernel, head_dim=head_dim),
        grid=(n_seq,),
        in_specs=[seq_spec, w_spec],
        out_specs=[seq_spec, qkv_spec],
        out_shape=[jax.ShapeDtypeStruct(tokens.shape, BF16), jax.ShapeDtypeStruct((n_seq, seq_len, 3 * d_model), BF16)],
        scratch_shapes=[pltpu.VMEM((d_model, seq_len), BF16)],
        name='attention',
        **settings(90, 60),
    )(tokens, weights)


def attention_grad_kernel(dh_ref, x_ref, qkv_ref, w_ref, dx_ref, dctx, dqkv, *, head_dim):
    seq_len, d_model = x_ref.shape[1:]
    n_fsdp, n_ep, rows, half = w_ref.shape
    n_qkv = rows * 3 // 4
    n_out = rows - n_qkv
    dh = dh_ref[0]
    for p in range(n_ep):
        part = nt_dot(dh[:, :half], w_ref[0, p, n_qkv:]) + nt_dot(dh[:, half:], w_ref[1, p, n_qkv:])
        dctx[:, p * n_out:(p + 1) * n_out] = part.astype(BF16)
    scale = head_dim ** -0.5

    def pair(i, carry):
        col = pl.multiple_of(i * LANES, LANES)
        q2, k2, v2 = (qkv_ref[0, :, pl.ds(pl.multiple_of(t * d_model + i * LANES, LANES), LANES)] for t in range(3))
        d2 = dctx[:, pl.ds(col, LANES)]
        dk = [jnp.zeros((BLOCK, LANES), F32)] * (seq_len // BLOCK)
        dv = list(dk)
        for first in range(0, seq_len, BLOCK):
            end = first + BLOCK
            keys, vals = k2[:end], v2[:end]
            causal = lax.broadcasted_iota(jnp.int32, (end, BLOCK), 1) + first >= lax.broadcasted_iota(jnp.int32, (end, BLOCK), 0)
            dq = jnp.zeros((BLOCK, LANES), F32)
            for head in range(2):
                q, d = lanes_of(head, q2[first:end]), lanes_of(head, d2[first:end])
                scores = jnp.where(causal, nt_dot(keys, q) * (scale * LOG2E), -1e30)
                probs = jnp.exp2(scores - jnp.max(scores, axis=0, keepdims=True))
                probs = probs * (1.0 / jnp.sum(probs, axis=0, keepdims=True))
                d_probs = nt_dot(vals, d)
                d_scores = probs * (d_probs - jnp.sum(probs * d_probs, axis=0, keepdims=True))
                d_scores = (d_scores * scale).astype(BF16)
                dv_part = jnp.dot(probs.astype(BF16), d, preferred_element_type=F32)
                dk_part = jnp.dot(d_scores, q, preferred_element_type=F32)
                dq = dq + tn_dot(d_scores, lanes_of(head, keys))
                for n in range(end // BLOCK):
                    dk[n] = dk[n] + dk_part[n * BLOCK:(n + 1) * BLOCK]
                    dv[n] = dv[n] + dv_part[n * BLOCK:(n + 1) * BLOCK]
            dqkv[first:end, pl.ds(col, LANES)] = dq.astype(BF16)
        for n in range(seq_len // BLOCK):
            dqkv[n * BLOCK:(n + 1) * BLOCK, pl.ds(pl.multiple_of(d_model + i * LANES, LANES), LANES)] = dk[n].astype(BF16)
            dqkv[n * BLOCK:(n + 1) * BLOCK, pl.ds(pl.multiple_of(2 * d_model + i * LANES, LANES), LANES)] = dv[n].astype(BF16)
        return carry

    lax.fori_loop(0, d_model // LANES, pair, 0)
    x = x_ref[0].astype(F32)
    d_normed = []
    for f in range(n_fsdp):
        w_qkv = jnp.concatenate([w_ref[f, p, :n_qkv] for p in range(n_ep)], axis=0)
        d_normed.append(jnp.dot(dqkv[...], w_qkv, preferred_element_type=F32).astype(BF16))
    d_normed = jnp.concatenate(d_normed, axis=1).astype(F32)
    inv = lax.rsqrt(jnp.mean(x * x, axis=-1, keepdims=True) + EPS)
    proj = jnp.mean(d_normed * x, axis=-1, keepdims=True)
    d_x = (d_normed * inv - x * (inv * inv * inv * proj)).astype(BF16).astype(F32)
    dx_ref[0] = (dh_ref[0].astype(F32) + d_x).astype(BF16)


def attention_grad(d_h, tokens, qkv, weights, head_dim):
    n_seq, seq_len, d_model = tokens.shape
    seq_spec = pl.BlockSpec((1, seq_len, d_model), lambda s: (s, 0, 0))
    qkv_spec = pl.BlockSpec((1, seq_len, 3 * d_model), lambda s: (s, 0, 0))
    w_spec = pl.BlockSpec(weights.shape, lambda s: (0, 0, 0, 0))
    return pl.pallas_call(
        functools.partial(attention_grad_kernel, head_dim=head_dim),
        grid=(n_seq,),
        in_specs=[seq_spec, seq_spec, qkv_spec, w_spec],
        out_specs=seq_spec,
        out_shape=jax.ShapeDtypeStruct(tokens.shape, BF16),
        scratch_shapes=[pltpu.VMEM((seq_len, d_model), BF16), pltpu.VMEM((seq_len, 3 * d_model), BF16)],
        name='attention_grad',
        **settings(150, 70),
    )(d_h, tokens, qkv, weights)


def capacity_of(tok_count, top_k, num_experts):
    return max(8, (5 * tok_count * top_k // (4 * num_experts) + 7) // 8 * 8)


def route_kernel(loc_ref, dest_ref, start_ref, rows_ref, off_ref, total, *, n_local):
    top_k = loc_ref.shape[1]
    ids = lax.broadcasted_iota(jnp.int32, (n_local, BLOCK), 0)
    upper = (lax.broadcasted_iota(jnp.int32, (BLOCK, BLOCK), 0) <= lax.broadcasted_iota(jnp.int32, (BLOCK, BLOCK), 1)).astype(F32).astype(BF16)
    before = (lax.broadcasted_iota(jnp.int32, (n_local, n_local), 0) > lax.broadcasted_iota(jnp.int32, (n_local, n_local), 1)).astype(F32).astype(BF16)

    @pl.when(pl.program_id(0) == 0)
    def _():
        total[...] = jnp.zeros(total.shape, jnp.int32)

    so_far = total[...]
    for s in range(loc_ref.shape[0]):
        for p in range(loc_ref.shape[2] // BLOCK):
            q = s * (loc_ref.shape[2] // BLOCK) + p
            loc = loc_ref[s, :, p * BLOCK:(p + 1) * BLOCK]
            member = jnp.zeros((n_local, BLOCK), F32)
            for j in range(top_k):
                member = jnp.where(loc[j:j + 1] == ids, 1.0, member)
            count = jnp.dot(member.astype(BF16), upper, preferred_element_type=F32)
            units = (count[:, BLOCK - 1:].astype(jnp.int32) + (ALIGN - 1)) // ALIGN
            units = jnp.broadcast_to(units, (n_local, LANES))
            start = jnp.dot(before, units.astype(F32).astype(BF16), preferred_element_type=F32).astype(jnp.int32) * ALIGN
            place = start[:, :1] + count.astype(jnp.int32) - 1
            for j in range(top_k):
                row = jnp.sum(jnp.where(loc[j:j + 1] == ids, place, 0), axis=0, keepdims=True)
                dest_ref[q, j:j + 1, :] = jnp.where(loc[j:j + 1] >= 0, row, -1)
            start_ref[q] = start
            rows_ref[q] = units * ALIGN
            off_ref[q] = so_far
            so_far = so_far + units * ALIGN
    total[...] = so_far


def route(local_ids, n_local):
    n_seq, top_k, seq_len = local_ids.shape
    per_seq = seq_len // BLOCK
    step = 2 if n_seq % 2 == 0 else 1
    n_blocks = n_seq * per_seq
    seg = jax.ShapeDtypeStruct((n_blocks, n_local, LANES), jnp.int32)
    seg_spec = pl.BlockSpec((step * per_seq, n_local, LANES), lambda s: (s, 0, 0))
    dest, *segs = pl.pallas_call(
        functools.partial(route_kernel, n_local=n_local),
        grid=(n_seq // step,),
        in_specs=[pl.BlockSpec((step, top_k, seq_len), lambda s: (s, 0, 0))],
        out_specs=[pl.BlockSpec((step * per_seq, top_k, BLOCK), lambda s: (s, 0, 0)), seg_spec, seg_spec, seg_spec],
        out_shape=[jax.ShapeDtypeStruct((n_blocks, top_k, BLOCK), jnp.int32), seg, seg, seg],
        scratch_shapes=[pltpu.VMEM((n_local, LANES), jnp.int32)],
        name='route',
        **settings(1, 3),
    )(local_ids)
    return dest, [part[:, :, 0] for part in segs]


def one_hot(dest_ref, gate_ref, first_row):
    rows = lax.broadcasted_iota(jnp.int32, (TILE, BLOCK), 0).astype(F32).astype(BF16)
    dest = jnp.clip(dest_ref[0] - first_row, -1, TILE).astype(F32).astype(BF16)
    gate = gate_ref[0]
    picked = jnp.zeros((TILE, BLOCK), BF16)
    for j in range(dest.shape[0]):
        picked = jnp.where(rows == dest[j:j + 1], gate[j:j + 1], picked)
    return picked, jnp.where(picked > 0, jnp.ones_like(picked), jnp.zeros_like(picked))


def dispatch_kernel(start_ref, rows_ref, off_ref, h_ref, dout_ref, dest_ref, gate_ref, *refs, base):
    r_hbm, d_hbm, u_s, rbuf, dbuf, sem = refs[-6:]
    step = pl.program_id(0)
    n_blocks = pl.num_programs(0)
    b = step + base
    n_exp = rows_ref.shape[1]
    slot = lax.rem(b, 2)

    def total(blk):
        return start_ref[blk, n_exp - 1] + rows_ref[blk, n_exp - 1]

    def drain(blk, which):
        n = pl.multiple_of(total(blk), ALIGN)

        @pl.when(n > 0)
        def _():
            pltpu.make_async_copy(rbuf.at[which, pl.ds(0, n), :], rbuf.at[which, pl.ds(0, n), :], sem.at[0, which]).wait()
            pltpu.make_async_copy(dbuf.at[which, pl.ds(0, n), :], dbuf.at[which, pl.ds(0, n), :], sem.at[1, which]).wait()

    @pl.when(step >= 2)
    def _():
        drain(b - 2, slot)

    hf = h_ref[...].astype(F32)
    u_s[...] = (hf * lax.rsqrt(jnp.mean(hf * hf, axis=-1, keepdims=True) + EPS)).astype(BF16)

    def tile(i, carry):
        first = pl.multiple_of(i * TILE, TILE)
        picked, ones = one_hot(dest_ref, gate_ref, first)
        rbuf[slot, pl.ds(first, TILE), :] = jnp.dot(ones, u_s[...], preferred_element_type=F32).astype(BF16)
        dbuf[slot, pl.ds(first, TILE), :] = jnp.dot(picked, dout_ref[...], preferred_element_type=F32).astype(BF16)
        return carry

    lax.fori_loop(0, (total(b) + (TILE - 1)) // TILE, tile, 0)

    def send(e, carry):
        n = pl.multiple_of(rows_ref[b, e], ALIGN)
        src = pl.multiple_of(start_ref[b, e], ALIGN)
        dst = pl.multiple_of(off_ref[b, e], ALIGN)

        @pl.when(n > 0)
        def _():
            pltpu.make_async_copy(rbuf.at[slot, pl.ds(src, n), :], r_hbm.at[e, pl.ds(dst, n), :], sem.at[0, slot]).start()
            pltpu.make_async_copy(dbuf.at[slot, pl.ds(src, n), :], d_hbm.at[e, pl.ds(dst, n), :], sem.at[1, slot]).start()

        return carry

    lax.fori_loop(0, n_exp, send, 0)

    @pl.when(step == n_blocks - 1)
    def _():
        @pl.when(n_blocks > 1)
        def _():
            drain(b - 1, 1 - slot)

        drain(b, slot)


def block_rows(top_k, n_local):
    return -(-(BLOCK * top_k + n_local * (ALIGN - 1)) // TILE) * TILE


def dispatch(h_tok, dout_tok, dest, gate, segs, base, held, n_local, max_rows):
    tok_count, d_model = h_tok.shape
    top_k = dest.shape[1]
    n_blocks = tok_count // BLOCK
    buf_rows = block_rows(top_k, n_local)
    tok_spec = pl.BlockSpec((BLOCK, d_model), lambda b, *_: (b, 0))
    map_spec = pl.BlockSpec((1, top_k, BLOCK), lambda b, *_: (b + base, 0, 0))
    rows_shape = jax.ShapeDtypeStruct((n_local, max_rows, d_model), BF16)
    hbm = pl.BlockSpec(memory_space=pl.ANY)
    return pl.pallas_call(
        functools.partial(dispatch_kernel, base=base),
        grid_spec=pltpu.PrefetchScalarGridSpec(
            num_scalar_prefetch=3,
            grid=(n_blocks,),
            in_specs=[tok_spec, tok_spec, map_spec, map_spec] + [hbm] * len(held),
            out_specs=[hbm, hbm],
            scratch_shapes=[
                pltpu.VMEM((BLOCK, d_model), BF16),
                pltpu.VMEM((2, buf_rows, d_model), BF16),
                pltpu.VMEM((2, buf_rows, d_model), BF16),
                pltpu.SemaphoreType.DMA((2, 2)),
            ],
        ),
        out_shape=[rows_shape, rows_shape],
        input_output_aliases={7: 0, 8: 1} if held else {},
        name='dispatch',
        **settings(40, 90),
    )(*segs, h_tok, dout_tok, dest, gate, *held)


def expert_kernel(count_ref, flip_ref, r_hbm, d_hbm, w_lo, w_hi, y_hbm, dr_hbm, dw_ref, rbuf, dbuf, ybuf, drbuf, done, in_sem, out_sem, *, expert_of, x_first):
    step = pl.program_id(0)
    n_steps = pl.num_programs(0)
    expert = expert_of(step)
    n_rows = count_ref[expert]
    n_tiles = jnp.maximum((n_rows + (TILE - 1)) // TILE, 1)
    half = dw_ref.shape[-1]

    def copies(who, i, slot, load):
        rows = pl.ds(pl.multiple_of(i * TILE, TILE), TILE)
        pairs = ((r_hbm, rbuf), (d_hbm, dbuf)) if load else ((ybuf, y_hbm), (drbuf, dr_hbm))
        for k, (src, dst) in enumerate(pairs):
            src = src.at[who, rows, :] if load else src.at[slot]
            dst = dst.at[slot] if load else dst.at[who, rows, :]
            yield pltpu.make_async_copy(src, dst, (in_sem if load else out_sem).at[k, slot])

    def start(*args):
        for copy in copies(*args):
            copy.start()

    def wait(*args):
        for copy in copies(*args):
            copy.wait()

    @pl.when(step == 0)
    def _():
        done[0] = 0
        start(expert, 0, 0, True)

    before = done[0]
    for p in range(dw_ref.shape[0]):
        for q in range(dw_ref.shape[1]):
            for t in range(dw_ref.shape[2]):
                clear(dw_ref.at[p, q, t, 0])

    def tile(i, carry):
        slot = lax.rem(before + i, 2)

        @pl.when(i + 1 < n_tiles)
        def _():
            start(expert, i + 1, 1 - slot, True)

        @pl.when((i + 1 == n_tiles) & (step + 1 < n_steps))
        def _():
            start(expert_of(step + 1), 0, 1 - slot, True)

        wait(expert, i, slot, True)

        @pl.when(before + i >= 2)
        def _():
            wait(expert, i, slot, False)

        valid = lax.broadcasted_iota(jnp.int32, (TILE, 1), 0) + i * TILE < n_rows
        r = jnp.where(valid, rbuf[slot], 0)
        dy = jnp.where(valid, dbuf[slot], 0)
        w1, w3, w2 = (jnp.concatenate([w[0, t, 0] for w in (w_lo, w_hi)], axis=t // 2) for t in range(3))
        act_a = jnp.dot(r, w1, preferred_element_type=F32)
        act_b = jnp.dot(r, w3, preferred_element_type=F32)
        d_g = nt_dot(dy, w2)
        sig = 1.0 / (1.0 + jnp.exp(-act_a))
        silu = act_a * sig
        g = (silu * act_b).astype(BF16)
        d_up = (d_g * silu).astype(BF16)
        d_gate = (d_g * act_b * sig * (1.0 + act_a * (1.0 - sig))).astype(BF16)
        ybuf[slot] = jnp.dot(g, w2, preferred_element_type=F32).astype(BF16)
        drbuf[slot] = (nt_dot(d_gate, w1) + nt_dot(d_up, w3)).astype(BF16)
        start(expert, i, slot, False)
        for f in range(2):
            part = slice(f * half, (f + 1) * half)
            to = lax.rem(f + flip_ref[0], 2)
            for t, (lhs, rhs) in enumerate(((r[:, part], d_gate), (r[:, part], d_up), (g, dy[:, part]))):
                dw_ref[(0, to, t, 0) if x_first else (to, 0, t, 0)] += tn_dot(lhs, rhs)
        return carry

    lax.fori_loop(0, n_tiles, tile, 0)
    done[0] = before + n_tiles

    @pl.when(step == n_steps - 1)
    def _():
        last = before + n_tiles - 1
        wait(expert, 0, lax.rem(last, 2), False)

        @pl.when(last >= 1)
        def _():
            wait(expert, 0, lax.rem(last + 1, 2), False)


def experts(rows, d_rows, weights, counts, flips, first, local_experts, x_first=False):
    d_model = rows.shape[2]
    n_owners, three, size, half, _ = weights.shape
    n_fsdp = d_model // half
    n_side = n_owners // n_fsdp

    def expert_of(g):
        return g // size * local_experts + first + lax.rem(g, size)

    def side(g, flip):
        return lax.rem(g // size + flip[1], n_side)

    def w_spec(f):
        return pl.BlockSpec((1, three, 1, half, half), lambda g, _, flip: (lax.rem(f + flip[0], n_fsdp) * n_side + side(g, flip), 0, lax.rem(g, size), 0, 0))

    def dw_index(g, _, flip):
        place = (side(g, flip), 0) if x_first else (0, side(g, flip))
        return (*place, 0, lax.rem(g, size), 0, 0)

    hbm = pl.BlockSpec(memory_space=pl.ANY)
    grads = (n_side, n_fsdp) if x_first else (n_fsdp, n_side)
    dw_block = (1, n_fsdp) if x_first else (n_fsdp, 1)
    return pl.pallas_call(
        functools.partial(expert_kernel, expert_of=expert_of, x_first=x_first),
        grid_spec=pltpu.PrefetchScalarGridSpec(
            num_scalar_prefetch=2,
            grid=(n_side * size,),
            in_specs=[hbm, hbm, w_spec(0), w_spec(1)],
            out_specs=[hbm, hbm, pl.BlockSpec((*dw_block, three, 1, half, half), dw_index)],
            scratch_shapes=[pltpu.VMEM((2, TILE, d_model), BF16)] * 4 + [pltpu.SMEM((1,), jnp.int32)] + [pltpu.SemaphoreType.DMA((2, 2))] * 2,
        ),
        out_shape=[jax.ShapeDtypeStruct(rows.shape, BF16)] * 2 + [jax.ShapeDtypeStruct((*grads, three, size, half, half), F32)],
        input_output_aliases={2: 0, 3: 1},
        name='experts',
        **settings(56 * size, 100 * size),
    )(counts, flips, rows, d_rows, weights, weights)


def clear(ref):
    def rows(i, carry):
        ref[pl.ds(pl.multiple_of(i * LANES, LANES), LANES), :] = jnp.zeros((LANES, ref.shape[1]), ref.dtype)
        return carry

    lax.fori_loop(0, ref.shape[0] // LANES, rows, 0)


def combine_kernel(start_ref, rows_ref, off_ref, y_hbm, dr_hbm, dest_ref, gate_ref, *refs, base, own):
    ybuf, dbuf, acc_y, acc_d, sem = refs[-5:]
    step = pl.program_id(0)
    n_blocks = pl.num_programs(0)
    b = step + base
    n_exp = rows_ref.shape[1]
    slot = lax.rem(step, 2)

    def total(blk):
        return start_ref[blk, n_exp - 1] + rows_ref[blk, n_exp - 1]

    def fetch(blk, which):
        def one(e, carry):
            n = pl.multiple_of(rows_ref[blk, e], ALIGN)
            dst = pl.multiple_of(start_ref[blk, e], ALIGN)
            src = pl.multiple_of(off_ref[blk, e], ALIGN)

            @pl.when(n > 0)
            def _():
                pltpu.make_async_copy(y_hbm.at[e, pl.ds(src, n), :], ybuf.at[which, pl.ds(dst, n), :], sem.at[0, which]).start()
                pltpu.make_async_copy(dr_hbm.at[e, pl.ds(src, n), :], dbuf.at[which, pl.ds(dst, n), :], sem.at[1, which]).start()

            return carry

        lax.fori_loop(0, n_exp, one, 0)

    @pl.when(step == 0)
    def _():
        for which in range(2):
            clear(ybuf.at[which])
            clear(dbuf.at[which])
        fetch(b, 0)

    @pl.when(step + 1 < n_blocks)
    def _():
        fetch(b + 1, 1 - slot)

    n = pl.multiple_of(total(b), ALIGN)

    @pl.when(n > 0)
    def _():
        pltpu.make_async_copy(ybuf.at[slot, pl.ds(0, n), :], ybuf.at[slot, pl.ds(0, n), :], sem.at[0, slot]).wait()
        pltpu.make_async_copy(dbuf.at[slot, pl.ds(0, n), :], dbuf.at[slot, pl.ds(0, n), :], sem.at[1, slot]).wait()

    acc_y[...] = jnp.zeros(acc_y.shape, F32)
    acc_d[...] = jnp.zeros(acc_d.shape, F32)

    def tile(i, carry):
        first = pl.multiple_of(i * TILE, TILE)
        picked, ones = one_hot(dest_ref, gate_ref, first)
        acc_y[...] += tn_dot(picked, ybuf[slot, pl.ds(first, TILE), :])
        acc_d[...] += tn_dot(ones, dbuf[slot, pl.ds(first, TILE), :])
        return carry

    lax.fori_loop(0, (n + (TILE - 1)) // TILE, tile, 0)

    if not own:
        out_y, out_d = refs[:2]
        out_y[...] = acc_y[...]
        out_d[...] = acc_d[...]
        return
    more_y, more_d, h_ref, dout_ref, out_ref, dh_ref = refs[:6]
    hf = h_ref[...].astype(F32)
    out_ref[...] = (hf + (acc_y[...] + more_y[...])).astype(BF16)
    d_u = (acc_d[...] + more_d[...]).astype(BF16).astype(F32)
    inv = lax.rsqrt(jnp.mean(hf * hf, axis=-1, keepdims=True) + EPS)
    proj = jnp.mean(d_u * hf, axis=-1, keepdims=True)
    d_norm = (d_u * inv - hf * (inv * inv * inv * proj)).astype(BF16).astype(F32)
    dh_ref[...] = (dout_ref[...].astype(F32) + d_norm).astype(BF16)


def combine(y_rows, dr_rows, dest, gate, segs, base, n_blocks, extra):
    n_local, _, d_model = y_rows.shape
    top_k = dest.shape[1]
    buf_rows = block_rows(top_k, n_local)
    tok_spec = pl.BlockSpec((BLOCK, d_model), lambda b, *_: (b, 0))
    map_spec = pl.BlockSpec((1, top_k, BLOCK), lambda b, *_: (b + base, 0, 0))
    hbm = pl.BlockSpec(memory_space=pl.ANY)
    out = jax.ShapeDtypeStruct((n_blocks * BLOCK, d_model), BF16 if extra else F32)
    return pl.pallas_call(
        functools.partial(combine_kernel, base=base, own=bool(extra)),
        grid_spec=pltpu.PrefetchScalarGridSpec(
            num_scalar_prefetch=3,
            grid=(n_blocks,),
            in_specs=[hbm, hbm, map_spec, map_spec] + [tok_spec] * len(extra),
            out_specs=[tok_spec, tok_spec],
            scratch_shapes=[
                pltpu.VMEM((2, buf_rows, d_model), BF16),
                pltpu.VMEM((2, buf_rows, d_model), BF16),
                pltpu.VMEM((BLOCK, d_model), F32),
                pltpu.VMEM((BLOCK, d_model), F32),
                pltpu.SemaphoreType.DMA((2, 2)),
            ],
        ),
        out_shape=[out, out],
        name='combine',
        **settings(45, 120),
    )(*segs, y_rows, dr_rows, dest, gate, *extra)


def place_kernel(*refs, n_parts):
    for k, out_ref in enumerate(refs[-3:]):
        value = refs[0][k]
        for part_ref in refs[1:n_parts]:
            value = value + part_ref[k]
        out_ref[...] = value


def place(parts, held, first, n_total):
    three, size, rows, cols = parts[0].shape
    hbm = pl.BlockSpec(memory_space=pl.ANY)
    return pl.pallas_call(
        functools.partial(place_kernel, n_parts=len(parts)),
        grid=(size,),
        in_specs=[pl.BlockSpec((three, 1, rows, cols), lambda i: (0, i, 0, 0))] * len(parts) + [hbm] * len(held),
        out_specs=[pl.BlockSpec((1, rows, cols), lambda i: (first + i, 0, 0))] * three,
        out_shape=[jax.ShapeDtypeStruct((n_total, rows, cols), F32)] * three,
        input_output_aliases={len(parts) + k: k for k in range(len(held))},
        name='place',
        **settings(1, 12),
    )(*parts, *held)


CHUNKS = (2, 4)
CORES = 2


def solution(mesh):
    ep_size, fsdp_size = mesh.shape['ep'], mesh.shape['fsdp']
    tok_spec = P(('data', 'fsdp', 'ep'))
    in_specs = (tok_spec, P('fsdp'), P(None, None, 'fsdp'), P('ep', 'fsdp'), P('ep', 'fsdp'), P('ep', None, 'fsdp'), tok_spec, tok_spec, tok_spec, tok_spec)
    out_specs = (tok_spec, tok_spec, P(('data', 'ep'), 'fsdp'), P(('data', 'ep'), 'fsdp'), P(('data', 'ep'), None, 'fsdp'))

    def device_fn(tokens, w_qkv, w_out, w_gate, w_up, w_down, expert_idx, expert_slot, gate_wts, d_out):
        n_seq, seq_len, d_model = tokens.shape
        tok_count = n_seq * seq_len
        top_k = expert_idx.shape[2]
        local_experts, half, _ = w_gate.shape
        num_experts = local_experts * ep_size
        n_side = ep_size // CORES
        n_local = local_experts * n_side
        n_blocks = tok_count // BLOCK
        capacity = capacity_of(tok_count, top_k, num_experts)
        max_rows = -(-(CORES * (capacity + n_blocks * (ALIGN - 1))) // TILE) * TILE
        ep = lax.axis_index('ep')
        groups = [[c + CORES * i for i in range(fsdp_size * n_side)] for c in range(CORES)]

        fsdp, side = lax.axis_index('fsdp'), ep // CORES
        flips = jnp.stack([fsdp, side]).astype(jnp.int32)

        def swap(values):
            return lax.ppermute(values, 'ep', [(i, i ^ 1) for i in range(ep_size)])

        def swap_x(values):
            return lax.ppermute(values, 'ep', [(i, i ^ CORES) for i in range(ep_size)])

        def swap_y(values):
            return lax.ppermute(values, 'fsdp', [(i, i ^ 1) for i in range(fsdp_size)])

        def own_weights(part):
            return jnp.stack([w_gate[part], w_up[part], w_down[part]], axis=0)

        _, head_dim, _ = w_out.shape
        qkv_rows = w_qkv.transpose(1, 2, 3, 0).reshape(-1, half)
        qkv_rows = lax.dynamic_slice_in_dim(qkv_rows, ep * (3 * d_model // ep_size), 3 * d_model // ep_size, axis=0)
        out_rows = lax.dynamic_slice_in_dim(w_out.reshape(-1, half), ep * (d_model // ep_size), d_model // ep_size, axis=0)
        attn_w = lax.all_gather(jnp.concatenate([qkv_rows, out_rows], axis=0), ('fsdp', 'ep'), axis=0, tiled=False)
        attn_w = attn_w.reshape(fsdp_size, ep_size, -1, half)
        weights, first = [], 0
        for size in CHUNKS:
            mine = own_weights(slice(first, first + size))
            full = lax.all_gather(mine, ('fsdp', 'ep'), axis=0, tiled=False, axis_index_groups=groups)
            weights.append(full)
            first += size
        mid = first + (local_experts - first) // 2
        w_a, w_b = own_weights(slice(first, mid)), own_weights(slice(mid, local_experts))
        w_ax, w_ay, w_bx, w_by = swap_x(w_a), swap_y(w_a), swap_x(w_b), swap_y(w_b)

        dout_tok = d_out.reshape(tok_count, d_model)
        dout_other = swap(dout_tok)
        kept_ids = jnp.where(expert_slot >= 0, expert_idx, -1).transpose(0, 2, 1)
        all_ids = jnp.concatenate([kept_ids, swap(kept_ids)], axis=0)
        owner = all_ids // local_experts
        mine_too = (all_ids >= 0) & (lax.rem(owner, CORES) == lax.rem(ep, CORES))
        local_ids = jnp.where(mine_too, owner // CORES * local_experts + lax.rem(all_ids, local_experts), -1)
        dest, segs = route(local_ids, n_local)
        counts = jnp.sum(segs[1], axis=0)
        gate = gate_wts.transpose(0, 2, 1)
        gate = jnp.concatenate([gate, swap(gate)], axis=0)
        gate = gate.reshape(2 * n_seq, top_k, seq_len // BLOCK, BLOCK).transpose(0, 2, 1, 3).reshape(2 * n_blocks, top_k, BLOCK)

        tokens, dest, segs, counts, gate = lax.optimization_barrier((tokens, dest, segs, counts, gate))
        h_seq, qkv = attention(tokens, attn_w, head_dim)
        w_axy, w_byx = swap_y(w_ax), swap_x(w_by)
        w_a = jnp.stack([w_a, w_ax, w_ay, w_axy])
        w_b = jnp.stack([w_b, w_bx, w_by, w_byx])
        h_tok = h_seq.reshape(tok_count, d_model)
        h_other = swap(h_tok)
        held = dispatch(h_tok, dout_tok, dest, gate, segs, 0, [], n_local, max_rows)
        rows, d_rows = dispatch(h_other, dout_other, dest, gate, segs, n_blocks, held, n_local, max_rows)
        sums, grads, start = [], [], 0
        for n, size in enumerate(CHUNKS):
            rows, d_rows, d_w = experts(rows, d_rows, (w_a, w_b)[n], counts, flips, (first, mid)[n], local_experts, x_first=n == 0)
            sums.append(d_w[0] + (swap_x, swap_y)[n](d_w[1]))
            rows, d_rows, d_w = experts(rows, d_rows, weights[n], counts, jnp.zeros_like(flips), start, local_experts)
            d_w = d_w.reshape(fsdp_size * n_side, *d_w.shape[2:])
            grads.append(([lax.psum_scatter(d_w, ('fsdp', 'ep'), scatter_dimension=0, tiled=False, axis_index_groups=groups)], start))
            start += size
        more_a, more_b = swap_y(sums[0][1]), swap_x(sums[1][1])
        done = [grads[0], ([sums[0][0], more_a], first), ([sums[1][0], more_b], mid), grads[1]]
        sums = combine(rows, d_rows, dest, gate, segs, n_blocks, n_blocks, [])
        more = [swap(value) for value in sums]
        layer_out, d_h = combine(rows, d_rows, dest, gate, segs, 0, n_blocks, [*more, h_tok, dout_tok])
        d_tokens = attention_grad(d_h.reshape(n_seq, seq_len, d_model), tokens, qkv, attn_w, head_dim)
        d_ws = []
        for parts, where in done:
            d_ws = place(parts, d_ws, where, local_experts)
        return layer_out.reshape(n_seq, seq_len, d_model), d_tokens, *d_ws

    return jax.shard_map(device_fn, mesh=mesh, in_specs=in_specs, out_specs=out_specs, check_vma=False)
```

```python
import functools
import math

import jax
import jax.numpy as jnp
from jax import lax
from jax.experimental import pallas as pl
from jax.experimental.pallas import tpu as pltpu
from jax.sharding import PartitionSpec as P


F32 = jnp.float32
BF16 = jnp.bfloat16
BLOCK = 256
TILE = 256
ALIGN = 16
LANES = 128
LOG2E = math.log2(math.e)
EPS = 1e-6
VMEM_BYTES = 60 * 2 ** 20


def settings(gflop, mbytes):
    return {
        'compiler_params': pltpu.CompilerParams(dimension_semantics=('arbitrary',), vmem_limit_bytes=VMEM_BYTES),
        'cost_estimate': pl.CostEstimate(flops=gflop * 10 ** 9, bytes_accessed=mbytes * 10 ** 6, transcendentals=0),
    }


def nt_dot(lhs, rhs):
    return lax.dot_general(lhs, rhs, (((1,), (1,)), ((), ())), preferred_element_type=F32)


def tn_dot(lhs, rhs):
    return lax.dot_general(lhs, rhs, (((0,), (0,)), ((), ())), preferred_element_type=F32)


def lanes_of(head, values):
    lane = lax.broadcasted_iota(jnp.int32, values.shape, 1)
    return jnp.where((lane >= LANES // 2) == bool(head), values, jnp.zeros_like(values))


def attention_kernel(x_ref, w_ref, h_ref, qkv_ref, ctx, *, head_dim):
    seq_len, d_model = x_ref.shape[1:]
    n_fsdp, n_ep, rows, half = w_ref.shape
    n_qkv = rows * 3 // 4
    x = x_ref[0].astype(F32)
    normed = (x * lax.rsqrt(jnp.mean(x * x, axis=-1, keepdims=True) + EPS)).astype(BF16)
    for p in range(n_ep):
        part = nt_dot(normed[:, :half], w_ref[0, p, :n_qkv]) + nt_dot(normed[:, half:], w_ref[1, p, :n_qkv])
        qkv_ref[0, :, p * n_qkv:(p + 1) * n_qkv] = part.astype(BF16)
    scale = head_dim ** -0.5 * LOG2E

    diagonal = lax.broadcasted_iota(jnp.int32, (BLOCK, BLOCK), 1) >= lax.broadcasted_iota(jnp.int32, (BLOCK, BLOCK), 0)

    def pair(i, carry):
        q2, k2, v2 = (qkv_ref[0, :, pl.ds(pl.multiple_of(t * d_model + i * LANES, LANES), LANES)] for t in range(3))
        for first in range(0, seq_len, BLOCK):
            both = []
            for head in range(2):
                query = lanes_of(head, q2[first:first + BLOCK])
                parts = [nt_dot(k2[at:at + BLOCK], query) * scale for at in range(0, first + BLOCK, BLOCK)]
                parts[-1] = jnp.where(diagonal, parts[-1], -1e30)
                top = functools.reduce(jnp.maximum, [jnp.max(part, axis=0, keepdims=True) for part in parts])
                parts = [jnp.exp2(part - top) for part in parts]
                inverse = 1.0 / sum(jnp.sum(part, axis=0, keepdims=True) for part in parts)
                probs = jnp.concatenate([(part * inverse).astype(BF16) for part in parts], axis=0)
                both.append(tn_dot(v2[:first + BLOCK], probs))
            row = lax.broadcasted_iota(jnp.int32, (LANES, BLOCK), 0)
            ctx[pl.ds(pl.multiple_of(i * LANES, LANES), LANES), first:first + BLOCK] = jnp.where(row < LANES // 2, both[0], both[1]).astype(BF16)
        return carry

    lax.fori_loop(0, d_model // LANES, pair, 0)
    for f in range(n_fsdp):
        w_out = jnp.concatenate([w_ref[f, p, n_qkv:] for p in range(n_ep)], axis=0)
        cols = slice(f * half, (f + 1) * half)
        h_ref[0, :, cols] = (x_ref[0, :, cols].astype(F32) + tn_dot(ctx[...], w_out)).astype(BF16)


def attention(tokens, weights, head_dim):
    n_seq, seq_len, d_model = tokens.shape
    seq_spec = pl.BlockSpec((1, seq_len, d_model), lambda s: (s, 0, 0))
    qkv_spec = pl.BlockSpec((1, seq_len, 3 * d_model), lambda s: (s, 0, 0))
    w_spec = pl.BlockSpec(weights.shape, lambda s: (0, 0, 0, 0))
    return pl.pallas_call(
        functools.partial(attention_kernel, head_dim=head_dim),
        grid=(n_seq,),
        in_specs=[seq_spec, w_spec],
        out_specs=[seq_spec, qkv_spec],
        out_shape=[jax.ShapeDtypeStruct(tokens.shape, BF16), jax.ShapeDtypeStruct((n_seq, seq_len, 3 * d_model), BF16)],
        scratch_shapes=[pltpu.VMEM((d_model, seq_len), BF16)],
        name='attention',
        **settings(90, 60),
    )(tokens, weights)


def attention_grad_kernel(dh_ref, x_ref, qkv_ref, w_ref, dx_ref, dctx, dqkv, *, head_dim):
    seq_len, d_model = x_ref.shape[1:]
    n_fsdp, n_ep, rows, half = w_ref.shape
    n_qkv = rows * 3 // 4
    n_out = rows - n_qkv
    dh = dh_ref[0]
    for p in range(n_ep):
        part = nt_dot(dh[:, :half], w_ref[0, p, n_qkv:]) + nt_dot(dh[:, half:], w_ref[1, p, n_qkv:])
        dctx[:, p * n_out:(p + 1) * n_out] = part.astype(BF16)
    scale = head_dim ** -0.5

    def pair(i, carry):
        col = pl.multiple_of(i * LANES, LANES)
        q2, k2, v2 = (qkv_ref[0, :, pl.ds(pl.multiple_of(t * d_model + i * LANES, LANES), LANES)] for t in range(3))
        d2 = dctx[:, pl.ds(col, LANES)]
        dk = [jnp.zeros((BLOCK, LANES), F32)] * (seq_len // BLOCK)
        dv = list(dk)
        for first in range(0, seq_len, BLOCK):
            end = first + BLOCK
            keys, vals = k2[:end], v2[:end]
            causal = lax.broadcasted_iota(jnp.int32, (end, BLOCK), 1) + first >= lax.broadcasted_iota(jnp.int32, (end, BLOCK), 0)
            dq = jnp.zeros((BLOCK, LANES), F32)
            for head in range(2):
                q, d = lanes_of(head, q2[first:end]), lanes_of(head, d2[first:end])
                scores = jnp.where(causal, nt_dot(keys, q) * (scale * LOG2E), -1e30)
                probs = jnp.exp2(scores - jnp.max(scores, axis=0, keepdims=True))
                probs = probs * (1.0 / jnp.sum(probs, axis=0, keepdims=True))
                d_probs = nt_dot(vals, d)
                d_scores = probs * (d_probs - jnp.sum(probs * d_probs, axis=0, keepdims=True))
                d_scores = (d_scores * scale).astype(BF16)
                dv_part = jnp.dot(probs.astype(BF16), d, preferred_element_type=F32)
                dk_part = jnp.dot(d_scores, q, preferred_element_type=F32)
                dq = dq + tn_dot(d_scores, lanes_of(head, keys))
                for n in range(end // BLOCK):
                    dk[n] = dk[n] + dk_part[n * BLOCK:(n + 1) * BLOCK]
                    dv[n] = dv[n] + dv_part[n * BLOCK:(n + 1) * BLOCK]
            dqkv[first:end, pl.ds(col, LANES)] = dq.astype(BF16)
        for n in range(seq_len // BLOCK):
            dqkv[n * BLOCK:(n + 1) * BLOCK, pl.ds(pl.multiple_of(d_model + i * LANES, LANES), LANES)] = dk[n].astype(BF16)
            dqkv[n * BLOCK:(n + 1) * BLOCK, pl.ds(pl.multiple_of(2 * d_model + i * LANES, LANES), LANES)] = dv[n].astype(BF16)
        return carry

    lax.fori_loop(0, d_model // LANES, pair, 0)
    x = x_ref[0].astype(F32)
    d_normed = []
    for f in range(n_fsdp):
        w_qkv = jnp.concatenate([w_ref[f, p, :n_qkv] for p in range(n_ep)], axis=0)
        d_normed.append(jnp.dot(dqkv[...], w_qkv, preferred_element_type=F32).astype(BF16))
    d_normed = jnp.concatenate(d_normed, axis=1).astype(F32)
    inv = lax.rsqrt(jnp.mean(x * x, axis=-1, keepdims=True) + EPS)
    proj = jnp.mean(d_normed * x, axis=-1, keepdims=True)
    d_x = (d_normed * inv - x * (inv * inv * inv * proj)).astype(BF16).astype(F32)
    dx_ref[0] = (dh_ref[0].astype(F32) + d_x).astype(BF16)


def attention_grad(d_h, tokens, qkv, weights, head_dim):
    n_seq, seq_len, d_model = tokens.shape
    seq_spec = pl.BlockSpec((1, seq_len, d_model), lambda s: (s, 0, 0))
    qkv_spec = pl.BlockSpec((1, seq_len, 3 * d_model), lambda s: (s, 0, 0))
    w_spec = pl.BlockSpec(weights.shape, lambda s: (0, 0, 0, 0))
    return pl.pallas_call(
        functools.partial(attention_grad_kernel, head_dim=head_dim),
        grid=(n_seq,),
        in_specs=[seq_spec, seq_spec, qkv_spec, w_spec],
        out_specs=seq_spec,
        out_shape=jax.ShapeDtypeStruct(tokens.shape, BF16),
        scratch_shapes=[pltpu.VMEM((seq_len, d_model), BF16), pltpu.VMEM((seq_len, 3 * d_model), BF16)],
        name='attention_grad',
        **settings(150, 70),
    )(d_h, tokens, qkv, weights)


def capacity_of(tok_count, top_k, num_experts):
    return max(8, (5 * tok_count * top_k // (4 * num_experts) + 7) // 8 * 8)


def route_kernel(loc_ref, dest_ref, start_ref, rows_ref, off_ref, total, *, n_local):
    top_k = loc_ref.shape[1]
    ids = lax.broadcasted_iota(jnp.int32, (n_local, BLOCK), 0)
    upper = (lax.broadcasted_iota(jnp.int32, (BLOCK, BLOCK), 0) <= lax.broadcasted_iota(jnp.int32, (BLOCK, BLOCK), 1)).astype(F32).astype(BF16)
    before = (lax.broadcasted_iota(jnp.int32, (n_local, n_local), 0) > lax.broadcasted_iota(jnp.int32, (n_local, n_local), 1)).astype(F32).astype(BF16)

    @pl.when(pl.program_id(0) == 0)
    def _():
        total[...] = jnp.zeros(total.shape, jnp.int32)

    so_far = total[...]
    for s in range(loc_ref.shape[0]):
        for p in range(loc_ref.shape[2] // BLOCK):
            q = s * (loc_ref.shape[2] // BLOCK) + p
            loc = loc_ref[s, :, p * BLOCK:(p + 1) * BLOCK]
            member = jnp.zeros((n_local, BLOCK), F32)
            for j in range(top_k):
                member = jnp.where(loc[j:j + 1] == ids, 1.0, member)
            count = jnp.dot(member.astype(BF16), upper, preferred_element_type=F32)
            units = (count[:, BLOCK - 1:].astype(jnp.int32) + (ALIGN - 1)) // ALIGN
            units = jnp.broadcast_to(units, (n_local, LANES))
            start = jnp.dot(before, units.astype(F32).astype(BF16), preferred_element_type=F32).astype(jnp.int32) * ALIGN
            place = start[:, :1] + count.astype(jnp.int32) - 1
            for j in range(top_k):
                row = jnp.sum(jnp.where(loc[j:j + 1] == ids, place, 0), axis=0, keepdims=True)
                dest_ref[q, j:j + 1, :] = jnp.where(loc[j:j + 1] >= 0, row, -1)
            start_ref[q] = start
            rows_ref[q] = units * ALIGN
            off_ref[q] = so_far
            so_far = so_far + units * ALIGN
    total[...] = so_far


def route(local_ids, n_local):
    n_seq, top_k, seq_len = local_ids.shape
    per_seq = seq_len // BLOCK
    step = 2 if n_seq % 2 == 0 else 1
    n_blocks = n_seq * per_seq
    seg = jax.ShapeDtypeStruct((n_blocks, n_local, LANES), jnp.int32)
    seg_spec = pl.BlockSpec((step * per_seq, n_local, LANES), lambda s: (s, 0, 0))
    dest, *segs = pl.pallas_call(
        functools.partial(route_kernel, n_local=n_local),
        grid=(n_seq // step,),
        in_specs=[pl.BlockSpec((step, top_k, seq_len), lambda s: (s, 0, 0))],
        out_specs=[pl.BlockSpec((step * per_seq, top_k, BLOCK), lambda s: (s, 0, 0)), seg_spec, seg_spec, seg_spec],
        out_shape=[jax.ShapeDtypeStruct((n_blocks, top_k, BLOCK), jnp.int32), seg, seg, seg],
        scratch_shapes=[pltpu.VMEM((n_local, LANES), jnp.int32)],
        name='route',
        **settings(1, 3),
    )(local_ids)
    return dest, [part[:, :, 0] for part in segs]


def one_hot(dest_ref, gate_ref, first_row):
    rows = lax.broadcasted_iota(jnp.int32, (TILE, BLOCK), 0).astype(F32).astype(BF16)
    dest = jnp.clip(dest_ref[0] - first_row, -1, TILE).astype(F32).astype(BF16)
    gate = gate_ref[0]
    picked = jnp.zeros((TILE, BLOCK), BF16)
    for j in range(dest.shape[0]):
        picked = jnp.where(rows == dest[j:j + 1], gate[j:j + 1], picked)
    return picked, jnp.where(picked > 0, jnp.ones_like(picked), jnp.zeros_like(picked))


def dispatch_kernel(start_ref, rows_ref, off_ref, h_ref, dout_ref, dest_ref, gate_ref, *refs, base):
    r_hbm, d_hbm, u_s, rbuf, dbuf, sem = refs[-6:]
    step = pl.program_id(0)
    n_blocks = pl.num_programs(0)
    b = step + base
    n_exp = rows_ref.shape[1]
    slot = lax.rem(b, 2)

    def total(blk):
        return start_ref[blk, n_exp - 1] + rows_ref[blk, n_exp - 1]

    def drain(blk, which):
        n = pl.multiple_of(total(blk), ALIGN)

        @pl.when(n > 0)
        def _():
            pltpu.make_async_copy(rbuf.at[which, pl.ds(0, n), :], rbuf.at[which, pl.ds(0, n), :], sem.at[0, which]).wait()
            pltpu.make_async_copy(dbuf.at[which, pl.ds(0, n), :], dbuf.at[which, pl.ds(0, n), :], sem.at[1, which]).wait()

    @pl.when(step >= 2)
    def _():
        drain(b - 2, slot)

    hf = h_ref[...].astype(F32)
    u_s[...] = (hf * lax.rsqrt(jnp.mean(hf * hf, axis=-1, keepdims=True) + EPS)).astype(BF16)

    def tile(i, carry):
        first = pl.multiple_of(i * TILE, TILE)
        picked, ones = one_hot(dest_ref, gate_ref, first)
        rbuf[slot, pl.ds(first, TILE), :] = jnp.dot(ones, u_s[...], preferred_element_type=F32).astype(BF16)
        dbuf[slot, pl.ds(first, TILE), :] = jnp.dot(picked, dout_ref[...], preferred_element_type=F32).astype(BF16)
        return carry

    lax.fori_loop(0, (total(b) + (TILE - 1)) // TILE, tile, 0)

    def send(e, carry):
        n = pl.multiple_of(rows_ref[b, e], ALIGN)
        src = pl.multiple_of(start_ref[b, e], ALIGN)
        dst = pl.multiple_of(off_ref[b, e], ALIGN)

        @pl.when(n > 0)
        def _():
            pltpu.make_async_copy(rbuf.at[slot, pl.ds(src, n), :], r_hbm.at[e, pl.ds(dst, n), :], sem.at[0, slot]).start()
            pltpu.make_async_copy(dbuf.at[slot, pl.ds(src, n), :], d_hbm.at[e, pl.ds(dst, n), :], sem.at[1, slot]).start()

        return carry

    lax.fori_loop(0, n_exp, send, 0)

    @pl.when(step == n_blocks - 1)
    def _():
        @pl.when(n_blocks > 1)
        def _():
            drain(b - 1, 1 - slot)

        drain(b, slot)


def block_rows(top_k, n_local):
    return -(-(BLOCK * top_k + n_local * (ALIGN - 1)) // TILE) * TILE


def dispatch(h_tok, dout_tok, dest, gate, segs, base, held, n_local, max_rows):
    tok_count, d_model = h_tok.shape
    top_k = dest.shape[1]
    n_blocks = tok_count // BLOCK
    buf_rows = block_rows(top_k, n_local)
    tok_spec = pl.BlockSpec((BLOCK, d_model), lambda b, *_: (b, 0))
    map_spec = pl.BlockSpec((1, top_k, BLOCK), lambda b, *_: (b + base, 0, 0))
    rows_shape = jax.ShapeDtypeStruct((n_local, max_rows, d_model), BF16)
    hbm = pl.BlockSpec(memory_space=pl.ANY)
    return pl.pallas_call(
        functools.partial(dispatch_kernel, base=base),
        grid_spec=pltpu.PrefetchScalarGridSpec(
            num_scalar_prefetch=3,
            grid=(n_blocks,),
            in_specs=[tok_spec, tok_spec, map_spec, map_spec] + [hbm] * len(held),
            out_specs=[hbm, hbm],
            scratch_shapes=[
                pltpu.VMEM((BLOCK, d_model), BF16),
                pltpu.VMEM((2, buf_rows, d_model), BF16),
                pltpu.VMEM((2, buf_rows, d_model), BF16),
                pltpu.SemaphoreType.DMA((2, 2)),
            ],
        ),
        out_shape=[rows_shape, rows_shape],
        input_output_aliases={7: 0, 8: 1} if held else {},
        name='dispatch',
        **settings(40, 90),
    )(*segs, h_tok, dout_tok, dest, gate, *held)


def expert_kernel(count_ref, flip_ref, r_hbm, d_hbm, w_lo, w_hi, y_hbm, dr_hbm, dw_ref, rbuf, dbuf, ybuf, drbuf, done, in_sem, out_sem, *, expert_of, x_first):
    step = pl.program_id(0)
    n_steps = pl.num_programs(0)
    expert = expert_of(step)
    n_rows = count_ref[expert]
    n_tiles = jnp.maximum((n_rows + (TILE - 1)) // TILE, 1)
    half = dw_ref.shape[-1]

    def copies(who, i, slot, load):
        rows = pl.ds(pl.multiple_of(i * TILE, TILE), TILE)
        pairs = ((r_hbm, rbuf), (d_hbm, dbuf)) if load else ((ybuf, y_hbm), (drbuf, dr_hbm))
        for k, (src, dst) in enumerate(pairs):
            src = src.at[who, rows, :] if load else src.at[slot]
            dst = dst.at[slot] if load else dst.at[who, rows, :]
            yield pltpu.make_async_copy(src, dst, (in_sem if load else out_sem).at[k, slot])

    def start(*args):
        for copy in copies(*args):
            copy.start()

    def wait(*args):
        for copy in copies(*args):
            copy.wait()

    @pl.when(step == 0)
    def _():
        done[0] = 0
        start(expert, 0, 0, True)

    before = done[0]
    for p in range(dw_ref.shape[0]):
        for q in range(dw_ref.shape[1]):
            for t in range(dw_ref.shape[2]):
                clear(dw_ref.at[p, q, t, 0])

    def tile(i, carry):
        slot = lax.rem(before + i, 2)

        @pl.when(i + 1 < n_tiles)
        def _():
            start(expert, i + 1, 1 - slot, True)

        @pl.when((i + 1 == n_tiles) & (step + 1 < n_steps))
        def _():
            start(expert_of(step + 1), 0, 1 - slot, True)

        wait(expert, i, slot, True)

        @pl.when(before + i >= 2)
        def _():
            wait(expert, i, slot, False)

        valid = lax.broadcasted_iota(jnp.int32, (TILE, 1), 0) + i * TILE < n_rows
        r = jnp.where(valid, rbuf[slot], 0)
        dy = jnp.where(valid, dbuf[slot], 0)
        w1, w3, w2 = (jnp.concatenate([w[0, t, 0] for w in (w_lo, w_hi)], axis=t // 2) for t in range(3))
        act_a = jnp.dot(r, w1, preferred_element_type=F32)
        act_b = jnp.dot(r, w3, preferred_element_type=F32)
        d_g = nt_dot(dy, w2)
        sig = 1.0 / (1.0 + jnp.exp(-act_a))
        silu = act_a * sig
        g = (silu * act_b).astype(BF16)
        d_up = (d_g * silu).astype(BF16)
        d_gate = (d_g * act_b * sig * (1.0 + act_a * (1.0 - sig))).astype(BF16)
        ybuf[slot] = jnp.dot(g, w2, preferred_element_type=F32).astype(BF16)
        drbuf[slot] = (nt_dot(d_gate, w1) + nt_dot(d_up, w3)).astype(BF16)
        start(expert, i, slot, False)
        for f in range(2):
            part = slice(f * half, (f + 1) * half)
            to = lax.rem(f + flip_ref[0], 2)
            for t, (lhs, rhs) in enumerate(((r[:, part], d_gate), (r[:, part], d_up), (g, dy[:, part]))):
                dw_ref[(0, to, t, 0) if x_first else (to, 0, t, 0)] += tn_dot(lhs, rhs)
        return carry

    lax.fori_loop(0, n_tiles, tile, 0)
    done[0] = before + n_tiles

    @pl.when(step == n_steps - 1)
    def _():
        last = before + n_tiles - 1
        wait(expert, 0, lax.rem(last, 2), False)

        @pl.when(last >= 1)
        def _():
            wait(expert, 0, lax.rem(last + 1, 2), False)


def experts(rows, d_rows, weights, counts, flips, first, local_experts, x_first=False):
    d_model = rows.shape[2]
    n_owners, three, size, half, _ = weights.shape
    n_fsdp = d_model // half
    n_side = n_owners // n_fsdp

    def expert_of(g):
        return g // size * local_experts + first + lax.rem(g, size)

    def side(g, flip):
        return lax.rem(g // size + flip[1], n_side)

    def w_spec(f):
        return pl.BlockSpec((1, three, 1, half, half), lambda g, _, flip: (lax.rem(f + flip[0], n_fsdp) * n_side + side(g, flip), 0, lax.rem(g, size), 0, 0))

    def dw_index(g, _, flip):
        place = (side(g, flip), 0) if x_first else (0, side(g, flip))
        return (*place, 0, lax.rem(g, size), 0, 0)

    hbm = pl.BlockSpec(memory_space=pl.ANY)
    grads = (n_side, n_fsdp) if x_first else (n_fsdp, n_side)
    dw_block = (1, n_fsdp) if x_first else (n_fsdp, 1)
    return pl.pallas_call(
        functools.partial(expert_kernel, expert_of=expert_of, x_first=x_first),
        grid_spec=pltpu.PrefetchScalarGridSpec(
            num_scalar_prefetch=2,
            grid=(n_side * size,),
            in_specs=[hbm, hbm, w_spec(0), w_spec(1)],
            out_specs=[hbm, hbm, pl.BlockSpec((*dw_block, three, 1, half, half), dw_index)],
            scratch_shapes=[pltpu.VMEM((2, TILE, d_model), BF16)] * 4 + [pltpu.SMEM((1,), jnp.int32)] + [pltpu.SemaphoreType.DMA((2, 2))] * 2,
        ),
        out_shape=[jax.ShapeDtypeStruct(rows.shape, BF16)] * 2 + [jax.ShapeDtypeStruct((*grads, three, size, half, half), F32)],
        input_output_aliases={2: 0, 3: 1},
        name='experts',
        **settings(56 * size, 100 * size),
    )(counts, flips, rows, d_rows, weights, weights)


def clear(ref):
    def rows(i, carry):
        ref[pl.ds(pl.multiple_of(i * LANES, LANES), LANES), :] = jnp.zeros((LANES, ref.shape[1]), ref.dtype)
        return carry

    lax.fori_loop(0, ref.shape[0] // LANES, rows, 0)


def combine_kernel(start_ref, rows_ref, off_ref, y_hbm, dr_hbm, dest_ref, gate_ref, *refs, base, own):
    ybuf, dbuf, acc_y, acc_d, sem = refs[-5:]
    step = pl.program_id(0)
    n_blocks = pl.num_programs(0)
    b = step + base
    n_exp = rows_ref.shape[1]
    slot = lax.rem(step, 2)

    def total(blk):
        return start_ref[blk, n_exp - 1] + rows_ref[blk, n_exp - 1]

    def fetch(blk, which):
        def one(e, carry):
            n = pl.multiple_of(rows_ref[blk, e], ALIGN)
            dst = pl.multiple_of(start_ref[blk, e], ALIGN)
            src = pl.multiple_of(off_ref[blk, e], ALIGN)

            @pl.when(n > 0)
            def _():
                pltpu.make_async_copy(y_hbm.at[e, pl.ds(src, n), :], ybuf.at[which, pl.ds(dst, n), :], sem.at[0, which]).start()
                pltpu.make_async_copy(dr_hbm.at[e, pl.ds(src, n), :], dbuf.at[which, pl.ds(dst, n), :], sem.at[1, which]).start()

            return carry

        lax.fori_loop(0, n_exp, one, 0)

    @pl.when(step == 0)
    def _():
        for which in range(2):
            clear(ybuf.at[which])
            clear(dbuf.at[which])
        fetch(b, 0)

    @pl.when(step + 1 < n_blocks)
    def _():
        fetch(b + 1, 1 - slot)

    n = pl.multiple_of(total(b), ALIGN)

    @pl.when(n > 0)
    def _():
        pltpu.make_async_copy(ybuf.at[slot, pl.ds(0, n), :], ybuf.at[slot, pl.ds(0, n), :], sem.at[0, slot]).wait()
        pltpu.make_async_copy(dbuf.at[slot, pl.ds(0, n), :], dbuf.at[slot, pl.ds(0, n), :], sem.at[1, slot]).wait()

    acc_y[...] = jnp.zeros(acc_y.shape, F32)
    acc_d[...] = jnp.zeros(acc_d.shape, F32)

    def tile(i, carry):
        first = pl.multiple_of(i * TILE, TILE)
        picked, ones = one_hot(dest_ref, gate_ref, first)
        acc_y[...] += tn_dot(picked, ybuf[slot, pl.ds(first, TILE), :])
        acc_d[...] += tn_dot(ones, dbuf[slot, pl.ds(first, TILE), :])
        return carry

    lax.fori_loop(0, (n + (TILE - 1)) // TILE, tile, 0)

    if not own:
        out_y, out_d = refs[:2]
        out_y[...] = acc_y[...]
        out_d[...] = acc_d[...]
        return
    more_y, more_d, h_ref, dout_ref, out_ref, dh_ref = refs[:6]
    hf = h_ref[...].astype(F32)
    out_ref[...] = (hf + (acc_y[...] + more_y[...])).astype(BF16)
    d_u = (acc_d[...] + more_d[...]).astype(BF16).astype(F32)
    inv = lax.rsqrt(jnp.mean(hf * hf, axis=-1, keepdims=True) + EPS)
    proj = jnp.mean(d_u * hf, axis=-1, keepdims=True)
    d_norm = (d_u * inv - hf * (inv * inv * inv * proj)).astype(BF16).astype(F32)
    dh_ref[...] = (dout_ref[...].astype(F32) + d_norm).astype(BF16)


def combine(y_rows, dr_rows, dest, gate, segs, base, n_blocks, extra):
    n_local, _, d_model = y_rows.shape
    top_k = dest.shape[1]
    buf_rows = block_rows(top_k, n_local)
    tok_spec = pl.BlockSpec((BLOCK, d_model), lambda b, *_: (b, 0))
    map_spec = pl.BlockSpec((1, top_k, BLOCK), lambda b, *_: (b + base, 0, 0))
    hbm = pl.BlockSpec(memory_space=pl.ANY)
    out = jax.ShapeDtypeStruct((n_blocks * BLOCK, d_model), BF16 if extra else F32)
    return pl.pallas_call(
        functools.partial(combine_kernel, base=base, own=bool(extra)),
        grid_spec=pltpu.PrefetchScalarGridSpec(
            num_scalar_prefetch=3,
            grid=(n_blocks,),
            in_specs=[hbm, hbm, map_spec, map_spec] + [tok_spec] * len(extra),
            out_specs=[tok_spec, tok_spec],
            scratch_shapes=[
                pltpu.VMEM((2, buf_rows, d_model), BF16),
                pltpu.VMEM((2, buf_rows, d_model), BF16),
                pltpu.VMEM((BLOCK, d_model), F32),
                pltpu.VMEM((BLOCK, d_model), F32),
                pltpu.SemaphoreType.DMA((2, 2)),
            ],
        ),
        out_shape=[out, out],
        name='combine',
        **settings(45, 120),
    )(*segs, y_rows, dr_rows, dest, gate, *extra)


def place_kernel(*refs, n_parts):
    for k, out_ref in enumerate(refs[-3:]):
        value = refs[0][k]
        for part_ref in refs[1:n_parts]:
            value = value + part_ref[k]
        out_ref[...] = value


def place(parts, held, first, n_total):
    three, size, rows, cols = parts[0].shape
    hbm = pl.BlockSpec(memory_space=pl.ANY)
    return pl.pallas_call(
        functools.partial(place_kernel, n_parts=len(parts)),
        grid=(size,),
        in_specs=[pl.BlockSpec((three, 1, rows, cols), lambda i: (0, i, 0, 0))] * len(parts) + [hbm] * len(held),
        out_specs=[pl.BlockSpec((1, rows, cols), lambda i: (first + i, 0, 0))] * three,
        out_shape=[jax.ShapeDtypeStruct((n_total, rows, cols), F32)] * three,
        input_output_aliases={len(parts) + k: k for k in range(len(held))},
        name='place',
        **settings(1, 12),
    )(*parts, *held)


CHUNKS = (2, 4)
CORES = 2


def solution(mesh):
    ep_size, fsdp_size = mesh.shape['ep'], mesh.shape['fsdp']
    tok_spec = P(('data', 'fsdp', 'ep'))
    in_specs = (tok_spec, P('fsdp'), P(None, None, 'fsdp'), P('ep', 'fsdp'), P('ep', 'fsdp'), P('ep', None, 'fsdp'), tok_spec, tok_spec, tok_spec, tok_spec)
    out_specs = (tok_spec, tok_spec, P(('data', 'ep'), 'fsdp'), P(('data', 'ep'), 'fsdp'), P(('data', 'ep'), None, 'fsdp'))

    def device_fn(tokens, w_qkv, w_out, w_gate, w_up, w_down, expert_idx, expert_slot, gate_wts, d_out):
        n_seq, seq_len, d_model = tokens.shape
        tok_count = n_seq * seq_len
        top_k = expert_idx.shape[2]
        local_experts, half, _ = w_gate.shape
        num_experts = local_experts * ep_size
        n_side = ep_size // CORES
        n_local = local_experts * n_side
        n_blocks = tok_count // BLOCK
        capacity = capacity_of(tok_count, top_k, num_experts)
        max_rows = -(-(CORES * (capacity + n_blocks * (ALIGN - 1))) // TILE) * TILE
        ep = lax.axis_index('ep')
        groups = [[c + CORES * i for i in range(fsdp_size * n_side)] for c in range(CORES)]

        fsdp, side = lax.axis_index('fsdp'), ep // CORES
        flips = jnp.stack([fsdp, side]).astype(jnp.int32)

        def swap(values):
            return lax.ppermute(values, 'ep', [(i, i ^ 1) for i in range(ep_size)])

        def swap_x(values):
            return lax.ppermute(values, 'ep', [(i, i ^ CORES) for i in range(ep_size)])

        def swap_y(values):
            return lax.ppermute(values, 'fsdp', [(i, i ^ 1) for i in range(fsdp_size)])

        def own_weights(part):
            return jnp.stack([w_gate[part], w_up[part], w_down[part]], axis=0)

        _, head_dim, _ = w_out.shape
        qkv_rows = w_qkv.transpose(1, 2, 3, 0).reshape(-1, half)
        qkv_rows = lax.dynamic_slice_in_dim(qkv_rows, ep * (3 * d_model // ep_size), 3 * d_model // ep_size, axis=0)
        out_rows = lax.dynamic_slice_in_dim(w_out.reshape(-1, half), ep * (d_model // ep_size), d_model // ep_size, axis=0)
        attn_w = lax.all_gather(jnp.concatenate([qkv_rows, out_rows], axis=0), ('fsdp', 'ep'), axis=0, tiled=False)
        attn_w = attn_w.reshape(fsdp_size, ep_size, -1, half)
        weights, first = [], 0
        for size in CHUNKS:
            mine = own_weights(slice(first, first + size))
            full = lax.all_gather(mine, ('fsdp', 'ep'), axis=0, tiled=False, axis_index_groups=groups)
            weights.append(full)
            first += size
        mid = first + (local_experts - first) // 2
        w_a, w_b = own_weights(slice(first, mid)), own_weights(slice(mid, local_experts))
        w_ax, w_ay, w_bx, w_by = swap_x(w_a), swap_y(w_a), swap_x(w_b), swap_y(w_b)

        dout_tok = d_out.reshape(tok_count, d_model)
        dout_other = swap(dout_tok)
        kept_ids = jnp.where(expert_slot >= 0, expert_idx, -1).transpose(0, 2, 1)
        all_ids = jnp.concatenate([kept_ids, swap(kept_ids)], axis=0)
        owner = all_ids // local_experts
        mine_too = (all_ids >= 0) & (lax.rem(owner, CORES) == lax.rem(ep, CORES))
        local_ids = jnp.where(mine_too, owner // CORES * local_experts + lax.rem(all_ids, local_experts), -1)
        dest, segs = route(local_ids, n_local)
        counts = jnp.sum(segs[1], axis=0)
        gate = gate_wts.transpose(0, 2, 1)
        gate = jnp.concatenate([gate, swap(gate)], axis=0)
        gate = gate.reshape(2 * n_seq, top_k, seq_len // BLOCK, BLOCK).transpose(0, 2, 1, 3).reshape(2 * n_blocks, top_k, BLOCK)

        tokens, dest, segs, counts, gate = lax.optimization_barrier((tokens, dest, segs, counts, gate))
        h_seq, qkv = attention(tokens, attn_w, head_dim)
        w_axy, w_byx = swap_y(w_ax), swap_x(w_by)
        w_a = jnp.stack([w_a, w_ax, w_ay, w_axy])
        w_b = jnp.stack([w_b, w_bx, w_by, w_byx])
        h_tok = h_seq.reshape(tok_count, d_model)
        h_other = swap(h_tok)
        held = dispatch(h_tok, dout_tok, dest, gate, segs, 0, [], n_local, max_rows)
        rows, d_rows = dispatch(h_other, dout_other, dest, gate, segs, n_blocks, held, n_local, max_rows)
        grads, start = [], 0
        for n, size in enumerate(CHUNKS):
            rows, d_rows, d_w = experts(rows, d_rows, weights[n], counts, jnp.zeros_like(flips), start, local_experts)
            d_w = d_w.reshape(fsdp_size * n_side, *d_w.shape[2:])
            grads.append(([lax.psum_scatter(d_w, ('fsdp', 'ep'), scatter_dimension=0, tiled=False, axis_index_groups=groups)], start))
            start += size
            if n == 0:
                rows, d_rows, d_a = experts(rows, d_rows, w_a, counts, flips, first, local_experts, x_first=True)
                rows, d_rows, d_b = experts(rows, d_rows, w_b, counts, flips, mid, local_experts)
                d_a, d_b = lax.optimization_barrier((d_a, d_b))
                more_a, more_b = swap_x(d_a[1]), swap_y(d_b[1])
        sums = d_a[0] + more_a, d_b[0] + more_b
        more_a, more_b = swap_y(sums[0][1]), swap_x(sums[1][1])
        done = [grads[0], ([sums[0][0], more_a], first), ([sums[1][0], more_b], mid), grads[1]]
        sums = combine(rows, d_rows, dest, gate, segs, n_blocks, n_blocks, [])
        more = [swap(value) for value in sums]
        layer_out, d_h = combine(rows, d_rows, dest, gate, segs, 0, n_blocks, [*more, h_tok, dout_tok])
        d_tokens = attention_grad(d_h.reshape(n_seq, seq_len, d_model), tokens, qkv, attn_w, head_dim)
        d_ws = []
        for parts, where in done:
            d_ws = place(parts, d_ws, where, local_experts)
        return layer_out.reshape(n_seq, seq_len, d_model), d_tokens, *d_ws

    return jax.shard_map(device_fn, mesh=mesh, in_specs=in_specs, out_specs=out_specs, check_vma=False)
```

```python
import functools
import math

import jax
import jax.numpy as jnp
from jax import lax
from jax.experimental import pallas as pl
from jax.experimental.pallas import tpu as pltpu
from jax.sharding import PartitionSpec as P


F32 = jnp.float32
BF16 = jnp.bfloat16
BLOCK = 256
TILE = 256
ALIGN = 16
LANES = 128
LOG2E = math.log2(math.e)
EPS = 1e-6
VMEM_BYTES = 60 * 2 ** 20


def settings(gflop, mbytes):
    return {
        'compiler_params': pltpu.CompilerParams(dimension_semantics=('arbitrary',), vmem_limit_bytes=VMEM_BYTES),
        'cost_estimate': pl.CostEstimate(flops=gflop * 10 ** 9, bytes_accessed=mbytes * 10 ** 6, transcendentals=0),
    }


def nt_dot(lhs, rhs):
    return lax.dot_general(lhs, rhs, (((1,), (1,)), ((), ())), preferred_element_type=F32)


def tn_dot(lhs, rhs):
    return lax.dot_general(lhs, rhs, (((0,), (0,)), ((), ())), preferred_element_type=F32)


def lanes_of(head, values):
    lane = lax.broadcasted_iota(jnp.int32, values.shape, 1)
    return jnp.where((lane >= LANES // 2) == bool(head), values, jnp.zeros_like(values))


def attention_kernel(x_ref, w_ref, h_ref, qkv_ref, ctx, *, head_dim):
    seq_len, d_model = x_ref.shape[1:]
    n_fsdp, n_ep, rows, half = w_ref.shape
    n_qkv = rows * 3 // 4
    x = x_ref[0].astype(F32)
    normed = (x * lax.rsqrt(jnp.mean(x * x, axis=-1, keepdims=True) + EPS)).astype(BF16)
    for p in range(n_ep):
        part = nt_dot(normed[:, :half], w_ref[0, p, :n_qkv]) + nt_dot(normed[:, half:], w_ref[1, p, :n_qkv])
        qkv_ref[0, :, p * n_qkv:(p + 1) * n_qkv] = part.astype(BF16)
    scale = head_dim ** -0.5 * LOG2E

    diagonal = lax.broadcasted_iota(jnp.int32, (BLOCK, BLOCK), 1) >= lax.broadcasted_iota(jnp.int32, (BLOCK, BLOCK), 0)

    def pair(i, carry):
        q2, k2, v2 = (qkv_ref[0, :, pl.ds(pl.multiple_of(t * d_model + i * LANES, LANES), LANES)] for t in range(3))
        for first in range(0, seq_len, BLOCK):
            both = []
            for head in range(2):
                query = lanes_of(head, q2[first:first + BLOCK])
                parts = [nt_dot(k2[at:at + BLOCK], query) * scale for at in range(0, first + BLOCK, BLOCK)]
                parts[-1] = jnp.where(diagonal, parts[-1], -1e30)
                top = functools.reduce(jnp.maximum, [jnp.max(part, axis=0, keepdims=True) for part in parts])
                parts = [jnp.exp2(part - top) for part in parts]
                inverse = 1.0 / sum(jnp.sum(part, axis=0, keepdims=True) for part in parts)
                probs = jnp.concatenate([(part * inverse).astype(BF16) for part in parts], axis=0)
                both.append(tn_dot(v2[:first + BLOCK], probs))
            row = lax.broadcasted_iota(jnp.int32, (LANES, BLOCK), 0)
            ctx[pl.ds(pl.multiple_of(i * LANES, LANES), LANES), first:first + BLOCK] = jnp.where(row < LANES // 2, both[0], both[1]).astype(BF16)
        return carry

    lax.fori_loop(0, d_model // LANES, pair, 0)
    for f in range(n_fsdp):
        w_out = jnp.concatenate([w_ref[f, p, n_qkv:] for p in range(n_ep)], axis=0)
        cols = slice(f * half, (f + 1) * half)
        h_ref[0, :, cols] = (x_ref[0, :, cols].astype(F32) + tn_dot(ctx[...], w_out)).astype(BF16)


def attention(tokens, weights, head_dim):
    n_seq, seq_len, d_model = tokens.shape
    seq_spec = pl.BlockSpec((1, seq_len, d_model), lambda s: (s, 0, 0))
    qkv_spec = pl.BlockSpec((1, seq_len, 3 * d_model), lambda s: (s, 0, 0))
    w_spec = pl.BlockSpec(weights.shape, lambda s: (0, 0, 0, 0))
    return pl.pallas_call(
        functools.partial(attention_kernel, head_dim=head_dim),
        grid=(n_seq,),
        in_specs=[seq_spec, w_spec],
        out_specs=[seq_spec, qkv_spec],
        out_shape=[jax.ShapeDtypeStruct(tokens.shape, BF16), jax.ShapeDtypeStruct((n_seq, seq_len, 3 * d_model), BF16)],
        scratch_shapes=[pltpu.VMEM((d_model, seq_len), BF16)],
        name='attention',
        **settings(90, 60),
    )(tokens, weights)


def attention_grad_kernel(dh_ref, x_ref, qkv_ref, w_ref, dx_ref, dctx, dqkv, *, head_dim):
    seq_len, d_model = x_ref.shape[1:]
    n_fsdp, n_ep, rows, half = w_ref.shape
    n_qkv = rows * 3 // 4
    n_out = rows - n_qkv
    dh = dh_ref[0]
    for p in range(n_ep):
        part = nt_dot(dh[:, :half], w_ref[0, p, n_qkv:]) + nt_dot(dh[:, half:], w_ref[1, p, n_qkv:])
        dctx[:, p * n_out:(p + 1) * n_out] = part.astype(BF16)
    scale = head_dim ** -0.5

    def pair(i, carry):
        col = pl.multiple_of(i * LANES, LANES)
        q2, k2, v2 = (qkv_ref[0, :, pl.ds(pl.multiple_of(t * d_model + i * LANES, LANES), LANES)] for t in range(3))
        d2 = dctx[:, pl.ds(col, LANES)]
        dk = [jnp.zeros((BLOCK, LANES), F32)] * (seq_len // BLOCK)
        dv = list(dk)
        for first in range(0, seq_len, BLOCK):
            end = first + BLOCK
            keys, vals = k2[:end], v2[:end]
            causal = lax.broadcasted_iota(jnp.int32, (end, BLOCK), 1) + first >= lax.broadcasted_iota(jnp.int32, (end, BLOCK), 0)
            dq = jnp.zeros((BLOCK, LANES), F32)
            for head in range(2):
                q, d = lanes_of(head, q2[first:end]), lanes_of(head, d2[first:end])
                scores = jnp.where(causal, nt_dot(keys, q) * (scale * LOG2E), -1e30)
                probs = jnp.exp2(scores - jnp.max(scores, axis=0, keepdims=True))
                probs = probs * (1.0 / jnp.sum(probs, axis=0, keepdims=True))
                d_probs = nt_dot(vals, d)
                d_scores = probs * (d_probs - jnp.sum(probs * d_probs, axis=0, keepdims=True))
                d_scores = (d_scores * scale).astype(BF16)
                dv_part = jnp.dot(probs.astype(BF16), d, preferred_element_type=F32)
                dk_part = jnp.dot(d_scores, q, preferred_element_type=F32)
                dq = dq + tn_dot(d_scores, lanes_of(head, keys))
                for n in range(end // BLOCK):
                    dk[n] = dk[n] + dk_part[n * BLOCK:(n + 1) * BLOCK]
                    dv[n] = dv[n] + dv_part[n * BLOCK:(n + 1) * BLOCK]
            dqkv[first:end, pl.ds(col, LANES)] = dq.astype(BF16)
        for n in range(seq_len // BLOCK):
            dqkv[n * BLOCK:(n + 1) * BLOCK, pl.ds(pl.multiple_of(d_model + i * LANES, LANES), LANES)] = dk[n].astype(BF16)
            dqkv[n * BLOCK:(n + 1) * BLOCK, pl.ds(pl.multiple_of(2 * d_model + i * LANES, LANES), LANES)] = dv[n].astype(BF16)
        return carry

    lax.fori_loop(0, d_model // LANES, pair, 0)
    x = x_ref[0].astype(F32)
    d_normed = []
    for f in range(n_fsdp):
        w_qkv = jnp.concatenate([w_ref[f, p, :n_qkv] for p in range(n_ep)], axis=0)
        d_normed.append(jnp.dot(dqkv[...], w_qkv, preferred_element_type=F32).astype(BF16))
    d_normed = jnp.concatenate(d_normed, axis=1).astype(F32)
    inv = lax.rsqrt(jnp.mean(x * x, axis=-1, keepdims=True) + EPS)
    proj = jnp.mean(d_normed * x, axis=-1, keepdims=True)
    d_x = (d_normed * inv - x * (inv * inv * inv * proj)).astype(BF16).astype(F32)
    dx_ref[0] = (dh_ref[0].astype(F32) + d_x).astype(BF16)


def attention_grad(d_h, tokens, qkv, weights, head_dim):
    n_seq, seq_len, d_model = tokens.shape
    seq_spec = pl.BlockSpec((1, seq_len, d_model), lambda s: (s, 0, 0))
    qkv_spec = pl.BlockSpec((1, seq_len, 3 * d_model), lambda s: (s, 0, 0))
    w_spec = pl.BlockSpec(weights.shape, lambda s: (0, 0, 0, 0))
    return pl.pallas_call(
        functools.partial(attention_grad_kernel, head_dim=head_dim),
        grid=(n_seq,),
        in_specs=[seq_spec, seq_spec, qkv_spec, w_spec],
        out_specs=seq_spec,
        out_shape=jax.ShapeDtypeStruct(tokens.shape, BF16),
        scratch_shapes=[pltpu.VMEM((seq_len, d_model), BF16), pltpu.VMEM((seq_len, 3 * d_model), BF16)],
        name='attention_grad',
        **settings(150, 70),
    )(d_h, tokens, qkv, weights)


def capacity_of(tok_count, top_k, num_experts):
    return max(8, (5 * tok_count * top_k // (4 * num_experts) + 7) // 8 * 8)


def route_kernel(loc_ref, dest_ref, start_ref, rows_ref, off_ref, total, *, n_local):
    top_k = loc_ref.shape[1]
    ids = lax.broadcasted_iota(jnp.int32, (n_local, BLOCK), 0)
    upper = (lax.broadcasted_iota(jnp.int32, (BLOCK, BLOCK), 0) <= lax.broadcasted_iota(jnp.int32, (BLOCK, BLOCK), 1)).astype(F32).astype(BF16)
    before = (lax.broadcasted_iota(jnp.int32, (n_local, n_local), 0) > lax.broadcasted_iota(jnp.int32, (n_local, n_local), 1)).astype(F32).astype(BF16)

    @pl.when(pl.program_id(0) == 0)
    def _():
        total[...] = jnp.zeros(total.shape, jnp.int32)

    so_far = total[...]
    for s in range(loc_ref.shape[0]):
        for p in range(loc_ref.shape[2] // BLOCK):
            q = s * (loc_ref.shape[2] // BLOCK) + p
            loc = loc_ref[s, :, p * BLOCK:(p + 1) * BLOCK]
            member = jnp.zeros((n_local, BLOCK), F32)
            for j in range(top_k):
                member = jnp.where(loc[j:j + 1] == ids, 1.0, member)
            count = jnp.dot(member.astype(BF16), upper, preferred_element_type=F32)
            units = (count[:, BLOCK - 1:].astype(jnp.int32) + (ALIGN - 1)) // ALIGN
            units = jnp.broadcast_to(units, (n_local, LANES))
            start = jnp.dot(before, units.astype(F32).astype(BF16), preferred_element_type=F32).astype(jnp.int32) * ALIGN
            place = start[:, :1] + count.astype(jnp.int32) - 1
            for j in range(top_k):
                row = jnp.sum(jnp.where(loc[j:j + 1] == ids, place, 0), axis=0, keepdims=True)
                dest_ref[q, j:j + 1, :] = jnp.where(loc[j:j + 1] >= 0, row, -1)
            start_ref[q] = start
            rows_ref[q] = units * ALIGN
            off_ref[q] = so_far
            so_far = so_far + units * ALIGN
    total[...] = so_far


def route(local_ids, n_local):
    n_seq, top_k, seq_len = local_ids.shape
    per_seq = seq_len // BLOCK
    step = 2 if n_seq % 2 == 0 else 1
    n_blocks = n_seq * per_seq
    seg = jax.ShapeDtypeStruct((n_blocks, n_local, LANES), jnp.int32)
    seg_spec = pl.BlockSpec((step * per_seq, n_local, LANES), lambda s: (s, 0, 0))
    dest, *segs = pl.pallas_call(
        functools.partial(route_kernel, n_local=n_local),
        grid=(n_seq // step,),
        in_specs=[pl.BlockSpec((step, top_k, seq_len), lambda s: (s, 0, 0))],
        out_specs=[pl.BlockSpec((step * per_seq, top_k, BLOCK), lambda s: (s, 0, 0)), seg_spec, seg_spec, seg_spec],
        out_shape=[jax.ShapeDtypeStruct((n_blocks, top_k, BLOCK), jnp.int32), seg, seg, seg],
        scratch_shapes=[pltpu.VMEM((n_local, LANES), jnp.int32)],
        name='route',
        **settings(1, 3),
    )(local_ids)
    return dest, [part[:, :, 0] for part in segs]


def one_hot(dest_ref, gate_ref, first_row):
    rows = lax.broadcasted_iota(jnp.int32, (TILE, BLOCK), 0).astype(F32).astype(BF16)
    dest = jnp.clip(dest_ref[0] - first_row, -1, TILE).astype(F32).astype(BF16)
    gate = gate_ref[0]
    picked = jnp.zeros((TILE, BLOCK), BF16)
    for j in range(dest.shape[0]):
        picked = jnp.where(rows == dest[j:j + 1], gate[j:j + 1], picked)
    return picked, jnp.where(picked > 0, jnp.ones_like(picked), jnp.zeros_like(picked))


def dispatch_kernel(start_ref, rows_ref, off_ref, h_ref, dout_ref, dest_ref, gate_ref, *refs, base):
    r_hbm, d_hbm, u_s, rbuf, dbuf, sem = refs[-6:]
    step = pl.program_id(0)
    n_blocks = pl.num_programs(0)
    b = step + base
    n_exp = rows_ref.shape[1]
    slot = lax.rem(b, 2)

    def total(blk):
        return start_ref[blk, n_exp - 1] + rows_ref[blk, n_exp - 1]

    def drain(blk, which):
        n = pl.multiple_of(total(blk), ALIGN)

        @pl.when(n > 0)
        def _():
            pltpu.make_async_copy(rbuf.at[which, pl.ds(0, n), :], rbuf.at[which, pl.ds(0, n), :], sem.at[0, which]).wait()
            pltpu.make_async_copy(dbuf.at[which, pl.ds(0, n), :], dbuf.at[which, pl.ds(0, n), :], sem.at[1, which]).wait()

    @pl.when(step >= 2)
    def _():
        drain(b - 2, slot)

    hf = h_ref[...].astype(F32)
    u_s[...] = (hf * lax.rsqrt(jnp.mean(hf * hf, axis=-1, keepdims=True) + EPS)).astype(BF16)

    def tile(i, carry):
        first = pl.multiple_of(i * TILE, TILE)
        picked, ones = one_hot(dest_ref, gate_ref, first)
        rbuf[slot, pl.ds(first, TILE), :] = jnp.dot(ones, u_s[...], preferred_element_type=F32).astype(BF16)
        dbuf[slot, pl.ds(first, TILE), :] = jnp.dot(picked, dout_ref[...], preferred_element_type=F32).astype(BF16)
        return carry

    lax.fori_loop(0, (total(b) + (TILE - 1)) // TILE, tile, 0)

    def send(e, carry):
        n = pl.multiple_of(rows_ref[b, e], ALIGN)
        src = pl.multiple_of(start_ref[b, e], ALIGN)
        dst = pl.multiple_of(off_ref[b, e], ALIGN)

        @pl.when(n > 0)
        def _():
            pltpu.make_async_copy(rbuf.at[slot, pl.ds(src, n), :], r_hbm.at[e, pl.ds(dst, n), :], sem.at[0, slot]).start()
            pltpu.make_async_copy(dbuf.at[slot, pl.ds(src, n), :], d_hbm.at[e, pl.ds(dst, n), :], sem.at[1, slot]).start()

        return carry

    lax.fori_loop(0, n_exp, send, 0)

    @pl.when(step == n_blocks - 1)
    def _():
        @pl.when(n_blocks > 1)
        def _():
            drain(b - 1, 1 - slot)

        drain(b, slot)


def block_rows(top_k, n_local):
    return -(-(BLOCK * top_k + n_local * (ALIGN - 1)) // TILE) * TILE


def dispatch(h_tok, dout_tok, dest, gate, segs, base, held, n_local, max_rows):
    tok_count, d_model = h_tok.shape
    top_k = dest.shape[1]
    n_blocks = tok_count // BLOCK
    buf_rows = block_rows(top_k, n_local)
    tok_spec = pl.BlockSpec((BLOCK, d_model), lambda b, *_: (b, 0))
    map_spec = pl.BlockSpec((1, top_k, BLOCK), lambda b, *_: (b + base, 0, 0))
    rows_shape = jax.ShapeDtypeStruct((n_local, max_rows, d_model), BF16)
    hbm = pl.BlockSpec(memory_space=pl.ANY)
    return pl.pallas_call(
        functools.partial(dispatch_kernel, base=base),
        grid_spec=pltpu.PrefetchScalarGridSpec(
            num_scalar_prefetch=3,
            grid=(n_blocks,),
            in_specs=[tok_spec, tok_spec, map_spec, map_spec] + [hbm] * len(held),
            out_specs=[hbm, hbm],
            scratch_shapes=[
                pltpu.VMEM((BLOCK, d_model), BF16),
                pltpu.VMEM((2, buf_rows, d_model), BF16),
                pltpu.VMEM((2, buf_rows, d_model), BF16),
                pltpu.SemaphoreType.DMA((2, 2)),
            ],
        ),
        out_shape=[rows_shape, rows_shape],
        input_output_aliases={7: 0, 8: 1} if held else {},
        name='dispatch',
        **settings(40, 90),
    )(*segs, h_tok, dout_tok, dest, gate, *held)


def expert_kernel(count_ref, flip_ref, r_hbm, d_hbm, w_lo, w_hi, y_hbm, dr_hbm, dw_ref, rbuf, dbuf, ybuf, drbuf, done, in_sem, out_sem, *, expert_of, x_first):
    step = pl.program_id(0)
    n_steps = pl.num_programs(0)
    expert = expert_of(step)
    n_rows = count_ref[expert]
    n_tiles = jnp.maximum((n_rows + (TILE - 1)) // TILE, 1)
    half = dw_ref.shape[-1]

    def copies(who, i, slot, load):
        rows = pl.ds(pl.multiple_of(i * TILE, TILE), TILE)
        pairs = ((r_hbm, rbuf), (d_hbm, dbuf)) if load else ((ybuf, y_hbm), (drbuf, dr_hbm))
        for k, (src, dst) in enumerate(pairs):
            src = src.at[who, rows, :] if load else src.at[slot]
            dst = dst.at[slot] if load else dst.at[who, rows, :]
            yield pltpu.make_async_copy(src, dst, (in_sem if load else out_sem).at[k, slot])

    def start(*args):
        for copy in copies(*args):
            copy.start()

    def wait(*args):
        for copy in copies(*args):
            copy.wait()

    @pl.when(step == 0)
    def _():
        done[0] = 0
        start(expert, 0, 0, True)

    before = done[0]
    for p in range(dw_ref.shape[0]):
        for q in range(dw_ref.shape[1]):
            for t in range(dw_ref.shape[2]):
                clear(dw_ref.at[p, q, t, 0])

    def tile(i, carry):
        slot = lax.rem(before + i, 2)

        @pl.when(i + 1 < n_tiles)
        def _():
            start(expert, i + 1, 1 - slot, True)

        @pl.when((i + 1 == n_tiles) & (step + 1 < n_steps))
        def _():
            start(expert_of(step + 1), 0, 1 - slot, True)

        wait(expert, i, slot, True)

        @pl.when(before + i >= 2)
        def _():
            wait(expert, i, slot, False)

        valid = lax.broadcasted_iota(jnp.int32, (TILE, 1), 0) + i * TILE < n_rows
        r = jnp.where(valid, rbuf[slot], 0)
        dy = jnp.where(valid, dbuf[slot], 0)
        w1, w3, w2 = (jnp.concatenate([w[0, t, 0] for w in (w_lo, w_hi)], axis=t // 2) for t in range(3))
        act_a = jnp.dot(r, w1, preferred_element_type=F32)
        act_b = jnp.dot(r, w3, preferred_element_type=F32)
        d_g = nt_dot(dy, w2)
        sig = 1.0 / (1.0 + jnp.exp(-act_a))
        silu = act_a * sig
        g = (silu * act_b).astype(BF16)
        d_up = (d_g * silu).astype(BF16)
        d_gate = (d_g * act_b * sig * (1.0 + act_a * (1.0 - sig))).astype(BF16)
        ybuf[slot] = jnp.dot(g, w2, preferred_element_type=F32).astype(BF16)
        drbuf[slot] = (nt_dot(d_gate, w1) + nt_dot(d_up, w3)).astype(BF16)
        start(expert, i, slot, False)
        for f in range(2):
            part = slice(f * half, (f + 1) * half)
            to = lax.rem(f + flip_ref[0], 2)
            for t, (lhs, rhs) in enumerate(((r[:, part], d_gate), (r[:, part], d_up), (g, dy[:, part]))):
                dw_ref[(0, to, t, 0) if x_first else (to, 0, t, 0)] += tn_dot(lhs, rhs)
        return carry

    lax.fori_loop(0, n_tiles, tile, 0)
    done[0] = before + n_tiles

    @pl.when(step == n_steps - 1)
    def _():
        last = before + n_tiles - 1
        wait(expert, 0, lax.rem(last, 2), False)

        @pl.when(last >= 1)
        def _():
            wait(expert, 0, lax.rem(last + 1, 2), False)


def experts(rows, d_rows, weights, counts, flips, first, local_experts, x_first=False):
    d_model = rows.shape[2]
    n_owners, three, size, half, _ = weights.shape
    n_fsdp = d_model // half
    n_side = n_owners // n_fsdp

    def expert_of(g):
        return g // size * local_experts + first + lax.rem(g, size)

    def side(g, flip):
        return lax.rem(g // size + flip[1], n_side)

    def w_spec(f):
        return pl.BlockSpec((1, three, 1, half, half), lambda g, _, flip: (lax.rem(f + flip[0], n_fsdp) * n_side + side(g, flip), 0, lax.rem(g, size), 0, 0))

    def dw_index(g, _, flip):
        place = (side(g, flip), 0) if x_first else (0, side(g, flip))
        return (*place, 0, lax.rem(g, size), 0, 0)

    hbm = pl.BlockSpec(memory_space=pl.ANY)
    grads = (n_side, n_fsdp) if x_first else (n_fsdp, n_side)
    dw_block = (1, n_fsdp) if x_first else (n_fsdp, 1)
    return pl.pallas_call(
        functools.partial(expert_kernel, expert_of=expert_of, x_first=x_first),
        grid_spec=pltpu.PrefetchScalarGridSpec(
            num_scalar_prefetch=2,
            grid=(n_side * size,),
            in_specs=[hbm, hbm, w_spec(0), w_spec(1)],
            out_specs=[hbm, hbm, pl.BlockSpec((*dw_block, three, 1, half, half), dw_index)],
            scratch_shapes=[pltpu.VMEM((2, TILE, d_model), BF16)] * 4 + [pltpu.SMEM((1,), jnp.int32)] + [pltpu.SemaphoreType.DMA((2, 2))] * 2,
        ),
        out_shape=[jax.ShapeDtypeStruct(rows.shape, BF16)] * 2 + [jax.ShapeDtypeStruct((*grads, three, size, half, half), F32)],
        input_output_aliases={2: 0, 3: 1},
        name='experts',
        **settings(56 * size, 100 * size),
    )(counts, flips, rows, d_rows, weights, weights)


def clear(ref):
    def rows(i, carry):
        ref[pl.ds(pl.multiple_of(i * LANES, LANES), LANES), :] = jnp.zeros((LANES, ref.shape[1]), ref.dtype)
        return carry

    lax.fori_loop(0, ref.shape[0] // LANES, rows, 0)


def combine_kernel(start_ref, rows_ref, off_ref, y_hbm, dr_hbm, dest_ref, gate_ref, *refs, base, own):
    ybuf, dbuf, acc_y, acc_d, sem = refs[-5:]
    step = pl.program_id(0)
    n_blocks = pl.num_programs(0)
    b = step + base
    n_exp = rows_ref.shape[1]
    slot = lax.rem(step, 2)

    def total(blk):
        return start_ref[blk, n_exp - 1] + rows_ref[blk, n_exp - 1]

    def fetch(blk, which):
        def one(e, carry):
            n = pl.multiple_of(rows_ref[blk, e], ALIGN)
            dst = pl.multiple_of(start_ref[blk, e], ALIGN)
            src = pl.multiple_of(off_ref[blk, e], ALIGN)

            @pl.when(n > 0)
            def _():
                pltpu.make_async_copy(y_hbm.at[e, pl.ds(src, n), :], ybuf.at[which, pl.ds(dst, n), :], sem.at[0, which]).start()
                pltpu.make_async_copy(dr_hbm.at[e, pl.ds(src, n), :], dbuf.at[which, pl.ds(dst, n), :], sem.at[1, which]).start()

            return carry

        lax.fori_loop(0, n_exp, one, 0)

    @pl.when(step == 0)
    def _():
        for which in range(2):
            clear(ybuf.at[which])
            clear(dbuf.at[which])
        fetch(b, 0)

    @pl.when(step + 1 < n_blocks)
    def _():
        fetch(b + 1, 1 - slot)

    n = pl.multiple_of(total(b), ALIGN)

    @pl.when(n > 0)
    def _():
        pltpu.make_async_copy(ybuf.at[slot, pl.ds(0, n), :], ybuf.at[slot, pl.ds(0, n), :], sem.at[0, slot]).wait()
        pltpu.make_async_copy(dbuf.at[slot, pl.ds(0, n), :], dbuf.at[slot, pl.ds(0, n), :], sem.at[1, slot]).wait()

    acc_y[...] = jnp.zeros(acc_y.shape, F32)
    acc_d[...] = jnp.zeros(acc_d.shape, F32)

    def tile(i, carry):
        first = pl.multiple_of(i * TILE, TILE)
        picked, ones = one_hot(dest_ref, gate_ref, first)
        acc_y[...] += tn_dot(picked, ybuf[slot, pl.ds(first, TILE), :])
        acc_d[...] += tn_dot(ones, dbuf[slot, pl.ds(first, TILE), :])
        return carry

    lax.fori_loop(0, (n + (TILE - 1)) // TILE, tile, 0)

    if not own:
        out_y, out_d = refs[:2]
        out_y[...] = acc_y[...]
        out_d[...] = acc_d[...]
        return
    more_y, more_d, h_ref, dout_ref, out_ref, dh_ref = refs[:6]
    hf = h_ref[...].astype(F32)
    out_ref[...] = (hf + (acc_y[...] + more_y[...])).astype(BF16)
    d_u = (acc_d[...] + more_d[...]).astype(BF16).astype(F32)
    inv = lax.rsqrt(jnp.mean(hf * hf, axis=-1, keepdims=True) + EPS)
    proj = jnp.mean(d_u * hf, axis=-1, keepdims=True)
    d_norm = (d_u * inv - hf * (inv * inv * inv * proj)).astype(BF16).astype(F32)
    dh_ref[...] = (dout_ref[...].astype(F32) + d_norm).astype(BF16)


def combine(y_rows, dr_rows, dest, gate, segs, base, n_blocks, extra):
    n_local, _, d_model = y_rows.shape
    top_k = dest.shape[1]
    buf_rows = block_rows(top_k, n_local)
    tok_spec = pl.BlockSpec((BLOCK, d_model), lambda b, *_: (b, 0))
    map_spec = pl.BlockSpec((1, top_k, BLOCK), lambda b, *_: (b + base, 0, 0))
    hbm = pl.BlockSpec(memory_space=pl.ANY)
    out = jax.ShapeDtypeStruct((n_blocks * BLOCK, d_model), BF16 if extra else F32)
    return pl.pallas_call(
        functools.partial(combine_kernel, base=base, own=bool(extra)),
        grid_spec=pltpu.PrefetchScalarGridSpec(
            num_scalar_prefetch=3,
            grid=(n_blocks,),
            in_specs=[hbm, hbm, map_spec, map_spec] + [tok_spec] * len(extra),
            out_specs=[tok_spec, tok_spec],
            scratch_shapes=[
                pltpu.VMEM((2, buf_rows, d_model), BF16),
                pltpu.VMEM((2, buf_rows, d_model), BF16),
                pltpu.VMEM((BLOCK, d_model), F32),
                pltpu.VMEM((BLOCK, d_model), F32),
                pltpu.SemaphoreType.DMA((2, 2)),
            ],
        ),
        out_shape=[out, out],
        name='combine',
        **settings(45, 120),
    )(*segs, y_rows, dr_rows, dest, gate, *extra)


def place_kernel(*refs, n_parts):
    for k, out_ref in enumerate(refs[-3:]):
        value = refs[0][k]
        for part_ref in refs[1:n_parts]:
            value = value + part_ref[k]
        out_ref[...] = value


def place(parts, held, first, n_total):
    three, size, rows, cols = parts[0].shape
    hbm = pl.BlockSpec(memory_space=pl.ANY)
    return pl.pallas_call(
        functools.partial(place_kernel, n_parts=len(parts)),
        grid=(size,),
        in_specs=[pl.BlockSpec((three, 1, rows, cols), lambda i: (0, i, 0, 0))] * len(parts) + [hbm] * len(held),
        out_specs=[pl.BlockSpec((1, rows, cols), lambda i: (first + i, 0, 0))] * three,
        out_shape=[jax.ShapeDtypeStruct((n_total, rows, cols), F32)] * three,
        input_output_aliases={len(parts) + k: k for k in range(len(held))},
        name='place',
        **settings(1, 12),
    )(*parts, *held)


CHUNKS = (2, 4)
CORES = 2


def solution(mesh):
    ep_size, fsdp_size = mesh.shape['ep'], mesh.shape['fsdp']
    tok_spec = P(('data', 'fsdp', 'ep'))
    in_specs = (tok_spec, P('fsdp'), P(None, None, 'fsdp'), P('ep', 'fsdp'), P('ep', 'fsdp'), P('ep', None, 'fsdp'), tok_spec, tok_spec, tok_spec, tok_spec)
    out_specs = (tok_spec, tok_spec, P(('data', 'ep'), 'fsdp'), P(('data', 'ep'), 'fsdp'), P(('data', 'ep'), None, 'fsdp'))

    def device_fn(tokens, w_qkv, w_out, w_gate, w_up, w_down, expert_idx, expert_slot, gate_wts, d_out):
        n_seq, seq_len, d_model = tokens.shape
        tok_count = n_seq * seq_len
        top_k = expert_idx.shape[2]
        local_experts, half, _ = w_gate.shape
        num_experts = local_experts * ep_size
        n_side = ep_size // CORES
        n_local = local_experts * n_side
        n_blocks = tok_count // BLOCK
        capacity = capacity_of(tok_count, top_k, num_experts)
        max_rows = -(-(CORES * (capacity + n_blocks * (ALIGN - 1))) // TILE) * TILE
        ep = lax.axis_index('ep')
        groups = [[c + CORES * i for i in range(fsdp_size * n_side)] for c in range(CORES)]

        fsdp, side = lax.axis_index('fsdp'), ep // CORES
        flips = jnp.stack([fsdp, side]).astype(jnp.int32)

        def swap(values):
            return lax.ppermute(values, 'ep', [(i, i ^ 1) for i in range(ep_size)])

        def swap_x(values):
            return lax.ppermute(values, 'ep', [(i, i ^ CORES) for i in range(ep_size)])

        def swap_y(values):
            return lax.ppermute(values, 'fsdp', [(i, i ^ 1) for i in range(fsdp_size)])

        def own_weights(part):
            return jnp.stack([w[part] for w in all_w], axis=0)

        _, head_dim, _ = w_out.shape
        qkv_rows = w_qkv.transpose(1, 2, 3, 0).reshape(-1, half)
        qkv_rows = lax.dynamic_slice_in_dim(qkv_rows, ep * (3 * d_model // ep_size), 3 * d_model // ep_size, axis=0)
        out_rows = lax.dynamic_slice_in_dim(w_out.reshape(-1, half), ep * (d_model // ep_size), d_model // ep_size, axis=0)
        attn_w = lax.all_gather(jnp.concatenate([qkv_rows, out_rows], axis=0), ('fsdp', 'ep'), axis=0, tiled=False)
        attn_w = attn_w.reshape(fsdp_size, ep_size, -1, half)
        all_w = w_gate, w_up, w_down
        first = sum(CHUNKS)
        mid = first + (local_experts - first) // 2
        w_a, w_b = own_weights(slice(first, mid)), own_weights(slice(mid, local_experts))
        w_ax, w_ay, w_bx, w_by = swap_x(w_a), swap_y(w_a), swap_x(w_b), swap_y(w_b)
        weights, start = [], 0
        all_w, w_a, w_b = lax.optimization_barrier((all_w, w_a, w_b))
        for size in CHUNKS:
            mine = own_weights(slice(start, start + size))
            weights.append(lax.all_gather(mine, ('fsdp', 'ep'), axis=0, tiled=False, axis_index_groups=groups))
            start += size

        dout_tok = d_out.reshape(tok_count, d_model)
        dout_other = swap(dout_tok)
        kept_ids = jnp.where(expert_slot >= 0, expert_idx, -1).transpose(0, 2, 1)
        all_ids = jnp.concatenate([kept_ids, swap(kept_ids)], axis=0)
        owner = all_ids // local_experts
        mine_too = (all_ids >= 0) & (lax.rem(owner, CORES) == lax.rem(ep, CORES))
        local_ids = jnp.where(mine_too, owner // CORES * local_experts + lax.rem(all_ids, local_experts), -1)
        dest, segs = route(local_ids, n_local)
        counts = jnp.sum(segs[1], axis=0)
        gate = gate_wts.transpose(0, 2, 1)
        gate = jnp.concatenate([gate, swap(gate)], axis=0)
        gate = gate.reshape(2 * n_seq, top_k, seq_len // BLOCK, BLOCK).transpose(0, 2, 1, 3).reshape(2 * n_blocks, top_k, BLOCK)

        tokens, dest, segs, counts, gate = lax.optimization_barrier((tokens, dest, segs, counts, gate))
        h_seq, qkv = attention(tokens, attn_w, head_dim)
        w_axy, w_byx = swap_y(w_ax), swap_x(w_by)
        w_a = jnp.stack([w_a, w_ax, w_ay, w_axy])
        w_b = jnp.stack([w_b, w_bx, w_by, w_byx])
        h_tok = h_seq.reshape(tok_count, d_model)
        h_other = swap(h_tok)
        held = dispatch(h_tok, dout_tok, dest, gate, segs, 0, [], n_local, max_rows)
        rows, d_rows = dispatch(h_other, dout_other, dest, gate, segs, n_blocks, held, n_local, max_rows)
        grads, start = [], 0
        for n, size in enumerate(CHUNKS):
            rows, d_rows, d_w = experts(rows, d_rows, weights[n], counts, jnp.zeros_like(flips), start, local_experts)
            d_w = d_w.reshape(fsdp_size * n_side, *d_w.shape[2:])
            grads.append(([lax.psum_scatter(d_w, ('fsdp', 'ep'), scatter_dimension=0, tiled=False, axis_index_groups=groups)], start))
            start += size
            if n == 0:
                rows, d_rows, d_a = experts(rows, d_rows, w_a, counts, flips, first, local_experts, x_first=True)
                rows, d_rows, d_b = experts(rows, d_rows, w_b, counts, flips, mid, local_experts)
                d_a, d_b = lax.optimization_barrier((d_a, d_b))
                more_a, more_b = swap_x(d_a[1]), swap_y(d_b[1])
        sums = d_a[0] + more_a, d_b[0] + more_b
        more_a, more_b = swap_y(sums[0][1]), swap_x(sums[1][1])
        done = [grads[0], ([sums[0][0], more_a], first), ([sums[1][0], more_b], mid), grads[1]]
        sums = combine(rows, d_rows, dest, gate, segs, n_blocks, n_blocks, [])
        more = [swap(value) for value in sums]
        layer_out, d_h = combine(rows, d_rows, dest, gate, segs, 0, n_blocks, [*more, h_tok, dout_tok])
        d_tokens = attention_grad(d_h.reshape(n_seq, seq_len, d_model), tokens, qkv, attn_w, head_dim)
        d_ws = []
        for parts, where in done:
            d_ws = place(parts, d_ws, where, local_experts)
        return layer_out.reshape(n_seq, seq_len, d_model), d_tokens, *d_ws

    return jax.shard_map(device_fn, mesh=mesh, in_specs=in_specs, out_specs=out_specs, check_vma=False)
```

```python
import functools
import math

import jax
import jax.numpy as jnp
from jax import lax
from jax.experimental import pallas as pl
from jax.experimental.pallas import tpu as pltpu
from jax.sharding import PartitionSpec as P


F32 = jnp.float32
BF16 = jnp.bfloat16
BLOCK = 256
TILE = 256
ALIGN = 16
LANES = 128
LOG2E = math.log2(math.e)
EPS = 1e-6
VMEM_BYTES = 60 * 2 ** 20


def settings(gflop, mbytes):
    return {
        'compiler_params': pltpu.CompilerParams(dimension_semantics=('arbitrary',), vmem_limit_bytes=VMEM_BYTES),
        'cost_estimate': pl.CostEstimate(flops=gflop * 10 ** 9, bytes_accessed=mbytes * 10 ** 6, transcendentals=0),
    }


def nt_dot(lhs, rhs):
    return lax.dot_general(lhs, rhs, (((1,), (1,)), ((), ())), preferred_element_type=F32)


def tn_dot(lhs, rhs):
    return lax.dot_general(lhs, rhs, (((0,), (0,)), ((), ())), preferred_element_type=F32)


def lanes_of(head, values):
    lane = lax.broadcasted_iota(jnp.int32, values.shape, 1)
    return jnp.where((lane >= LANES // 2) == bool(head), values, jnp.zeros_like(values))


def attention_kernel(x_ref, w_ref, h_ref, qkv_ref, ctx, *, head_dim):
    seq_len, d_model = x_ref.shape[1:]
    n_fsdp, n_ep, rows, half = w_ref.shape
    n_qkv = rows * 3 // 4
    x = x_ref[0].astype(F32)
    normed = (x * lax.rsqrt(jnp.mean(x * x, axis=-1, keepdims=True) + EPS)).astype(BF16)

    def project(p, carry):
        part = nt_dot(normed[:, :half], w_ref[0, p, :n_qkv]) + nt_dot(normed[:, half:], w_ref[1, p, :n_qkv])
        qkv_ref[0, :, pl.ds(pl.multiple_of(p * n_qkv, LANES), n_qkv)] = part.astype(BF16)
        return carry

    lax.fori_loop(0, n_ep, project, 0)
    scale = head_dim ** -0.5 * LOG2E

    diagonal = lax.broadcasted_iota(jnp.int32, (BLOCK, BLOCK), 1) >= lax.broadcasted_iota(jnp.int32, (BLOCK, BLOCK), 0)

    def pair(i, carry):
        q2, k2, v2 = (qkv_ref[0, :, pl.ds(pl.multiple_of(t * d_model + i * LANES, LANES), LANES)] for t in range(3))
        for first in range(0, seq_len, BLOCK):
            both = []
            for head in range(2):
                query = lanes_of(head, q2[first:first + BLOCK])
                parts = [nt_dot(k2[at:at + BLOCK], query) * scale for at in range(0, first + BLOCK, BLOCK)]
                parts[-1] = jnp.where(diagonal, parts[-1], -1e30)
                top = functools.reduce(jnp.maximum, [jnp.max(part, axis=0, keepdims=True) for part in parts])
                parts = [jnp.exp2(part - top) for part in parts]
                inverse = 1.0 / sum(jnp.sum(part, axis=0, keepdims=True) for part in parts)
                probs = jnp.concatenate([(part * inverse).astype(BF16) for part in parts], axis=0)
                both.append(tn_dot(v2[:first + BLOCK], probs))
            row = lax.broadcasted_iota(jnp.int32, (LANES, BLOCK), 0)
            ctx[pl.ds(pl.multiple_of(i * LANES, LANES), LANES), first:first + BLOCK] = jnp.where(row < LANES // 2, both[0], both[1]).astype(BF16)
        return carry

    lax.fori_loop(0, d_model // LANES, pair, 0)

    def finish(f, carry):
        w_out = jnp.concatenate([w_ref[f, p, n_qkv:] for p in range(n_ep)], axis=0)
        cols = pl.ds(pl.multiple_of(f * half, LANES), half)
        h_ref[0, :, cols] = (x_ref[0, :, cols].astype(F32) + tn_dot(ctx[...], w_out)).astype(BF16)
        return carry

    lax.fori_loop(0, n_fsdp, finish, 0)


def attention(tokens, weights, head_dim):
    n_seq, seq_len, d_model = tokens.shape
    seq_spec = pl.BlockSpec((1, seq_len, d_model), lambda s: (s, 0, 0))
    qkv_spec = pl.BlockSpec((1, seq_len, 3 * d_model), lambda s: (s, 0, 0))
    w_spec = pl.BlockSpec(weights.shape, lambda s: (0, 0, 0, 0))
    return pl.pallas_call(
        functools.partial(attention_kernel, head_dim=head_dim),
        grid=(n_seq,),
        in_specs=[seq_spec, w_spec],
        out_specs=[seq_spec, qkv_spec],
        out_shape=[jax.ShapeDtypeStruct(tokens.shape, BF16), jax.ShapeDtypeStruct((n_seq, seq_len, 3 * d_model), BF16)],
        scratch_shapes=[pltpu.VMEM((d_model, seq_len), BF16)],
        name='attention',
        **settings(90, 60),
    )(tokens, weights)


def attention_grad_kernel(dh_ref, x_ref, qkv_ref, w_ref, dx_ref, dctx, dqkv, *, head_dim):
    seq_len, d_model = x_ref.shape[1:]
    n_fsdp, n_ep, rows, half = w_ref.shape
    n_qkv = rows * 3 // 4
    n_out = rows - n_qkv
    dh = dh_ref[0]

    def project(p, carry):
        part = nt_dot(dh[:, :half], w_ref[0, p, n_qkv:]) + nt_dot(dh[:, half:], w_ref[1, p, n_qkv:])
        dctx[:, pl.ds(pl.multiple_of(p * n_out, LANES), n_out)] = part.astype(BF16)
        return carry

    lax.fori_loop(0, n_ep, project, 0)
    scale = head_dim ** -0.5

    def pair(i, carry):
        col = pl.multiple_of(i * LANES, LANES)
        q2, k2, v2 = (qkv_ref[0, :, pl.ds(pl.multiple_of(t * d_model + i * LANES, LANES), LANES)] for t in range(3))
        d2 = dctx[:, pl.ds(col, LANES)]
        dk = [jnp.zeros((BLOCK, LANES), F32)] * (seq_len // BLOCK)
        dv = list(dk)
        for first in range(0, seq_len, BLOCK):
            end = first + BLOCK
            keys, vals = k2[:end], v2[:end]
            causal = lax.broadcasted_iota(jnp.int32, (end, BLOCK), 1) + first >= lax.broadcasted_iota(jnp.int32, (end, BLOCK), 0)
            dq = jnp.zeros((BLOCK, LANES), F32)
            for head in range(2):
                q, d = lanes_of(head, q2[first:end]), lanes_of(head, d2[first:end])
                scores = jnp.where(causal, nt_dot(keys, q) * (scale * LOG2E), -1e30)
                probs = jnp.exp2(scores - jnp.max(scores, axis=0, keepdims=True))
                probs = probs * (1.0 / jnp.sum(probs, axis=0, keepdims=True))
                d_probs = nt_dot(vals, d)
                d_scores = probs * (d_probs - jnp.sum(probs * d_probs, axis=0, keepdims=True))
                d_scores = (d_scores * scale).astype(BF16)
                dv_part = jnp.dot(probs.astype(BF16), d, preferred_element_type=F32)
                dk_part = jnp.dot(d_scores, q, preferred_element_type=F32)
                dq = dq + tn_dot(d_scores, lanes_of(head, keys))
                for n in range(end // BLOCK):
                    dk[n] = dk[n] + dk_part[n * BLOCK:(n + 1) * BLOCK]
                    dv[n] = dv[n] + dv_part[n * BLOCK:(n + 1) * BLOCK]
            dqkv[first:end, pl.ds(col, LANES)] = dq.astype(BF16)
        for n in range(seq_len // BLOCK):
            dqkv[n * BLOCK:(n + 1) * BLOCK, pl.ds(pl.multiple_of(d_model + i * LANES, LANES), LANES)] = dk[n].astype(BF16)
            dqkv[n * BLOCK:(n + 1) * BLOCK, pl.ds(pl.multiple_of(2 * d_model + i * LANES, LANES), LANES)] = dv[n].astype(BF16)
        return carry

    lax.fori_loop(0, d_model // LANES, pair, 0)
    x = x_ref[0].astype(F32)

    def back(f, carry):
        w_qkv = jnp.concatenate([w_ref[f, p, :n_qkv] for p in range(n_ep)], axis=0)
        dctx[:, pl.ds(pl.multiple_of(f * half, LANES), half)] = jnp.dot(dqkv[...], w_qkv, preferred_element_type=F32).astype(BF16)
        return carry

    lax.fori_loop(0, n_fsdp, back, 0)
    d_normed = dctx[...].astype(F32)
    inv = lax.rsqrt(jnp.mean(x * x, axis=-1, keepdims=True) + EPS)
    proj = jnp.mean(d_normed * x, axis=-1, keepdims=True)
    d_x = (d_normed * inv - x * (inv * inv * inv * proj)).astype(BF16).astype(F32)
    dx_ref[0] = (dh_ref[0].astype(F32) + d_x).astype(BF16)


def attention_grad(d_h, tokens, qkv, weights, head_dim):
    n_seq, seq_len, d_model = tokens.shape
    seq_spec = pl.BlockSpec((1, seq_len, d_model), lambda s: (s, 0, 0))
    qkv_spec = pl.BlockSpec((1, seq_len, 3 * d_model), lambda s: (s, 0, 0))
    w_spec = pl.BlockSpec(weights.shape, lambda s: (0, 0, 0, 0))
    return pl.pallas_call(
        functools.partial(attention_grad_kernel, head_dim=head_dim),
        grid=(n_seq,),
        in_specs=[seq_spec, seq_spec, qkv_spec, w_spec],
        out_specs=seq_spec,
        out_shape=jax.ShapeDtypeStruct(tokens.shape, BF16),
        scratch_shapes=[pltpu.VMEM((seq_len, d_model), BF16), pltpu.VMEM((seq_len, 3 * d_model), BF16)],
        name='attention_grad',
        **settings(150, 70),
    )(d_h, tokens, qkv, weights)


def capacity_of(tok_count, top_k, num_experts):
    return max(8, (5 * tok_count * top_k // (4 * num_experts) + 7) // 8 * 8)


def route_kernel(loc_ref, dest_ref, start_ref, rows_ref, off_ref, total, *, n_local):
    top_k = loc_ref.shape[1]
    ids = lax.broadcasted_iota(jnp.int32, (n_local, BLOCK), 0)
    upper = (lax.broadcasted_iota(jnp.int32, (BLOCK, BLOCK), 0) <= lax.broadcasted_iota(jnp.int32, (BLOCK, BLOCK), 1)).astype(F32).astype(BF16)
    before = (lax.broadcasted_iota(jnp.int32, (n_local, n_local), 0) > lax.broadcasted_iota(jnp.int32, (n_local, n_local), 1)).astype(F32).astype(BF16)

    @pl.when(pl.program_id(0) == 0)
    def _():
        total[...] = jnp.zeros(total.shape, jnp.int32)

    so_far = total[...]
    for s in range(loc_ref.shape[0]):
        for p in range(loc_ref.shape[2] // BLOCK):
            q = s * (loc_ref.shape[2] // BLOCK) + p
            loc = loc_ref[s, :, p * BLOCK:(p + 1) * BLOCK]
            member = jnp.zeros((n_local, BLOCK), F32)
            for j in range(top_k):
                member = jnp.where(loc[j:j + 1] == ids, 1.0, member)
            count = jnp.dot(member.astype(BF16), upper, preferred_element_type=F32)
            units = (count[:, BLOCK - 1:].astype(jnp.int32) + (ALIGN - 1)) // ALIGN
            units = jnp.broadcast_to(units, (n_local, LANES))
            start = jnp.dot(before, units.astype(F32).astype(BF16), preferred_element_type=F32).astype(jnp.int32) * ALIGN
            place = start[:, :1] + count.astype(jnp.int32) - 1
            for j in range(top_k):
                row = jnp.sum(jnp.where(loc[j:j + 1] == ids, place, 0), axis=0, keepdims=True)
                dest_ref[q, j:j + 1, :] = jnp.where(loc[j:j + 1] >= 0, row, -1)
            start_ref[q] = start
            rows_ref[q] = units * ALIGN
            off_ref[q] = so_far
            so_far = so_far + units * ALIGN
    total[...] = so_far


def route(local_ids, n_local):
    n_seq, top_k, seq_len = local_ids.shape
    per_seq = seq_len // BLOCK
    step = 2 if n_seq % 2 == 0 else 1
    n_blocks = n_seq * per_seq
    seg = jax.ShapeDtypeStruct((n_blocks, n_local, LANES), jnp.int32)
    seg_spec = pl.BlockSpec((step * per_seq, n_local, LANES), lambda s: (s, 0, 0))
    dest, *segs = pl.pallas_call(
        functools.partial(route_kernel, n_local=n_local),
        grid=(n_seq // step,),
        in_specs=[pl.BlockSpec((step, top_k, seq_len), lambda s: (s, 0, 0))],
        out_specs=[pl.BlockSpec((step * per_seq, top_k, BLOCK), lambda s: (s, 0, 0)), seg_spec, seg_spec, seg_spec],
        out_shape=[jax.ShapeDtypeStruct((n_blocks, top_k, BLOCK), jnp.int32), seg, seg, seg],
        scratch_shapes=[pltpu.VMEM((n_local, LANES), jnp.int32)],
        name='route',
        **settings(1, 3),
    )(local_ids)
    return dest, [part[:, :, 0] for part in segs]


def one_hot(dest_ref, gate_ref, first_row):
    rows = lax.broadcasted_iota(jnp.int32, (TILE, BLOCK), 0).astype(F32).astype(BF16)
    dest = jnp.clip(dest_ref[0] - first_row, -1, TILE).astype(F32).astype(BF16)
    gate = gate_ref[0]
    picked = jnp.zeros((TILE, BLOCK), BF16)
    for j in range(dest.shape[0]):
        picked = jnp.where(rows == dest[j:j + 1], gate[j:j + 1], picked)
    return picked, jnp.where(picked > 0, jnp.ones_like(picked), jnp.zeros_like(picked))


def dispatch_kernel(start_ref, rows_ref, off_ref, h_ref, dout_ref, dest_ref, gate_ref, *refs, base):
    r_hbm, d_hbm, u_s, rbuf, dbuf, sem = refs[-6:]
    step = pl.program_id(0)
    n_blocks = pl.num_programs(0)
    b = step + base
    n_exp = rows_ref.shape[1]
    slot = lax.rem(b, 2)

    def total(blk):
        return start_ref[blk, n_exp - 1] + rows_ref[blk, n_exp - 1]

    def drain(blk, which):
        n = pl.multiple_of(total(blk), ALIGN)

        @pl.when(n > 0)
        def _():
            pltpu.make_async_copy(rbuf.at[which, pl.ds(0, n), :], rbuf.at[which, pl.ds(0, n), :], sem.at[0, which]).wait()
            pltpu.make_async_copy(dbuf.at[which, pl.ds(0, n), :], dbuf.at[which, pl.ds(0, n), :], sem.at[1, which]).wait()

    @pl.when(step >= 2)
    def _():
        drain(b - 2, slot)

    hf = h_ref[...].astype(F32)
    u_s[...] = (hf * lax.rsqrt(jnp.mean(hf * hf, axis=-1, keepdims=True) + EPS)).astype(BF16)

    def tile(i, carry):
        first = pl.multiple_of(i * TILE, TILE)
        picked, ones = one_hot(dest_ref, gate_ref, first)
        rbuf[slot, pl.ds(first, TILE), :] = jnp.dot(ones, u_s[...], preferred_element_type=F32).astype(BF16)
        dbuf[slot, pl.ds(first, TILE), :] = jnp.dot(picked, dout_ref[...], preferred_element_type=F32).astype(BF16)
        return carry

    lax.fori_loop(0, (total(b) + (TILE - 1)) // TILE, tile, 0)

    def send(e, carry):
        n = pl.multiple_of(rows_ref[b, e], ALIGN)
        src = pl.multiple_of(start_ref[b, e], ALIGN)
        dst = pl.multiple_of(off_ref[b, e], ALIGN)

        @pl.when(n > 0)
        def _():
            pltpu.make_async_copy(rbuf.at[slot, pl.ds(src, n), :], r_hbm.at[e, pl.ds(dst, n), :], sem.at[0, slot]).start()
            pltpu.make_async_copy(dbuf.at[slot, pl.ds(src, n), :], d_hbm.at[e, pl.ds(dst, n), :], sem.at[1, slot]).start()

        return carry

    lax.fori_loop(0, n_exp, send, 0)

    @pl.when(step == n_blocks - 1)
    def _():
        @pl.when(n_blocks > 1)
        def _():
            drain(b - 1, 1 - slot)

        drain(b, slot)


def block_rows(top_k, n_local):
    return -(-(BLOCK * top_k + n_local * (ALIGN - 1)) // TILE) * TILE


def dispatch(h_tok, dout_tok, dest, gate, segs, base, held, n_local, max_rows):
    tok_count, d_model = h_tok.shape
    top_k = dest.shape[1]
    n_blocks = tok_count // BLOCK
    buf_rows = block_rows(top_k, n_local)
    tok_spec = pl.BlockSpec((BLOCK, d_model), lambda b, *_: (b, 0))
    map_spec = pl.BlockSpec((1, top_k, BLOCK), lambda b, *_: (b + base, 0, 0))
    rows_shape = jax.ShapeDtypeStruct((n_local, max_rows, d_model), BF16)
    hbm = pl.BlockSpec(memory_space=pl.ANY)
    return pl.pallas_call(
        functools.partial(dispatch_kernel, base=base),
        grid_spec=pltpu.PrefetchScalarGridSpec(
            num_scalar_prefetch=3,
            grid=(n_blocks,),
            in_specs=[tok_spec, tok_spec, map_spec, map_spec] + [hbm] * len(held),
            out_specs=[hbm, hbm],
            scratch_shapes=[
                pltpu.VMEM((BLOCK, d_model), BF16),
                pltpu.VMEM((2, buf_rows, d_model), BF16),
                pltpu.VMEM((2, buf_rows, d_model), BF16),
                pltpu.SemaphoreType.DMA((2, 2)),
            ],
        ),
        out_shape=[rows_shape, rows_shape],
        input_output_aliases={7: 0, 8: 1} if held else {},
        name='dispatch',
        **settings(40, 90),
    )(*segs, h_tok, dout_tok, dest, gate, *held)


def expert_kernel(count_ref, flip_ref, r_hbm, d_hbm, w_lo, w_hi, y_hbm, dr_hbm, dw_ref, rbuf, dbuf, ybuf, drbuf, done, in_sem, out_sem, *, expert_of, x_first):
    step = pl.program_id(0)
    n_steps = pl.num_programs(0)
    expert = expert_of(step)
    n_rows = count_ref[expert]
    n_tiles = jnp.maximum((n_rows + (TILE - 1)) // TILE, 1)
    half = dw_ref.shape[-1]

    def copies(who, i, slot, load):
        rows = pl.ds(pl.multiple_of(i * TILE, TILE), TILE)
        pairs = ((r_hbm, rbuf), (d_hbm, dbuf)) if load else ((ybuf, y_hbm), (drbuf, dr_hbm))
        for k, (src, dst) in enumerate(pairs):
            src = src.at[who, rows, :] if load else src.at[slot]
            dst = dst.at[slot] if load else dst.at[who, rows, :]
            yield pltpu.make_async_copy(src, dst, (in_sem if load else out_sem).at[k, slot])

    def start(*args):
        for copy in copies(*args):
            copy.start()

    def wait(*args):
        for copy in copies(*args):
            copy.wait()

    @pl.when(step == 0)
    def _():
        done[0] = 0
        start(expert, 0, 0, True)

    before = done[0]
    for p in range(dw_ref.shape[0]):
        for q in range(dw_ref.shape[1]):
            for t in range(dw_ref.shape[2]):
                clear(dw_ref.at[p, q, t, 0])

    def tile(i, carry):
        slot = lax.rem(before + i, 2)

        @pl.when(i + 1 < n_tiles)
        def _():
            start(expert, i + 1, 1 - slot, True)

        @pl.when((i + 1 == n_tiles) & (step + 1 < n_steps))
        def _():
            start(expert_of(step + 1), 0, 1 - slot, True)

        wait(expert, i, slot, True)

        @pl.when(before + i >= 2)
        def _():
            wait(expert, i, slot, False)

        valid = lax.broadcasted_iota(jnp.int32, (TILE, 1), 0) + i * TILE < n_rows
        r = jnp.where(valid, rbuf[slot], 0)
        dy = jnp.where(valid, dbuf[slot], 0)
        w1, w3, w2 = (jnp.concatenate([w[0, t, 0] for w in (w_lo, w_hi)], axis=t // 2) for t in range(3))
        act_a = jnp.dot(r, w1, preferred_element_type=F32)
        act_b = jnp.dot(r, w3, preferred_element_type=F32)
        d_g = nt_dot(dy, w2)
        sig = 1.0 / (1.0 + jnp.exp(-act_a))
        silu = act_a * sig
        g = (silu * act_b).astype(BF16)
        d_up = (d_g * silu).astype(BF16)
        d_gate = (d_g * act_b * sig * (1.0 + act_a * (1.0 - sig))).astype(BF16)
        ybuf[slot] = jnp.dot(g, w2, preferred_element_type=F32).astype(BF16)
        drbuf[slot] = (nt_dot(d_gate, w1) + nt_dot(d_up, w3)).astype(BF16)
        start(expert, i, slot, False)
        for f in range(2):
            part = slice(f * half, (f + 1) * half)
            to = lax.rem(f + flip_ref[0], 2)
            for t, (lhs, rhs) in enumerate(((r[:, part], d_gate), (r[:, part], d_up), (g, dy[:, part]))):
                dw_ref[(0, to, t, 0) if x_first else (to, 0, t, 0)] += tn_dot(lhs, rhs)
        return carry

    lax.fori_loop(0, n_tiles, tile, 0)
    done[0] = before + n_tiles

    @pl.when(step == n_steps - 1)
    def _():
        last = before + n_tiles - 1
        wait(expert, 0, lax.rem(last, 2), False)

        @pl.when(last >= 1)
        def _():
            wait(expert, 0, lax.rem(last + 1, 2), False)


def experts(rows, d_rows, weights, counts, flips, first, local_experts, x_first=False):
    d_model = rows.shape[2]
    n_owners, three, size, half, _ = weights.shape
    n_fsdp = d_model // half
    n_side = n_owners // n_fsdp

    def expert_of(g):
        return g // size * local_experts + first + lax.rem(g, size)

    def side(g, flip):
        return lax.rem(g // size + flip[1], n_side)

    def w_spec(f):
        return pl.BlockSpec((1, three, 1, half, half), lambda g, _, flip: (lax.rem(f + flip[0], n_fsdp) * n_side + side(g, flip), 0, lax.rem(g, size), 0, 0))

    def dw_index(g, _, flip):
        place = (side(g, flip), 0) if x_first else (0, side(g, flip))
        return (*place, 0, lax.rem(g, size), 0, 0)

    hbm = pl.BlockSpec(memory_space=pl.ANY)
    grads = (n_side, n_fsdp) if x_first else (n_fsdp, n_side)
    dw_block = (1, n_fsdp) if x_first else (n_fsdp, 1)
    return pl.pallas_call(
        functools.partial(expert_kernel, expert_of=expert_of, x_first=x_first),
        grid_spec=pltpu.PrefetchScalarGridSpec(
            num_scalar_prefetch=2,
            grid=(n_side * size,),
            in_specs=[hbm, hbm, w_spec(0), w_spec(1)],
            out_specs=[hbm, hbm, pl.BlockSpec((*dw_block, three, 1, half, half), dw_index)],
            scratch_shapes=[pltpu.VMEM((2, TILE, d_model), BF16)] * 4 + [pltpu.SMEM((1,), jnp.int32)] + [pltpu.SemaphoreType.DMA((2, 2))] * 2,
        ),
        out_shape=[jax.ShapeDtypeStruct(rows.shape, BF16)] * 2 + [jax.ShapeDtypeStruct((*grads, three, size, half, half), F32)],
        input_output_aliases={2: 0, 3: 1},
        name='experts',
        **settings(56 * size, 100 * size),
    )(counts, flips, rows, d_rows, weights, weights)


def clear(ref):
    def rows(i, carry):
        ref[pl.ds(pl.multiple_of(i * LANES, LANES), LANES), :] = jnp.zeros((LANES, ref.shape[1]), ref.dtype)
        return carry

    lax.fori_loop(0, ref.shape[0] // LANES, rows, 0)


def combine_kernel(start_ref, rows_ref, off_ref, y_hbm, dr_hbm, dest_ref, gate_ref, *refs, base, own):
    ybuf, dbuf, acc_y, acc_d, sem = refs[-5:]
    step = pl.program_id(0)
    n_blocks = pl.num_programs(0)
    b = step + base
    n_exp = rows_ref.shape[1]
    slot = lax.rem(step, 2)

    def total(blk):
        return start_ref[blk, n_exp - 1] + rows_ref[blk, n_exp - 1]

    def fetch(blk, which):
        def one(e, carry):
            n = pl.multiple_of(rows_ref[blk, e], ALIGN)
            dst = pl.multiple_of(start_ref[blk, e], ALIGN)
            src = pl.multiple_of(off_ref[blk, e], ALIGN)

            @pl.when(n > 0)
            def _():
                pltpu.make_async_copy(y_hbm.at[e, pl.ds(src, n), :], ybuf.at[which, pl.ds(dst, n), :], sem.at[0, which]).start()
                pltpu.make_async_copy(dr_hbm.at[e, pl.ds(src, n), :], dbuf.at[which, pl.ds(dst, n), :], sem.at[1, which]).start()

            return carry

        lax.fori_loop(0, n_exp, one, 0)

    @pl.when(step == 0)
    def _():
        for which in range(2):
            clear(ybuf.at[which])
            clear(dbuf.at[which])
        fetch(b, 0)

    @pl.when(step + 1 < n_blocks)
    def _():
        fetch(b + 1, 1 - slot)

    n = pl.multiple_of(total(b), ALIGN)

    @pl.when(n > 0)
    def _():
        pltpu.make_async_copy(ybuf.at[slot, pl.ds(0, n), :], ybuf.at[slot, pl.ds(0, n), :], sem.at[0, slot]).wait()
        pltpu.make_async_copy(dbuf.at[slot, pl.ds(0, n), :], dbuf.at[slot, pl.ds(0, n), :], sem.at[1, slot]).wait()

    acc_y[...] = jnp.zeros(acc_y.shape, F32)
    acc_d[...] = jnp.zeros(acc_d.shape, F32)

    def tile(i, carry):
        first = pl.multiple_of(i * TILE, TILE)
        picked, ones = one_hot(dest_ref, gate_ref, first)
        acc_y[...] += tn_dot(picked, ybuf[slot, pl.ds(first, TILE), :])
        acc_d[...] += tn_dot(ones, dbuf[slot, pl.ds(first, TILE), :])
        return carry

    lax.fori_loop(0, (n + (TILE - 1)) // TILE, tile, 0)

    if not own:
        out_y, out_d = refs[:2]
        out_y[...] = acc_y[...]
        out_d[...] = acc_d[...]
        return
    more_y, more_d, h_ref, dout_ref, out_ref, dh_ref = refs[:6]
    hf = h_ref[...].astype(F32)
    out_ref[...] = (hf + (acc_y[...] + more_y[...])).astype(BF16)
    d_u = (acc_d[...] + more_d[...]).astype(BF16).astype(F32)
    inv = lax.rsqrt(jnp.mean(hf * hf, axis=-1, keepdims=True) + EPS)
    proj = jnp.mean(d_u * hf, axis=-1, keepdims=True)
    d_norm = (d_u * inv - hf * (inv * inv * inv * proj)).astype(BF16).astype(F32)
    dh_ref[...] = (dout_ref[...].astype(F32) + d_norm).astype(BF16)


def combine(y_rows, dr_rows, dest, gate, segs, base, n_blocks, extra):
    n_local, _, d_model = y_rows.shape
    top_k = dest.shape[1]
    buf_rows = block_rows(top_k, n_local)
    tok_spec = pl.BlockSpec((BLOCK, d_model), lambda b, *_: (b, 0))
    map_spec = pl.BlockSpec((1, top_k, BLOCK), lambda b, *_: (b + base, 0, 0))
    hbm = pl.BlockSpec(memory_space=pl.ANY)
    out = jax.ShapeDtypeStruct((n_blocks * BLOCK, d_model), BF16 if extra else F32)
    return pl.pallas_call(
        functools.partial(combine_kernel, base=base, own=bool(extra)),
        grid_spec=pltpu.PrefetchScalarGridSpec(
            num_scalar_prefetch=3,
            grid=(n_blocks,),
            in_specs=[hbm, hbm, map_spec, map_spec] + [tok_spec] * len(extra),
            out_specs=[tok_spec, tok_spec],
            scratch_shapes=[
                pltpu.VMEM((2, buf_rows, d_model), BF16),
                pltpu.VMEM((2, buf_rows, d_model), BF16),
                pltpu.VMEM((BLOCK, d_model), F32),
                pltpu.VMEM((BLOCK, d_model), F32),
                pltpu.SemaphoreType.DMA((2, 2)),
            ],
        ),
        out_shape=[out, out],
        name='combine',
        **settings(45, 120),
    )(*segs, y_rows, dr_rows, dest, gate, *extra)


def place_kernel(*refs, n_parts):
    for k, out_ref in enumerate(refs[-3:]):
        value = refs[0][k]
        for part_ref in refs[1:n_parts]:
            value = value + part_ref[k]
        out_ref[...] = value


def place(parts, held, first, n_total):
    three, size, rows, cols = parts[0].shape
    hbm = pl.BlockSpec(memory_space=pl.ANY)
    return pl.pallas_call(
        functools.partial(place_kernel, n_parts=len(parts)),
        grid=(size,),
        in_specs=[pl.BlockSpec((three, 1, rows, cols), lambda i: (0, i, 0, 0))] * len(parts) + [hbm] * len(held),
        out_specs=[pl.BlockSpec((1, rows, cols), lambda i: (first + i, 0, 0))] * three,
        out_shape=[jax.ShapeDtypeStruct((n_total, rows, cols), F32)] * three,
        input_output_aliases={len(parts) + k: k for k in range(len(held))},
        name='place',
        **settings(1, 12),
    )(*parts, *held)


CHUNKS = (2, 4)
CORES = 2


def solution(mesh):
    ep_size, fsdp_size = mesh.shape['ep'], mesh.shape['fsdp']
    tok_spec = P(('data', 'fsdp', 'ep'))
    in_specs = (tok_spec, P('fsdp'), P(None, None, 'fsdp'), P('ep', 'fsdp'), P('ep', 'fsdp'), P('ep', None, 'fsdp'), tok_spec, tok_spec, tok_spec, tok_spec)
    out_specs = (tok_spec, tok_spec, P(('data', 'ep'), 'fsdp'), P(('data', 'ep'), 'fsdp'), P(('data', 'ep'), None, 'fsdp'))

    def device_fn(tokens, w_qkv, w_out, w_gate, w_up, w_down, expert_idx, expert_slot, gate_wts, d_out):
        n_seq, seq_len, d_model = tokens.shape
        tok_count = n_seq * seq_len
        top_k = expert_idx.shape[2]
        local_experts, half, _ = w_gate.shape
        num_experts = local_experts * ep_size
        n_side = ep_size // CORES
        n_local = local_experts * n_side
        n_blocks = tok_count // BLOCK
        capacity = capacity_of(tok_count, top_k, num_experts)
        max_rows = -(-(CORES * (capacity + n_blocks * (ALIGN - 1))) // TILE) * TILE
        ep = lax.axis_index('ep')
        groups = [[c + CORES * i for i in range(fsdp_size * n_side)] for c in range(CORES)]

        fsdp, side = lax.axis_index('fsdp'), ep // CORES
        flips = jnp.stack([fsdp, side]).astype(jnp.int32)

        def swap(values):
            return lax.ppermute(values, 'ep', [(i, i ^ 1) for i in range(ep_size)])

        def swap_x(values):
            return lax.ppermute(values, 'ep', [(i, i ^ CORES) for i in range(ep_size)])

        def swap_y(values):
            return lax.ppermute(values, 'fsdp', [(i, i ^ 1) for i in range(fsdp_size)])

        def own_weights(part):
            return jnp.stack([w_gate[part], w_up[part], w_down[part]], axis=0)

        _, head_dim, _ = w_out.shape
        qkv_rows = w_qkv.transpose(1, 2, 3, 0).reshape(-1, half)
        qkv_rows = lax.dynamic_slice_in_dim(qkv_rows, ep * (3 * d_model // ep_size), 3 * d_model // ep_size, axis=0)
        out_rows = lax.dynamic_slice_in_dim(w_out.reshape(-1, half), ep * (d_model // ep_size), d_model // ep_size, axis=0)
        attn_w = lax.all_gather(jnp.concatenate([qkv_rows, out_rows], axis=0), ('fsdp', 'ep'), axis=0, tiled=False)
        attn_w = attn_w.reshape(fsdp_size, ep_size, -1, half)
        weights, first = [], 0
        for size in CHUNKS:
            mine = own_weights(slice(first, first + size))
            full = lax.all_gather(mine, ('fsdp', 'ep'), axis=0, tiled=False, axis_index_groups=groups)
            weights.append(full)
            first += size
        mid = first + (local_experts - first) // 2
        w_a, w_b = own_weights(slice(first, mid)), own_weights(slice(mid, local_experts))
        w_ax, w_ay, w_bx, w_by = swap_x(w_a), swap_y(w_a), swap_x(w_b), swap_y(w_b)

        dout_tok = d_out.reshape(tok_count, d_model)
        dout_other = swap(dout_tok)
        kept_ids = jnp.where(expert_slot >= 0, expert_idx, -1).transpose(0, 2, 1)
        all_ids = jnp.concatenate([kept_ids, swap(kept_ids)], axis=0)
        owner = all_ids // local_experts
        mine_too = (all_ids >= 0) & (lax.rem(owner, CORES) == lax.rem(ep, CORES))
        local_ids = jnp.where(mine_too, owner // CORES * local_experts + lax.rem(all_ids, local_experts), -1)
        dest, segs = route(local_ids, n_local)
        counts = jnp.sum(segs[1], axis=0)
        gate = gate_wts.transpose(0, 2, 1)
        gate = jnp.concatenate([gate, swap(gate)], axis=0)
        gate = gate.reshape(2 * n_seq, top_k, seq_len // BLOCK, BLOCK).transpose(0, 2, 1, 3).reshape(2 * n_blocks, top_k, BLOCK)

        tokens, dest, segs, counts, gate = lax.optimization_barrier((tokens, dest, segs, counts, gate))
        h_seq, qkv = attention(tokens, attn_w, head_dim)
        w_axy, w_byx = swap_y(w_ax), swap_x(w_by)
        w_rest = jnp.stack([jnp.concatenate(pair, axis=1) for pair in ((w_a, w_b), (w_ax, w_bx), (w_ay, w_by), (w_axy, w_byx))])
        h_tok = h_seq.reshape(tok_count, d_model)
        h_other = swap(h_tok)
        held = dispatch(h_tok, dout_tok, dest, gate, segs, 0, [], n_local, max_rows)
        rows, d_rows = dispatch(h_other, dout_other, dest, gate, segs, n_blocks, held, n_local, max_rows)
        grads, start = [], 0
        for n, size in enumerate(CHUNKS):
            rows, d_rows, d_w = experts(rows, d_rows, weights[n], counts, jnp.zeros_like(flips), start, local_experts)
            d_w = d_w.reshape(fsdp_size * n_side, *d_w.shape[2:])
            grads.append(([lax.psum_scatter(d_w, ('fsdp', 'ep'), scatter_dimension=0, tiled=False, axis_index_groups=groups)], start))
            start += size
            if n == 0:
                rows, d_rows, d_rest = experts(rows, d_rows, w_rest, counts, flips, first, local_experts)
                d_a, d_b = d_rest[:, :, :, :mid - first], d_rest[:, :, :, mid - first:]
                more_a, more_b = swap_x(d_a[:, 1]), swap_y(d_b[1])
        sums = d_a[:, 0] + more_a, d_b[0] + more_b
        more_a, more_b = swap_y(sums[0][1]), swap_x(sums[1][1])
        done = [grads[0], ([sums[0][0], more_a], first), ([sums[1][0], more_b], mid), grads[1]]
        sums = combine(rows, d_rows, dest, gate, segs, n_blocks, n_blocks, [])
        more = [swap(value) for value in sums]
        layer_out, d_h = combine(rows, d_rows, dest, gate, segs, 0, n_blocks, [*more, h_tok, dout_tok])
        d_tokens = attention_grad(d_h.reshape(n_seq, seq_len, d_model), tokens, qkv, attn_w, head_dim)
        d_ws = []
        for parts, where in done:
            d_ws = place(parts, d_ws, where, local_experts)
        return layer_out.reshape(n_seq, seq_len, d_model), d_tokens, *d_ws

    return jax.shard_map(device_fn, mesh=mesh, in_specs=in_specs, out_specs=out_specs, check_vma=False)
```
